128 devices in a mesh: stage: 2 (over core), data: 64 (over z, y, x).
Axes of the slice: x: 4, y: 4, z: 4, core: 2. Of those that a mesh axis runs over, the one named last changes fastest.
Arguments:
- x_in: bfloat16 [16, 4096, 1024], P(None, 'data')
- targets: bfloat16 [16, 4096, 1024], P(None, 'data')
- w_work: bfloat16 [2, 1, 8388608], P('stage')
- w_master: float32 [2, 1, 8388608], P('stage', None, 'data')
- m_prior: float32 [2, 1, 8388608], P('stage', None, 'data')
- v_prior: float32 [2, 1, 8388608], P('stage', None, 'data')
- clip_tau: float32 [], replicated
Outputs:
- output 1: float32 [], replicated
- output 2: bfloat16 [2, 1, 8388608], P('stage')
- output 3: float32 [2, 1, 8388608], P('stage', None, 'data')
- output 4: float32 [2, 1, 8388608], P('stage', None, 'data')
- output 5: float32 [2, 1, 8388608], P('stage', None, 'data')
All inputs are finite; a program needn't handle non-finite values.
Results may differ from the reference program's by a relative error of at most 0.001.
Values are sent between devices in bfloat16 or wider.
A program may use at most 1 GiB of HBM per device.

```python
import math
import jax
import jax.numpy as jnp
from jax import lax

D_MODEL = 1024
LAYERS = 1
MICROBATCHES = 16
TOK_DEV = 64
STAGES = 2
DATA_SIZE = 64
ADAM_STEP = 10

ROW_COUNT = DATA_SIZE * TOK_DEV
HALF_LEN = 4 * D_MODEL * D_MODEL
FLAT_LEN = 2 * HALF_LEN
ADAM_BETA1 = 0.9
ADAM_BETA2 = 0.95
ADAM_EPS = 1e-8
WEIGHT_DECAY = 0.1
LEARN_RATE = 0.05 / math.sqrt(D_MODEL)


def gelu_tanh(z_val):
    return jax.nn.gelu(z_val, approximate=True)


def split_layer(w_flat):
    return w_flat[:HALF_LEN].reshape(D_MODEL, 4 * D_MODEL), w_flat[HALF_LEN:].reshape(4 * D_MODEL, D_MODEL)


def layer_forward(hidden, w_flat):
    w_in, w_out = split_layer(w_flat)
    pre_act = jnp.dot(hidden, w_in, preferred_element_type=jnp.float32).astype(jnp.bfloat16)
    act_bf = gelu_tanh(pre_act.astype(jnp.float32)).astype(jnp.bfloat16)
    out_rows = (hidden.astype(jnp.float32) + jnp.dot(act_bf, w_out, preferred_element_type=jnp.float32)).astype(jnp.bfloat16)
    return out_rows, pre_act


def layer_backward(hidden, pre_act, grad_h, w_flat):
    w_in, w_out = split_layer(w_flat)
    act_f, gelu_pull = jax.vjp(gelu_tanh, pre_act.astype(jnp.float32))
    act_bf = act_f.astype(jnp.bfloat16)
    grad_act = jnp.dot(grad_h, w_out.T, preferred_element_type=jnp.float32)
    grad_pre = gelu_pull(grad_act)[0].astype(jnp.bfloat16)
    grad_in = (grad_h.astype(jnp.float32) + jnp.dot(grad_pre, w_in.T, preferred_element_type=jnp.float32)).astype(jnp.bfloat16)
    g_first = jnp.dot(hidden.T, grad_pre, preferred_element_type=jnp.float32)
    g_second = jnp.dot(act_bf.T, grad_h, preferred_element_type=jnp.float32)
    return grad_in, jnp.concatenate([g_first.reshape(-1), g_second.reshape(-1)])


def loss_and_grads(x_in, targets, w_work):
    w_layers = w_work.reshape(-1, w_work.shape[-1])
    token_count = x_in.shape[0] * x_in.shape[1]

    def fwd_body(hidden, w_flat):
        out_rows, pre_act = layer_forward(hidden, w_flat)
        return out_rows, (hidden, pre_act)

    def bwd_body(grad_h, layer_data):
        hidden, pre_act, w_flat = layer_data
        return layer_backward(hidden, pre_act, grad_h, w_flat)

    def micro_step(scan_state, micro_batch):
        grad_acc, loss_acc = scan_state
        x_rows, t_rows = micro_batch
        y_rows, saved_acts = lax.scan(fwd_body, x_rows, w_layers)
        residual = y_rows.astype(jnp.float32) - t_rows.astype(jnp.float32)
        loss_acc = loss_acc + 0.5 * jnp.sum(residual * residual)
        grad_top = (residual / token_count).astype(jnp.bfloat16)
        _, layer_grads = lax.scan(bwd_body, grad_top, (saved_acts[0], saved_acts[1], w_layers), reverse=True)
        return (grad_acc + layer_grads, loss_acc), None

    start_state = (jnp.zeros(w_layers.shape, jnp.float32), jnp.zeros((), jnp.float32))
    (grad_acc, loss_acc), _ = lax.scan(micro_step, start_state, (x_in, targets))
    return loss_acc / token_count, grad_acc.reshape(w_work.shape)


def setup_inputs(seed: int = 0) -> dict:
    root_key = jax.random.key(seed)
    sub_keys = jax.random.split(root_key, 7)
    depth_n = STAGES * LAYERS
    x_in = jax.random.normal(sub_keys[0], (MICROBATCHES, ROW_COUNT, D_MODEL), jnp.float32).astype(jnp.bfloat16)
    targets = jax.random.normal(sub_keys[1], (MICROBATCHES, ROW_COUNT, D_MODEL), jnp.float32).astype(jnp.bfloat16)
    w_first = jax.random.normal(sub_keys[2], (STAGES, LAYERS, HALF_LEN), jnp.float32) / math.sqrt(D_MODEL)
    w_second = jax.random.normal(sub_keys[3], (STAGES, LAYERS, HALF_LEN), jnp.float32) / math.sqrt(4 * D_MODEL * depth_n)
    w_master = jnp.concatenate([w_first, w_second], axis=-1)
    w_work = w_master.astype(jnp.bfloat16)
    _, grads = loss_and_grads(x_in, targets, w_work)
    grad_norm = jnp.sqrt(jnp.sum(grads * grads))
    first_part = grads[:, :, :HALF_LEN]
    second_part = grads[:, :, HALF_LEN:]
    first_rms = jnp.sqrt(jnp.mean(first_part * first_part, axis=-1, keepdims=True))
    second_rms = jnp.sqrt(jnp.mean(second_part * second_part, axis=-1, keepdims=True))
    grad_scale = 0.4 * jnp.where(jnp.arange(FLAT_LEN) < HALF_LEN, first_rms, second_rms)
    m_prior = (1.0 - ADAM_BETA1) * grad_scale * jax.random.normal(sub_keys[4], w_master.shape, jnp.float32)
    v_prior = (1.0 - ADAM_BETA2) * grad_scale * grad_scale * jax.random.uniform(sub_keys[5], w_master.shape, jnp.float32, 0.5, 2.0)
    clip_tau = grad_norm * jax.random.uniform(sub_keys[6], (), jnp.float32, 0.3, 0.5)
    return {'x_in': x_in, 'targets': targets, 'w_work': w_work, 'w_master': w_master, 'm_prior': m_prior, 'v_prior': v_prior, 'clip_tau': clip_tau}


def reference(x_in, targets, w_work, w_master, m_prior, v_prior, clip_tau):
    loss_mean, grads = loss_and_grads(x_in, targets, w_work)
    grad_norm = jnp.sqrt(jnp.sum(grads * grads))
    clip_scale = jnp.minimum(1.0, clip_tau / grad_norm)
    scaled = clip_scale * grads
    m_new = ADAM_BETA1 * m_prior + (1.0 - ADAM_BETA1) * scaled
    v_new = ADAM_BETA2 * v_prior + (1.0 - ADAM_BETA2) * scaled * scaled
    m_hat = m_new / (1.0 - ADAM_BETA1 ** ADAM_STEP)
    v_hat = v_new / (1.0 - ADAM_BETA2 ** ADAM_STEP)
    w_new = w_master - LEARN_RATE * (m_hat / (jnp.sqrt(v_hat) + ADAM_EPS) + WEIGHT_DECAY * w_master)
    return (loss_mean, w_new.astype(jnp.bfloat16), w_new, m_new, v_new)
```

```python
import functools
import math
import jax
import jax.numpy as jnp
from jax import lax
from jax.experimental import pallas as pl
from jax.experimental.pallas import tpu as pltpu
from jax.sharding import PartitionSpec as P

ADAM_BETA1 = 0.9
ADAM_BETA2 = 0.95
ADAM_EPS = 1e-8
WEIGHT_DECAY = 0.1
ADAM_STEP = 10
LR_BASE = 0.05
MESH = pl.DeviceIdType.MESH
MIB = 1024 * 1024

SUBS = 4
SUB_ROWS = 256
ALL = slice(None)
RS_ORDER = ((2, 1, 0), (1, 0, 2), (0, 2, 1))
AG_ORDER = ((0, 1, 2), (1, 2, 0), (2, 0, 1))


def rs_split():
    table = {}
    for s in range(SUBS):
        sizes = [11, 11, 11]
        sizes[(s + 2) % 3] = 10
        start = 32 * s
        for c in range(3):
            n = sizes[c]
            first = (n + (s + c) % 2) // 2
            table[s, c] = (start * 8, first * 8, (n - first) * 8)
            start += n
    return table


def coords_of(me):
    return [me // 16, lax.rem(me // 4, 4), lax.rem(me, 4)]


def peer(coords, pos, delta):
    moved = list(coords)
    moved[pos] = lax.rem(coords[pos] + (delta + 4), 4)
    return moved[0] * 16 + moved[1] * 4 + moved[2]


def greet(coords):
    barrier = pltpu.get_barrier_semaphore()
    for pos in range(3):
        for delta in (1, -1):
            pl.semaphore_signal(barrier, inc=1, device_id={"data": peer(coords, pos, delta)}, device_id_type=MESH)
    pl.semaphore_wait(barrier, 6)


def rs_kernel(g_ref, out_ref, ra1, rb1, lb, own, ra2, rb2, ra3, rb3, ssem, rsem, lsem):
    coords = coords_of(lax.axis_index("data"))
    table = rs_split()
    ra = (ra1, ra2, ra3)
    rb = (rb1, rb2, rb3)
    copies = {}
    deltas = (1, -1)

    def rows(s, c, half):
        start, n0, n1 = table[s, c]
        if half == 0:
            return 0, n0
        if half == 1:
            return n0, n1
        return 0, n0 + n1

    def lead(ph, c, k):
        order = RS_ORDER[c]
        left = [p for p in (0, 1, 2) if p != order[0]]
        idx = []
        for p in left:
            if ph == 1:
                idx.append(k if p == order[1] else pl.ds(0, 4))
            else:
                idx.append(coords[order[1]] if p == order[1] else k)
        return tuple(idx)

    def lead_t(ph, c, k, t):
        if ph == 0:
            return (t // 4, lax.rem(t, 4))
        return tuple(t if not isinstance(i, jax.Array) and isinstance(i, pl.Slice) else i for i in lead(ph, c, k))

    def source(ph, s, c, k, half):
        lo, n = rows(s, c, half)
        if ph == 0:
            idx = [pl.ds(0, 4)] * 3
            idx[RS_ORDER[c][0]] = k
            return g_ref.at[tuple(idx) + (pl.ds(table[s, c][0] + lo, n), ALL)]
        return own.at[(s * 3 + c,) + lead(ph, c, k) + (pl.ds(lo, n), ALL)]

    def slot(ref, ph, i, lo, n):
        return ref.at[(i,) + (pl.ds(0, 4),) * (2 - ph) + (pl.ds(lo, n), ALL)]

    def start(ph, s, c, d, piece, src, dst):
        i = (((ph * SUBS + s) * 3 + c) * 2 + d) * 3 + piece
        target = peer(coords, RS_ORDER[c][ph], deltas[d])
        copy = pltpu.make_async_remote_copy(src_ref=src, dst_ref=dst, send_sem=ssem.at[i], recv_sem=rsem.at[i],
                                            device_id={"data": target}, device_id_type=MESH)
        copy.start()
        copies[ph, s, c, d, piece] = copy

    def at(c, ph, delta):
        return lax.rem(coords[RS_ORDER[c][ph]] + (delta + 4), 4)

    def send_a(ph, s, c):
        for d in range(2):
            n = rows(s, c, d)[1]
            start(ph, s, c, d, 0, source(ph, s, c, at(c, ph, 2), d), slot(ra[ph], ph, s * 6 + c * 2 + d, 0, n))

    def send_b1(ph, s, c):
        for d in range(2):
            lo, n = rows(s, c, 1 - d)
            start(ph, s, c, d, 1, source(ph, s, c, at(c, ph, deltas[d]), 1 - d), slot(rb[ph], ph, s * 6 + c * 2 + d, lo, n))

    def load(s, c):
        for d in range(2):
            i = s * 9 + c * 3 + d
            n = rows(s, c, d)[1]
            copy = pltpu.make_async_copy(source(0, s, c, at(c, 0, deltas[d]), d), slot(lb, 0, s * 6 + c * 2 + d, 0, n), lsem.at[i])
            copy.start()
            copies["lb", s, c, d] = copy
        n = rows(s, c, 2)[1]
        copy = pltpu.make_async_copy(source(0, s, c, at(c, 0, 0), 2), slot(own, 0, s * 3 + c, 0, n), lsem.at[s * 9 + c * 3 + 2])
        copy.start()
        copies["own", s, c] = copy

    def forward(ph, s, c):
        for d in range(2):
            i = s * 6 + c * 2 + d
            lo, n = rows(s, c, d)
            if ph == 0:
                copies["lb", s, c, d].wait()
            copies[ph, s, c, d, 0].wait_recv()
            buf = ra[ph]
            k = at(c, ph, deltas[d])
            if ph == 2:
                buf[i, pl.ds(0, n), :] += own[(s * 3 + c,) + lead(2, c, k) + (pl.ds(lo, n), ALL)]
            elif ph == 1:
                def body1(t, carry, i=i, n=n, lo=lo, buf=buf, k=k):
                    buf[i, t, pl.ds(0, n), :] += own[(s * 3 + c,) + lead_t(1, c, k, t) + (pl.ds(lo, n), ALL)]
                    return carry
                lax.fori_loop(0, 4, body1, 0)
            else:
                def body0(t, carry, i=i, n=n, buf=buf):
                    u, v = t // 4, lax.rem(t, 4)
                    buf[i, u, v, pl.ds(0, n), :] += lb[i, u, v, pl.ds(0, n), :]
                    return carry
                lax.fori_loop(0, 16, body0, 0)
            start(ph, s, c, d, 2, slot(buf, ph, i, 0, n), slot(rb[ph], ph, i, lo, n))

    def finish(ph, s, c):
        if ph == 0:
            copies["own", s, c].wait()
        for d in range(2):
            copies[ph, s, c, d, 1].wait_recv()
            copies[ph, s, c, d, 2].wait_recv()
        n = rows(s, c, 2)[1]
        i, j = s * 6 + c * 2, s * 3 + c
        buf = rb[ph]
        k = at(c, ph, 0)
        span = pl.ds(0, n)
        if ph == 2:
            total = own[(j,) + lead(2, c, k) + (span, ALL)] + buf[i, span, :] + buf[i + 1, span, :]
            out_ref[pl.ds(table[s, c][0], n), :] = total
            return
        if ph == 1:
            def body1(t, carry):
                where = (j,) + lead_t(1, c, k, t) + (span, ALL)
                own[where] = own[where] + buf[i, t, span, :] + buf[i + 1, t, span, :]
                return carry
            lax.fori_loop(0, 4, body1, 0)
            return

        def body0(t, carry):
            u, v = t // 4, lax.rem(t, 4)
            own[j, u, v, span, :] = own[j, u, v, span, :] + buf[i, u, v, span, :] + buf[i + 1, u, v, span, :]
            return carry
        lax.fori_loop(0, 16, body0, 0)

    def st0(s):
        for c in range(3):
            send_a(0, s, c)
            load(s, c)

    def st0b(s):
        for c in range(3):
            send_b1(0, s, c)

    def mid(ph, s):
        for c in range(3):
            forward(ph, s, c)

    def turn(ph, s):
        for c in range(3):
            finish(ph, s, c)
            if ph < 2:
                send_a(ph + 1, s, c)
                send_b1(ph + 1, s, c)

    def opening(s):
        if s < SUBS:
            st0(s)

    def second(s):
        if s < SUBS:
            st0b(s)

    steps = []
    for s in range(SUBS):
        done = 3 * s + 4
        steps.append((max(s, 3 * s - 1), 0, mid, 0, s))
        for ph in range(3):
            steps.append((done + 4 * ph, 1, turn, ph, s))
            if ph:
                steps.append((done + 4 * ph - 2, 1, mid, ph, s))
    greet(coords)
    opening(0)
    opening(1)
    second(0)
    for _, _, act, ph, s in sorted(steps, key=lambda e: e[:2]):
        act(ph, s)
        if act is mid and ph == 0:
            opening(s + 2)
            second(s + 1)
    for key, copy in copies.items():
        if not isinstance(key[0], str):
            copy.wait_send()


def reduce_scatter(g):
    sems = 3 * SUBS * 3 * 2 * 3
    f32 = jnp.float32
    return pl.pallas_call(
        rs_kernel,
        out_shape=jax.ShapeDtypeStruct((1024, 128), f32),
        in_specs=[pl.BlockSpec(memory_space=pl.ANY)],
        out_specs=pl.BlockSpec(memory_space=pltpu.VMEM),
        scratch_shapes=[
            pltpu.VMEM((SUBS * 6, 4, 4, 48, 128), f32),
            pltpu.VMEM((SUBS * 6, 4, 4, 88, 128), f32),
            pltpu.VMEM((SUBS * 6, 4, 4, 48, 128), f32),
            pltpu.VMEM((SUBS * 3, 4, 4, 88, 128), f32),
            pltpu.VMEM((SUBS * 6, 4, 48, 128), f32),
            pltpu.VMEM((SUBS * 6, 4, 88, 128), f32),
            pltpu.VMEM((SUBS * 6, 48, 128), f32),
            pltpu.VMEM((SUBS * 6, 88, 128), f32),
            pltpu.SemaphoreType.DMA((sems,)),
            pltpu.SemaphoreType.DMA((sems,)),
            pltpu.SemaphoreType.DMA((SUBS * 9,)),
        ],
        compiler_params=pltpu.CompilerParams(collective_id=0, has_side_effects=True, vmem_limit_bytes=60 * MIB),
        name="grad_rs",
    )(g)


def ag_split():
    table = []
    start = 0
    for c, n in enumerate((22, 21, 21)):
        first = (n + c % 2) // 2
        table.append((start * 16, first * 16, (n - first) * 16))
        start += n
    return table


def ag_kernel(w_ref, out_ref, ssem, rsem, lsem):
    coords = coords_of(lax.axis_index("data"))
    table = ag_split()
    deltas = (1, -1)
    copies = {}

    def rows(c, half):
        start, n0, n1 = table[c]
        return (start, n0) if half == 0 else (start + n0, n1)

    def region(c, unit, shift, half):
        first, second, third = AG_ORDER[c]
        idx = [None] * 3
        if unit == 0:
            idx[first], idx[second], idx[third] = lax.rem(coords[first] + (shift + 4), 4), coords[second], coords[third]
        elif unit == 1:
            idx[first], idx[second], idx[third] = pl.ds(0, 4), lax.rem(coords[second] + (shift + 4), 4), coords[third]
        else:
            q = lax.rem(coords[second] + ((0, -1, 1, 2)[unit - 2] + 4), 4)
            idx[first], idx[second], idx[third] = pl.ds(0, 4), q, lax.rem(coords[third] + (shift + 4), 4)
        lo, n = rows(c, half)
        return out_ref.at[tuple(idx) + (pl.ds(lo, n), ALL)]

    def start(c, unit, d, piece, src, dst):
        i = ((unit * 3 + c) * 2 + d) * 3 + piece
        target = peer(coords, AG_ORDER[c][min(unit, 2)], deltas[d])
        copy = pltpu.make_async_remote_copy(src_ref=src, dst_ref=dst, send_sem=ssem.at[i], recv_sem=rsem.at[i],
                                            device_id={"data": target}, device_id_type=MESH)
        copy.start()
        copies[c, unit, d, piece] = copy

    def begin(unit):
        for c in range(3):
            for d in range(2):
                for piece, half in ((0, d), (1, 1 - d)):
                    lo, n = rows(c, half)
                    here = region(c, unit, 0, half)
                    src = w_ref.at[pl.ds(lo, n), :] if unit == 0 else here
                    start(c, unit, d, piece, src, here)

    def middle(unit):
        for c in range(3):
            for d in range(2):
                copies[c, unit, d, 0].wait_recv()
                part = region(c, unit, -deltas[d], d)
                start(c, unit, d, 2, part, part)

    def arrive(unit, piece):
        for c in range(3):
            for d in range(2):
                copies[c, unit, d, piece].wait_recv()

    greet(coords)
    local = pltpu.make_async_copy(w_ref, out_ref.at[coords[0], coords[1], coords[2]], lsem)
    local.start()
    begin(0)
    middle(0)
    arrive(0, 1)
    arrive(0, 2)
    local.wait()
    begin(1)
    begin(2)
    middle(1)
    arrive(1, 1)
    begin(3)
    begin(4)
    middle(2)
    arrive(1, 2)
    begin(5)
    middle(3)
    middle(4)
    middle(5)
    for unit in (2, 3, 4, 5):
        arrive(unit, 1)
        arrive(unit, 2)
    for copy in copies.values():
        copy.wait_send()


def all_gather_rows(w):
    sems = 6 * 3 * 2 * 3
    return pl.pallas_call(
        ag_kernel,
        out_shape=jax.ShapeDtypeStruct((4, 4, 4, 1024, 128), w.dtype),
        in_specs=[pl.BlockSpec(memory_space=pltpu.VMEM)],
        out_specs=pl.BlockSpec(memory_space=pl.ANY),
        scratch_shapes=[
            pltpu.SemaphoreType.DMA((sems,)),
            pltpu.SemaphoreType.DMA((sems,)),
            pltpu.SemaphoreType.DMA,
        ],
        compiler_params=pltpu.CompilerParams(collective_id=1, has_side_effects=True),
        name="weight_ag",
    )(w)


def wgrad_kernel(x_ref, du_ref, a_ref, g_ref, out_ref):
    part = pl.program_id(1)

    @pl.when(part == 0)
    def _():
        def body(m, carry):
            cols = pl.ds(pl.multiple_of(m * 256, 256), 256)
            val = lax.dot_general(x_ref[:, cols], du_ref[...], (((0,), (0,)), ((), ())), preferred_element_type=jnp.float32)
            for ct in range(8):
                out_ref[pl.ds(m * 8, 8), ct * 32:(ct + 1) * 32, :] = val[:, ct * 128:(ct + 1) * 128].reshape(8, 32, 128)
            return carry
        lax.fori_loop(0, 4, body, 0)

    @pl.when(part == 1)
    def _():
        def body(m, carry):
            cols = pl.ds(pl.multiple_of(m * 1024, 1024), 1024)
            val = lax.dot_general(a_ref[:, cols], g_ref[...], (((0,), (0,)), ((), ())), preferred_element_type=jnp.float32)
            for ct in range(2):
                out_ref[pl.ds(m * 8, 8), ct * 128:(ct + 1) * 128, :] = val[:, ct * 128:(ct + 1) * 128].reshape(8, 128, 128)
            return carry
        lax.fori_loop(0, 4, body, 0)


def weight_grads(x, du, a, g):
    rows, d = x.shape
    return pl.pallas_call(
        wgrad_kernel,
        grid=(SUBS, 2),
        out_shape=jax.ShapeDtypeStruct((64, 1024, 128), jnp.float32),
        in_specs=[
            pl.BlockSpec((rows, d), lambda s, p: (0, 0)),
            pl.BlockSpec((rows, d), lambda s, p: (0, s)),
            pl.BlockSpec((rows, 4 * d), lambda s, p: (0, 0)),
            pl.BlockSpec((rows, d // 4), lambda s, p: (0, s)),
        ],
        out_specs=pl.BlockSpec((32, SUB_ROWS, 128), lambda s, p: (p, s, 0)),
        compiler_params=pltpu.CompilerParams(vmem_limit_bytes=56 * MIB, dimension_semantics=("arbitrary", "arbitrary")),
        cost_estimate=pl.CostEstimate(flops=4 * rows * d * 4 * d, bytes_accessed=52 * MIB, transcendentals=0),
        name="wgrad",
    )(x, du, a, g)


def unflatten_kernel(cols, w_ref, o_ref, wide):
    n = wide.shape[0] // 8
    for j in range(n):
        wide[j * 8:(j + 1) * 8, :] = w_ref[:, j * 1024:(j + 1) * 1024].astype(jnp.float32).reshape(8, 128)
    blocks = cols // 128
    rows = o_ref.shape[0]
    for cb in range(blocks):
        o_ref[:, cb * 128:(cb + 1) * 128] = wide[pl.ds(cb, rows, stride=blocks), :].astype(o_ref.dtype)


def unflatten(flat, part, cols):
    chunk = 131072
    steps = flat.shape[1] // 2 // chunk
    rows = chunk // cols
    return pl.pallas_call(
        functools.partial(unflatten_kernel, cols),
        grid=(steps,),
        out_shape=jax.ShapeDtypeStruct((rows * steps, cols), flat.dtype),
        in_specs=[pl.BlockSpec((1, chunk), lambda i: (0, part * steps + i))],
        out_specs=pl.BlockSpec((rows, cols), lambda i: (i, 0)),
        scratch_shapes=[pltpu.VMEM((chunk // 128, 128), jnp.float32)],
        name="unflatten",
    )(flat)


def flatten_kernel(w_ref, o_ref):
    for j in range(o_ref.shape[1] // 2048):
        o_ref[:, j * 2048:(j + 1) * 2048] = w_ref[j * 16:(j + 1) * 16, :].astype(jnp.float32).reshape(1, 2048).astype(o_ref.dtype)


def flatten(rows):
    chunk = 131072
    total = rows.size
    return pl.pallas_call(
        flatten_kernel,
        grid=(total // chunk,),
        out_shape=jax.ShapeDtypeStruct((1, total), rows.dtype),
        in_specs=[pl.BlockSpec((chunk // 128, 128), lambda i: (i, 0))],
        out_specs=pl.BlockSpec((1, chunk), lambda i: (0, i)),
        name="flatten",
    )(rows)


def gelu_tanh(z_val):
    return jax.nn.gelu(z_val, approximate=True)


def dot32(a, b, dims=((1,), (0,))):
    return lax.dot_general(a, b, (dims, ((), ())), preferred_element_type=jnp.float32)


def block_forward(x, w1, w2):
    u = dot32(x, w1).astype(jnp.bfloat16)
    a = gelu_tanh(u.astype(jnp.float32)).astype(jnp.bfloat16)
    return u, a, (x.astype(jnp.float32) + dot32(a, w2)).astype(jnp.bfloat16)


def pre_grad(u, g, w2):
    e = dot32(g, w2, ((1,), (1,)))
    _, pull = jax.vjp(gelu_tanh, u.astype(jnp.float32))
    return pull(e)[0].astype(jnp.bfloat16)


def adam_update(w_master, m_prior, v_prior, grad_part, clip_scale, d_model):
    scaled = clip_scale * grad_part
    m_new = ADAM_BETA1 * m_prior + (1.0 - ADAM_BETA1) * scaled
    v_new = ADAM_BETA2 * v_prior + (1.0 - ADAM_BETA2) * scaled * scaled
    m_hat = m_new / (1.0 - ADAM_BETA1 ** ADAM_STEP)
    v_hat = v_new / (1.0 - ADAM_BETA2 ** ADAM_STEP)
    learn_rate = LR_BASE / math.sqrt(d_model)
    w_new = w_master - learn_rate * (m_hat / (jnp.sqrt(v_hat) + ADAM_EPS) + WEIGHT_DECAY * w_master)
    return w_new, m_new, v_new


def solution(mesh):
    data_size = mesh.shape['data']

    def device_step(x_in, targets, w_work, w_master, m_prior, v_prior, clip_tau):
        d = x_in.shape[-1]
        rows = x_in.shape[0] * x_in.shape[1]
        token_count = rows * data_size
        x0 = x_in.reshape(rows, d)
        t0 = targets.reshape(rows, d)
        flat = w_work.reshape(1, -1)
        w1 = unflatten(flat, 0, 4 * d)
        w2 = unflatten(flat, 1, d)
        stage = lax.axis_index('stage')
        is_first = stage == 0
        bf = jnp.bfloat16
        wide = jnp.zeros((rows, 4 * d), bf)
        narrow = jnp.zeros((rows, d), bf)

        u0, a0, h0 = lax.cond(is_first, lambda: block_forward(x0, w1, w2), lambda: (wide, wide, narrow))
        h_recv = lax.ppermute(h0, 'stage', [(0, 1)])

        def last_stage():
            u, a, y = block_forward(h_recv, w1, w2)
            res = y.astype(jnp.float32) - t0.astype(jnp.float32)
            loss = 0.5 * jnp.sum(res * res)
            g = (res / token_count).astype(bf)
            du = pre_grad(u, g, w2)
            g_in = (g.astype(jnp.float32) + dot32(du, w1, ((1,), (1,)))).astype(bf)
            return h_recv, u, a, g, du, g_in, loss

        x, u, a, g1, du1, g_in, loss_acc = lax.cond(
            is_first, lambda: (x0, u0, a0, narrow, wide, narrow, jnp.zeros((), jnp.float32)), last_stage)
        g_recv = lax.ppermute(g_in, 'stage', [(1, 0)])
        g, du = lax.cond(is_first, lambda: (g_recv, pre_grad(u, g_recv, w2)), lambda: (g1, du1))

        grads = weight_grads(x, du, a, g)
        part = reduce_scatter(grads.reshape(4, 4, 4, 1024, 128))
        totals = lax.psum(jnp.stack([jnp.sum(part * part), loss_acc]), ('stage', 'data'))
        clip_scale = jnp.minimum(1.0, clip_tau / jnp.sqrt(totals[0]))
        early = lax.axis_index('data') < data_size // 2
        part_flat = jnp.where(early, part.reshape(32, 32, 128).transpose(1, 0, 2).reshape(1, 1, -1),
                              part.reshape(8, 128, 128).transpose(1, 0, 2).reshape(1, 1, -1))
        w_new, m_new, v_new = adam_update(w_master, m_prior, v_prior, part_flat, clip_scale, d)
        gathered = all_gather_rows(w_new.astype(bf).reshape(1024, 128))
        return totals[1] / token_count, flatten(gathered.reshape(-1, 128)).reshape(1, 1, -1), w_new, m_new, v_new

    row_spec = P(None, 'data', None)
    shard_spec = P('stage', None, 'data')
    stage_spec = P('stage', None, None)
    return jax.shard_map(device_step, mesh=mesh, in_specs=(row_spec, row_spec, stage_spec, shard_spec, shard_spec, shard_spec, P()), out_specs=(P(), stage_spec, shard_spec, shard_spec, shard_spec), check_vma=False)
```

```python
import functools
import math
import jax
import jax.numpy as jnp
from jax import lax
from jax.experimental import pallas as pl
from jax.experimental.pallas import tpu as pltpu
from jax.sharding import PartitionSpec as P

ADAM_BETA1 = 0.9
ADAM_BETA2 = 0.95
ADAM_EPS = 1e-8
WEIGHT_DECAY = 0.1
ADAM_STEP = 10
LR_BASE = 0.05
MESH = pl.DeviceIdType.MESH
MIB = 1024 * 1024

SUBS = 4
SUB_ROWS = 256
ALL = slice(None)
RING = pl.ds(0, 4)
BOTH = range(2)
AXES = range(3)
LEADS = (16, 4, 1)
ROWWISE = ((0,), (0,))
DELTAS = (1, -1)
RS_ORDER = ((2, 1, 0), (1, 0, 2), (0, 2, 1))
UNIT_SHIFT = {2: 0, 3: -1, 4: 1, 5: 2}
AG_ORDER = ((0, 1, 2), (1, 2, 0), (2, 0, 1))


def upto(n):
    return pl.ds(0, n)


def divide(t):
    return t // 4, lax.rem(t, 4)


def wrap(k):
    return lax.rem(k + 4, 4)


def rs_split():
    table = {}
    for s in range(SUBS):
        sizes = [11, 11, 11]
        sizes[(s + 2) % 3] = 10
        start = 32 * s
        for c in AXES:
            n = sizes[c]
            first = (n + (s + c) % 2) // 2
            table[s, c] = tuple(8 * k for k in (start, first, n - first))
            start += n
    return table


def coords_of(me):
    return [me // 16, lax.rem(me // 4, 4), lax.rem(me, 4)]


def peer(coords, pos, delta):
    moved = list(coords)
    moved[pos] = wrap(coords[pos] + delta)
    z, y, x = moved
    return z * 16 + y * 4 + x


def greet(coords, deltas, partner):
    barrier = pltpu.get_barrier_semaphore()
    ids = [{"data": peer(coords, pos, delta)} for pos in AXES for delta in deltas]
    if partner:
        ids.append({"stage": 1 - lax.axis_index("stage")})
    for other in ids:
        pl.semaphore_signal(barrier, inc=1, device_id=other, device_id_type=MESH)
    pl.semaphore_wait(barrier, len(ids))


def sum_everywhere(coords, acc, got, ssem, rsem):
    copies = []
    for ph in range(4):
        if ph < 3:
            mine = coords[ph]
            targets = [{"data": peer(coords, ph, k)} for k in range(1, 4)]
        else:
            mine = lax.axis_index("stage")
            targets = [{"stage": 1 - mine}]
        batch = []
        for k, target in enumerate(targets):
            i = ph * 3 + k
            batch.append(pltpu.make_async_remote_copy(src_ref=acc.at[ph], dst_ref=got.at[ph, mine], send_sem=ssem.at[i],
                                                      recv_sem=rsem.at[i], device_id=target, device_id_type=MESH))
        for copy in batch:
            copy.start()
        got[ph, mine] = acc[ph]
        for copy in batch:
            copy.wait_recv()
        acc[ph + 1] = sum(got[ph, k] for k in range(len(batch) + 1))
        copies += batch
    for copy in copies:
        copy.wait_send()


def rs_kernel(g_ref, loss_ref, out_ref, total_ref, ra1, rb1, lb, own, ra2, rb2, ra3, rb3, ssem, rsem, lsem, acc, got, tsem, usem):
    coords = coords_of(lax.axis_index("data"))
    table = rs_split()
    ra = (ra1, ra2, ra3)
    rb = (rb1, rb2, rb3)
    copies = {}

    def rows(s, c, half):
        start, n0, n1 = table[s, c]
        if half == 0:
            return 0, n0
        if half == 1:
            return n0, n1
        return 0, n0 + n1

    def lead(ph, c, k):
        order = RS_ORDER[c]
        left = [p for p in AXES if p != order[0]]
        idx = []
        for p in left:
            if ph == 1:
                idx.append(k if p == order[1] else RING)
            else:
                idx.append(coords[order[1]] if p == order[1] else k)
        return tuple(idx)

    def lead_t(ph, c, k, t):
        if ph == 0:
            return divide(t), divide(t)
        mine = tuple(t if i is RING else i for i in lead(ph, c, k))
        return (t,) * (2 - ph), mine

    def source(ph, s, c, k, half):
        lo, n = rows(s, c, half)
        if ph == 0:
            idx = [RING] * 3
            idx[RS_ORDER[c][0]] = k
            return g_ref.at[tuple(idx) + (pl.ds(table[s, c][0] + lo, n), ALL)]
        return own.at[(s * 3 + c,) + lead(ph, c, k) + (pl.ds(lo, n), ALL)]

    def slot(ref, ph, i, lo, n):
        return ref.at[(i,) + (RING,) * (2 - ph) + (pl.ds(lo, n), ALL)]

    def start(ph, s, c, d, piece, src, dst):
        i = (((ph * SUBS + s) * 3 + c) * 2 + d) * 3 + piece
        target = peer(coords, RS_ORDER[c][ph], DELTAS[d])
        copy = pltpu.make_async_remote_copy(src_ref=src, dst_ref=dst, send_sem=ssem.at[i], recv_sem=rsem.at[i],
                                            device_id={"data": target}, device_id_type=MESH)
        copy.start()
        copies[ph, s, c, d, piece] = copy

    def at(c, ph, delta):
        return wrap(coords[RS_ORDER[c][ph]] + delta)

    def send_a(ph, s, c):
        for d in BOTH:
            n = rows(s, c, d)[1]
            start(ph, s, c, d, 0, source(ph, s, c, at(c, ph, 2), d), slot(ra[ph], ph, s * 6 + c * 2 + d, 0, n))

    def send_b1(ph, s, c):
        for d in BOTH:
            lo, n = rows(s, c, 1 - d)
            start(ph, s, c, d, 1, source(ph, s, c, at(c, ph, DELTAS[d]), 1 - d), slot(rb[ph], ph, s * 6 + c * 2 + d, lo, n))

    def load(s, c):
        for d in BOTH:
            i = s * 9 + c * 3 + d
            n = rows(s, c, d)[1]
            copy = pltpu.make_async_copy(source(0, s, c, at(c, 0, DELTAS[d]), d), slot(lb, 0, s * 6 + c * 2 + d, 0, n), lsem.at[i])
            copy.start()
            copies["lb", s, c, d] = copy
        n = rows(s, c, 2)[1]
        copy = pltpu.make_async_copy(source(0, s, c, at(c, 0, 0), 2), slot(own, 0, s * 3 + c, 0, n), lsem.at[s * 9 + c * 3 + 2])
        copy.start()
        copies["own", s, c] = copy

    def forward(ph, s, c):
        for d in BOTH:
            i = s * 6 + c * 2 + d
            lo, n = rows(s, c, d)
            if ph == 0:
                copies["lb", s, c, d].wait()
            copies[ph, s, c, d, 0].wait_recv()
            buf = ra[ph]
            k = at(c, ph, DELTAS[d])

            def body(t, carry, i=i, n=n, lo=lo, buf=buf, k=k):
                where, mine = lead_t(ph, c, k, t)
                term = lb[(i,) + where + (upto(n), ALL)] if ph == 0 else own[(s * 3 + c,) + mine + (pl.ds(lo, n), ALL)]
                buf[(i,) + where + (upto(n), ALL)] += term
                return carry

            lax.fori_loop(0, LEADS[ph], body, 0)
            start(ph, s, c, d, 2, slot(buf, ph, i, 0, n), slot(rb[ph], ph, i, lo, n))

    def finish(ph, s, c):
        if ph == 0:
            copies["own", s, c].wait()
        for d in BOTH:
            copies[ph, s, c, d, 1].wait_recv()
            copies[ph, s, c, d, 2].wait_recv()
        n = rows(s, c, 2)[1]
        i, j = s * 6 + c * 2, s * 3 + c
        buf = rb[ph]
        k = at(c, ph, 0)
        span = upto(n)

        def body(t, carry):
            where, mine = lead_t(ph, c, k, t)
            mine = (j,) + mine + (span, ALL)
            total = own[mine] + buf[(i,) + where + (span, ALL)] + buf[(i + 1,) + where + (span, ALL)]
            if ph < 2:
                own[mine] = total
            else:
                out_ref[pl.ds(table[s, c][0], n), :] = total
            return carry

        lax.fori_loop(0, LEADS[ph], body, 0)

    def st0(s):
        for c in AXES:
            send_a(0, s, c)
            load(s, c)

    def st0b(s):
        for c in AXES:
            send_b1(0, s, c)

    def mid(ph, s):
        for c in AXES:
            forward(ph, s, c)

    def turn(ph, s):
        for c in AXES:
            finish(ph, s, c)
            if ph < 2:
                send_a(ph + 1, s, c)
                send_b1(ph + 1, s, c)

    def opening(s):
        if s < SUBS:
            st0(s)

    def second(s):
        if s < SUBS:
            st0b(s)

    steps = []
    for s in range(SUBS):
        done = 3 * s + 4
        steps.append((max(s, 3 * s - 1), 0, mid, 0, s))
        for ph in AXES:
            steps.append((done + 4 * ph, 1, turn, ph, s))
            if ph:
                steps.append((done + 4 * ph - 2, 1, mid, ph, s))
    greet(coords, range(1, 4), True)
    opening(0)
    opening(1)
    second(0)
    for _, _, act, ph, s in sorted(steps, key=lambda e: e[:2]):
        act(ph, s)
        if act is mid and ph == 0:
            opening(s + 2)
            second(s + 1)
    for key, copy in copies.items():
        if not isinstance(key[0], str):
            copy.wait_send()
    part = out_ref[...]
    acc[0, 0] = jnp.sum((part * part).reshape(-1, 8, 128), axis=0)
    acc[0, 1] = loss_ref[...]
    sum_everywhere(coords, acc, got, tsem, usem)
    total_ref[...] = acc[4]


def reduce_scatter(g, loss):
    sems = 54 * SUBS
    f32 = jnp.float32
    dma = pltpu.SemaphoreType.DMA
    vmem = pl.BlockSpec(memory_space=pltpu.VMEM)

    def slots(n, axes, rows):
        return pltpu.VMEM((SUBS * n,) + (4,) * axes + (rows, 128), f32)

    return pl.pallas_call(
        rs_kernel,
        out_shape=(jax.ShapeDtypeStruct((1024, 128), f32), jax.ShapeDtypeStruct((2, 8, 128), f32)),
        in_specs=[pl.BlockSpec(memory_space=pl.ANY), vmem],
        out_specs=(vmem, vmem),
        scratch_shapes=[slots(6, 2, 48), slots(6, 2, 88), slots(6, 2, 48), slots(3, 2, 88), slots(6, 1, 48), slots(6, 1, 88),
                        slots(6, 0, 48), slots(6, 0, 88), dma((sems,)), dma((sems,)), dma((SUBS * 9,)),
                        pltpu.VMEM((5, 2, 8, 128), f32), pltpu.VMEM((4, 4, 2, 8, 128), f32), dma((10,)), dma((10,))],
        compiler_params=pltpu.CompilerParams(collective_id=0, has_side_effects=True, vmem_limit_bytes=60 * MIB),
        name="grad_rs",
    )(g, loss)


def ag_split():
    table = []
    start = 0
    for c, n in enumerate((22, 21, 21)):
        first = (n + c % 2) // 2
        table.append(tuple(16 * k for k in (start, first, n - first)))
        start += n
    return table


def ag_kernel(w_ref, wide_ref, out_ref, stage, ssem, rsem, lsem):
    coords = coords_of(lax.axis_index("data"))
    table = ag_split()
    copies = {}

    def rows(c, half):
        start, n0, n1 = table[c]
        return (start, n0) if half == 0 else (start + n0, n1)

    def region(c, unit, shift, half):
        first, second, third = AG_ORDER[c]
        idx = [None] * 3
        if unit == 0:
            idx[first], idx[second], idx[third] = wrap(coords[first] + shift), coords[second], coords[third]
        elif unit == 1:
            idx[first], idx[second], idx[third] = RING, wrap(coords[second] + shift), coords[third]
        else:
            q = wrap(coords[second] + UNIT_SHIFT[unit])
            idx[first], idx[second], idx[third] = RING, q, wrap(coords[third] + shift)
        lo, n = rows(c, half)
        return out_ref.at[tuple(idx) + (pl.ds(lo, n), ALL)]

    def start(c, unit, d, piece, src, dst):
        i = ((unit * 3 + c) * 2 + d) * 3 + piece
        target = peer(coords, AG_ORDER[c][min(unit, 2)], DELTAS[d])
        copy = pltpu.make_async_remote_copy(src_ref=src, dst_ref=dst, send_sem=ssem.at[i], recv_sem=rsem.at[i],
                                            device_id={"data": target}, device_id_type=MESH)
        copy.start()
        copies[c, unit, d, piece] = copy

    def begin(unit):
        for c in AXES:
            for d in BOTH:
                for piece, half in ((0, d), (1, 1 - d)):
                    lo, n = rows(c, half)
                    here = region(c, unit, 0, half)
                    src = w_ref.at[pl.ds(lo, n), :] if unit == 0 else here
                    start(c, unit, d, piece, src, here)

    def middle(unit):
        for c in AXES:
            for d in BOTH:
                copies[c, unit, d, 0].wait_recv()
                part = region(c, unit, -DELTAS[d], d)
                start(c, unit, d, 2, part, part)

    def arrive(unit, piece):
        for c in AXES:
            for d in BOTH:
                copies[c, unit, d, piece].wait_recv()

    flights = []

    def widen(unit):
        for c in AXES:
            start, n0, n1 = table[c]
            n = n0 + n1
            second = AG_ORDER[c][1]
            q = wrap(coords[second] + UNIT_SHIFT[unit])
            i = len(flights)
            if i > 1:
                flights[i - 2].wait()

            def body(t, carry):
                u, v = divide(t)
                where = [u, v]
                where.insert(second, q)
                stage[i % 2, u, v, upto(n), :] = out_ref[tuple(where) + (pl.ds(start, n), ALL)].astype(jnp.float32)
                return carry

            lax.fori_loop(0, 16, body, 0)
            where = [RING] * 2
            where.insert(second, q)
            flights.append(pltpu.make_async_copy(stage.at[i % 2, :, :, upto(n), :],
                                                 wide_ref.at[tuple(where) + (pl.ds(start, n), ALL)], lsem.at[i]))
            flights[i].start()

    greet(coords, DELTAS, False)
    begin(0)
    out_ref[tuple(coords)] = w_ref[...]
    middle(0)
    arrive(0, 1)
    arrive(0, 2)
    begin(1)
    begin(2)
    middle(1)
    arrive(1, 1)
    begin(3)
    begin(4)
    middle(2)
    arrive(1, 2)
    begin(5)
    middle(3)
    middle(4)
    middle(5)
    for unit in UNIT_SHIFT:
        arrive(unit, 1)
        arrive(unit, 2)
        widen(unit)
    for flight in flights[-2:]:
        flight.wait()
    for copy in copies.values():
        copy.wait_send()


def all_gather_rows(w):
    dma = pltpu.SemaphoreType.DMA
    sems = 36 * 3
    return pl.pallas_call(
        ag_kernel,
        out_shape=jax.ShapeDtypeStruct((4, 4, 4, 1024, 128), jnp.float32),
        in_specs=[pl.BlockSpec(memory_space=pltpu.VMEM)],
        out_specs=pl.BlockSpec(memory_space=pl.ANY),
        scratch_shapes=[pltpu.VMEM((4, 4, 4, 1024, 128), w.dtype), pltpu.VMEM((2, 4, 4, 352, 128), jnp.float32),
                        dma((sems,)), dma((sems,)), dma((12,))],
        compiler_params=pltpu.CompilerParams(collective_id=1, has_side_effects=True, vmem_limit_bytes=40 * MIB),
        name="weight_ag",
    )(w)


def wgrad_kernel(x_ref, du_ref, a_ref, g_ref, out_ref):
    part = pl.program_id(1)

    @pl.when(part == 0)
    def _():
        def body(m, carry):
            cols = pl.ds(pl.multiple_of(m * 256, 256), 256)
            val = lax.dot_general(x_ref[:, cols], du_ref[...], (ROWWISE, ((), ())), preferred_element_type=jnp.float32)
            for ct in range(8):
                out_ref[pl.ds(m * 8, 8), ct * 32:(ct + 1) * 32, :] = val[:, ct * 128:(ct + 1) * 128].reshape(8, 32, 128)
            return carry
        lax.fori_loop(0, 4, body, 0)

    @pl.when(part == 1)
    def _():
        def body(m, carry):
            cols = pl.ds(pl.multiple_of(m * 1024, 1024), 1024)
            val = lax.dot_general(a_ref[:, cols], g_ref[...], (ROWWISE, ((), ())), preferred_element_type=jnp.float32)
            for ct in BOTH:
                out_ref[pl.ds(m * 8, 8), ct * 128:(ct + 1) * 128, :] = val[:, ct * 128:(ct + 1) * 128].reshape(8, 128, 128)
            return carry
        lax.fori_loop(0, 4, body, 0)


def weight_grads(x, du, a, g):
    rows, d = x.shape
    return pl.pallas_call(
        wgrad_kernel,
        grid=(SUBS, 2),
        out_shape=jax.ShapeDtypeStruct((64, 1024, 128), jnp.float32),
        in_specs=[
            pl.BlockSpec((rows, d), lambda s, p: (0, 0)),
            pl.BlockSpec((rows, d), lambda s, p: (0, s)),
            pl.BlockSpec((rows, 4 * d), lambda s, p: (0, 0)),
            pl.BlockSpec((rows, d // 4), lambda s, p: (0, s)),
        ],
        out_specs=pl.BlockSpec((32, SUB_ROWS, 128), lambda s, p: (p, s, 0)),
        compiler_params=pltpu.CompilerParams(vmem_limit_bytes=56 * MIB, dimension_semantics=("arbitrary", "arbitrary")),
        cost_estimate=pl.CostEstimate(flops=4 * rows * d * 4 * d, bytes_accessed=52 * MIB, transcendentals=0),
        name="wgrad",
    )(x, du, a, g)


ROWS = 1024
WIDE = 4096
TILE = 256
COLS = 512
LANES = 128
STEPS = ROWS // TILE
PIECE = 131072
CHUNK = 4 * PIECE
CHUNKS = 2 * ROWS * WIDE // CHUNK
SLOTS = 4
PITCH = 40
GELU_A = math.sqrt(2.0 / math.pi)
GELU_B = GELU_A * 0.044715
BF16 = jnp.bfloat16
F32 = jnp.float32


def dot32(a, b, dims=((1,), (0,))):
    return lax.dot_general(a, b, (dims, ((), ())), preferred_element_type=F32)


def dot_t(a, b):
    return dot32(a, b, ((1,), (1,)))


def block_kernel(scale, w_ref, xin_ref, t_ref, x_out, a_out, du_out, g_out, loss_ref,
                 w1, w2, xb, hb, gb, ab, db, tb, raw, wide, wsem, insem, outsem, hs, hr, gs, gr):
    stage = lax.axis_index("stage")
    first = stage == 0
    last = stage == 1
    other = {"stage": 1 - stage}

    def chunk(i):
        return pltpu.make_async_copy(w_ref.at[:, pl.ds(pl.multiple_of(i * CHUNK, CHUNK), CHUNK)], raw.at[lax.rem(i, SLOTS)],
                                     wsem.at[lax.rem(i, SLOTS)])

    load_x = pltpu.make_async_copy(xin_ref, xb, insem.at[0])
    load_t = pltpu.make_async_copy(t_ref, tb, insem.at[1])

    def prefetch(i, carry):
        chunk(i).start()
        return carry

    lax.fori_loop(0, SLOTS, prefetch, 0)

    @pl.when(first)
    def _():
        load_x.start()

    @pl.when(last)
    def _():
        load_t.start()

    barrier = pltpu.get_barrier_semaphore()
    pl.semaphore_signal(barrier, inc=1, device_id=other, device_id_type=MESH)
    pl.semaphore_wait(barrier, 1)

    def convert(i, weight, blocks, pitch):
        rows = PIECE // (blocks * LANES)
        chunk(i).wait()

        def body(q, carry):
            for j in range(PIECE // ROWS):
                line = raw[lax.rem(i, SLOTS), :, pl.ds(pl.multiple_of(q * PIECE + j * ROWS, ROWS), ROWS)]
                at = (j * 8 // blocks) * pitch + j * 8 % blocks
                wide[at:at + 8, :] = line.astype(F32).reshape(8, LANES)
            base = pl.ds(pl.multiple_of((lax.rem(i, CHUNKS // 2) * 4 + q) * rows, rows), rows)
            for cb in range(blocks):
                weight[base, cb * LANES:(cb + 1) * LANES] = wide[pl.ds(cb, rows, stride=pitch), :].astype(BF16)
            return carry

        lax.fori_loop(0, 4, body, 0)

        @pl.when(i < CHUNKS - SLOTS)
        def _():
            chunk(i + SLOTS).start()

    def convert_first(i, carry):
        convert(i, w1, WIDE // LANES, PITCH)
        return carry

    def convert_second(i, carry):
        convert(i, w2, ROWS // LANES, ROWS // LANES)
        return carry

    lax.fori_loop(0, CHUNKS // 2, convert_first, 0)
    lax.fori_loop(CHUNKS // 2, CHUNKS, convert_second, 0)

    @pl.when(first)
    def _():
        load_x.wait()

    @pl.when(last)
    def _():
        load_t.wait()

    def span(i):
        return pl.ds(pl.multiple_of(i * TILE, TILE), TILE)

    def cols(j):
        return pl.ds(pl.multiple_of(j * COLS, COLS), COLS)

    def send_h(i):
        return pltpu.make_async_remote_copy(src_ref=hb.at[span(i)], dst_ref=xb.at[span(i)], send_sem=hs.at[i], recv_sem=hr.at[i],
                                            device_id=other, device_id_type=MESH)

    def send_g(i):
        return pltpu.make_async_remote_copy(src_ref=hb.at[span(i)], dst_ref=gb.at[span(i)], send_sem=gs.at[i], recv_sem=gr.at[i],
                                            device_id=other, device_id_type=MESH)

    def outputs(i):
        pairs = ((xb, x_out), (ab, a_out), (db, du_out), (gb, g_out))
        return [pltpu.make_async_copy(src.at[span(i)], dst.at[span(i)], outsem.at[i * 4 + k]) for k, (src, dst) in enumerate(pairs)]

    def forward(i):
        def up(j, carry):
            u = dot32(xb[span(i), :], w1[:, cols(j)]).astype(BF16)
            db[span(i), cols(j)] = u
            uf = u.astype(F32)
            half = 0.5 * uf
            ab[span(i), cols(j)] = (half + half * jnp.tanh(uf * (GELU_A + GELU_B * (uf * uf)))).astype(BF16)
            return carry

        def down(j, carry):
            hb[span(i), cols(j)] = (xb[span(i), cols(j)].astype(F32) + dot32(ab[span(i), :], w2[:, cols(j)])).astype(BF16)
            return carry

        lax.fori_loop(0, WIDE // COLS, up, 0, unroll=2)
        lax.fori_loop(0, ROWS // COLS, down, 0)

    def top(i):
        res = hb[span(i), :].astype(F32) - tb[span(i), :].astype(F32)
        gb[span(i), :] = (res * scale).astype(BF16)
        sums = jnp.sum((res * res).reshape(-1, 8, ROWS), axis=0)
        loss_ref[...] += sum(sums[:, k * LANES:(k + 1) * LANES] for k in range(ROWS // LANES))

    def backward(i):
        def body(j, carry):
            e = dot_t(gb[span(i), :], w2[cols(j), :])
            u = db[span(i), cols(j)].astype(F32)
            sq = u * u
            t = jnp.tanh(u * (GELU_A + GELU_B * sq))
            slope = 0.5 * (1.0 + t) + (0.5 * u) * (1.0 - t * t) * (GELU_A + (3.0 * GELU_B) * sq)
            db[span(i), cols(j)] = (e * slope).astype(BF16)
            return carry

        lax.fori_loop(0, WIDE // COLS, body, 0, unroll=2)

    def below(i):
        def body(j, carry):
            hb[span(i), cols(j)] = (gb[span(i), cols(j)].astype(F32) + dot_t(db[span(i), :], w1[cols(j), :])).astype(BF16)
            return carry

        lax.fori_loop(0, ROWS // COLS, body, 0)

    loss_ref[...] = jnp.zeros_like(loss_ref)

    def tick(it, carry):
        i = lax.rem(it, STEPS)

        @pl.when(it < STEPS)
        def _():
            @pl.when(last)
            def _():
                send_h(i).wait_recv()

            forward(i)

            @pl.when(first)
            def _():
                send_h(i).start()

            @pl.when(last)
            def _():
                top(i)

        @pl.when(it // STEPS + stage == 1)
        def _():
            @pl.when(first)
            def _():
                send_g(i).wait_recv()

            backward(i)

            @pl.when(last)
            def _():
                below(i)
                send_g(i).start()

            for copy in outputs(i):
                copy.start()
        return carry

    lax.fori_loop(0, 2 * STEPS, tick, 0)

    def drain(i, carry):
        @pl.when(first)
        def _():
            send_h(i).wait_send()

        @pl.when(last)
        def _():
            send_g(i).wait_send()

        for copy in outputs(i):
            copy.wait()
        return carry

    lax.fori_loop(0, STEPS, drain, 0)


def block_passes(flat, x_in, targets, token_count):
    anywhere = pl.BlockSpec(memory_space=pl.ANY)
    dma = pltpu.SemaphoreType.DMA
    narrow, wide = (ROWS, ROWS), (ROWS, WIDE)

    def shape(dims):
        return jax.ShapeDtypeStruct(dims, BF16)

    def room(dims):
        return pltpu.VMEM(dims, BF16)

    return pl.pallas_call(
        functools.partial(block_kernel, 1.0 / token_count),
        out_shape=(shape(narrow), shape(wide), shape(wide), shape(narrow), jax.ShapeDtypeStruct((8, LANES), F32)),
        in_specs=[anywhere] * 3,
        out_specs=(anywhere,) * 4 + (pl.BlockSpec(memory_space=pltpu.VMEM),),
        scratch_shapes=[room(wide), room((WIDE, ROWS)), room(narrow), room(narrow), room(narrow), room(wide), room(wide), room(narrow),
                        room((SLOTS, 1, CHUNK)), pltpu.VMEM((32 * PITCH, LANES), F32),
                        dma((SLOTS,)), dma((2,)), dma((STEPS * 4,)), dma((STEPS,)), dma((STEPS,)), dma((STEPS,)), dma((STEPS,))],
        compiler_params=pltpu.CompilerParams(collective_id=2, has_side_effects=True, vmem_limit_bytes=60 * MIB),
        name="block",
    )(flat, x_in, targets)


def adam_kernel(rate, token_count, part_ref, total_ref, tau_ref, w_ref, m_ref, v_ref, w_out, m_out, v_out, b_out, loss_out, grad):
    early = lax.axis_index("data") < 32

    def reorder(rows):
        blocks = ROWS // rows
        for r in range(rows):
            grad[r * blocks:(r + 1) * blocks, :] = part_ref[pl.ds(r, blocks, stride=rows), :]

    @pl.when(early)
    def _():
        reorder(32)

    @pl.when(jnp.logical_not(early))
    def _():
        reorder(LANES)

    nu = jnp.sqrt(jnp.sum(total_ref[0], keepdims=True))
    scaled = jnp.minimum(1.0, tau_ref[...] / nu) * grad[...]
    m_new = ADAM_BETA1 * m_ref[...] + (1.0 - ADAM_BETA1) * scaled
    v_new = ADAM_BETA2 * v_ref[...] + (1.0 - ADAM_BETA2) * scaled * scaled
    m_hat = m_new / (1.0 - ADAM_BETA1 ** ADAM_STEP)
    v_hat = v_new / (1.0 - ADAM_BETA2 ** ADAM_STEP)
    w_new = w_ref[...] - rate * (m_hat / (jnp.sqrt(v_hat) + ADAM_EPS) + WEIGHT_DECAY * w_ref[...])
    w_out[...] = w_new
    m_out[...] = m_new
    v_out[...] = v_new
    b_out[...] = w_new.astype(BF16)
    loss_out[...] = (0.5 * jnp.sum(total_ref[1], keepdims=True)) / token_count


def adam(rate, token_count, part, totals, tau, w, m, v):
    state = jax.ShapeDtypeStruct(part.shape, F32)
    vmem = pl.BlockSpec(memory_space=pltpu.VMEM)
    return pl.pallas_call(
        functools.partial(adam_kernel, rate, token_count),
        out_shape=(state, state, state, jax.ShapeDtypeStruct(part.shape, BF16), jax.ShapeDtypeStruct((1, 1), F32)),
        in_specs=[vmem] * 6,
        out_specs=(vmem,) * 5,
        scratch_shapes=[pltpu.VMEM(part.shape, F32)],
        name="adam",
    )(part, totals, tau, w, m, v)


def solution(mesh):
    data_size = mesh.shape['data']

    def device_step(x_in, targets, w_work, w_master, m_prior, v_prior, clip_tau):
        token_count = x_in.shape[0] * x_in.shape[1] * data_size
        x, a, du, g, loss = block_passes(w_work.reshape(1, -1), x_in.reshape(ROWS, ROWS), targets.reshape(ROWS, ROWS), token_count)
        grads = weight_grads(x, du, a, g)
        part, totals = reduce_scatter(grads.reshape(4, 4, 4, ROWS, LANES), loss)
        rate = LR_BASE / math.sqrt(x_in.shape[-1])
        state = [z.reshape(ROWS, LANES) for z in (w_master, m_prior, v_prior)]
        w_new, m_new, v_new, w_bf, loss_mean = adam(rate, token_count, part, totals, clip_tau.reshape(1, 1), *state)
        w_all = lax.optimization_barrier(all_gather_rows(w_bf).reshape(w_work.shape)).astype(BF16)
        return (loss_mean.reshape(()), w_all) + tuple(z.reshape(w_master.shape) for z in (w_new, m_new, v_new))

    row_spec = P(None, 'data', None)
    shard_spec = P('stage', None, 'data')
    stage_spec = P('stage', None, None)
    return jax.shard_map(device_step, mesh=mesh, in_specs=(row_spec, row_spec, stage_spec, shard_spec, shard_spec, shard_spec, P()), out_specs=(P(), stage_spec, shard_spec, shard_spec, shard_spec), check_vma=False)
```

```python
import functools
import math
import jax
import jax.numpy as jnp
from jax import lax
from jax.experimental import pallas as pl
from jax.experimental.pallas import tpu as pltpu
from jax.sharding import PartitionSpec as P

ADAM_BETA1 = 0.9
ADAM_BETA2 = 0.95
ADAM_EPS = 1e-8
WEIGHT_DECAY = 0.1
ADAM_STEP = 10
LR_BASE = 0.05
MESH = pl.DeviceIdType.MESH
MIB = 1024 * 1024

SUBS = 4
SUB_ROWS = 256
ALL = slice(None)
RING = pl.ds(0, 4)
BOTH = range(2)
AXES = range(3)
LEADS = (16, 4, 1)
ROWWISE = ((0,), (0,))
DELTAS = (1, -1)
RS_ORDER = ((2, 1, 0), (1, 0, 2), (0, 2, 1))
UNIT_SHIFT = {2: 0, 3: -1, 4: 1, 5: 2}
AG_ORDER = ((0, 1, 2), (1, 2, 0), (2, 0, 1))


ROWS = 1024
WIDE = 4096
TILE = 256
COLS = 512
LANES = 128
STEPS = ROWS // TILE
PIECE = 131072
CHUNK = 4 * PIECE
CHUNKS = 2 * ROWS * WIDE // CHUNK
SLOTS = 4
PITCH = 40
GELU_A = math.sqrt(2.0 / math.pi)
GELU_B = GELU_A * 0.044715
BF16 = jnp.bfloat16
F32 = jnp.float32


def upto(n):
    return pl.ds(0, n)


def divide(t):
    return t // 4, lax.rem(t, 4)


def wrap(k):
    return lax.rem(k + 4, 4)


def rs_split():
    table = {}
    for s in range(SUBS):
        sizes = [11, 11, 11]
        sizes[(s + 2) % 3] = 10
        start = 32 * s
        for c in AXES:
            n = sizes[c]
            first = (n + (s + c) % 2) // 2
            table[s, c] = tuple(8 * k for k in (start, first, n - first))
            start += n
    return table


def coords_of(me):
    return [me // 16, lax.rem(me // 4, 4), lax.rem(me, 4)]


def peer(coords, pos, delta):
    moved = list(coords)
    moved[pos] = wrap(coords[pos] + delta)
    z, y, x = moved
    return z * 16 + y * 4 + x


def greet(coords, deltas, partner):
    barrier = pltpu.get_barrier_semaphore()
    ids = [{"data": peer(coords, pos, delta)} for pos in AXES for delta in deltas]
    if partner:
        ids.append({"stage": 1 - lax.axis_index("stage")})
    for other in ids:
        pl.semaphore_signal(barrier, inc=1, device_id=other, device_id_type=MESH)
    pl.semaphore_wait(barrier, len(ids))


def sum_everywhere(coords, acc, got, ssem, rsem):
    copies = []
    for ph in range(4):
        if ph < 3:
            mine = coords[ph]
            targets = [{"data": peer(coords, ph, k)} for k in range(1, 4)]
        else:
            mine = lax.axis_index("stage")
            targets = [{"stage": 1 - mine}]
        batch = []
        for k, target in enumerate(targets):
            i = ph * 3 + k
            batch.append(pltpu.make_async_remote_copy(src_ref=acc.at[ph], dst_ref=got.at[ph, mine], send_sem=ssem.at[i],
                                                      recv_sem=rsem.at[i], device_id=target, device_id_type=MESH))
        for copy in batch:
            copy.start()
        got[ph, mine] = acc[ph]
        for copy in batch:
            copy.wait_recv()
        acc[ph + 1] = sum(got[ph, k] for k in range(len(batch) + 1))
        copies += batch
    for copy in copies:
        copy.wait_send()


def rs_kernel(x_ref, du_ref, a_ref, top_ref, loss_ref, out_ref, total_ref, g_ref, ra1, rb1, lb, own, ra2, rb2, ra3, rb3, ssem, rsem, lsem,
              acc, got, tsem, usem, xb, gb, dub, ab, put1, put2, insem, dusem, asem, psem1, psem2):
    coords = coords_of(lax.axis_index("data"))
    table = rs_split()
    ra = (ra1, ra2, ra3)
    rb = (rb1, rb2, rb3)
    copies = {}

    load_x = pltpu.make_async_copy(x_ref, xb, insem.at[0])
    load_g = pltpu.make_async_copy(top_ref, gb, insem.at[1])

    def load_du(s):
        return pltpu.make_async_copy(du_ref.at[:, pl.ds(s * ROWS, ROWS)], dub.at[s % 2], dusem.at[s % 2])

    def load_a(m):
        return pltpu.make_async_copy(a_ref.at[:, pl.ds(pl.multiple_of(m * COLS, COLS), COLS)], ab.at[lax.rem(m, 2)], asem.at[lax.rem(m, 2)])

    def grads(s):
        band = pl.ds(s * SUB_ROWS, SUB_ROWS)
        load_a(0).start()
        if s + 1 < SUBS:
            load_du(s + 1).start()
        load_du(s).wait()
        if s == 0:
            load_x.wait()
            load_g.wait()

        def write1(m):
            return pltpu.make_async_copy(put1.at[lax.rem(m, 2)], g_ref.at[m // 2, pl.ds(lax.rem(m, 2) * 2, 2), :, band, :],
                                         psem1.at[lax.rem(m, 2)])

        def write2(m):
            return pltpu.make_async_copy(put2.at[lax.rem(m, 2)], g_ref.at[m // 4 + 2, lax.rem(m, 4), :, band, :],
                                         psem2.at[lax.rem(m, 2)])

        def first(m, carry):
            val = dot32(xb[:, pl.ds(pl.multiple_of(m * TILE, TILE), TILE)], dub[s % 2], ROWWISE)

            @pl.when(m > 1)
            def _():
                write1(m - 2).wait()

            for ct in range(ROWS // LANES):
                put1[lax.rem(m, 2), :, :, ct * 32:(ct + 1) * 32, :] = val[:, ct * LANES:(ct + 1) * LANES].reshape(2, 4, 32, LANES)
            write1(m).start()
            return carry

        def second(m, carry):
            load_a(m).wait()

            @pl.when(m < 7)
            def _():
                load_a(m + 1).start()

            val = dot32(ab[lax.rem(m, 2)], gb[:, band], ROWWISE)

            @pl.when(m > 1)
            def _():
                write2(m - 2).wait()

            for ct in BOTH:
                part = slice(ct * LANES, (ct + 1) * LANES)
                put2[lax.rem(m, 2), :, part, :] = val[:, part].reshape(4, LANES, LANES)
            write2(m).start()
            return carry

        lax.fori_loop(0, 4, first, 0)
        lax.fori_loop(0, 8, second, 0)
        for m in BOTH:
            write1(m + 2).wait()
            write2(m + 6).wait()

    def rows(s, c, half):
        start, n0, n1 = table[s, c]
        if half == 0:
            return 0, n0
        if half == 1:
            return n0, n1
        return 0, n0 + n1

    def lead(ph, c, k):
        order = RS_ORDER[c]
        left = [p for p in AXES if p != order[0]]
        idx = []
        for p in left:
            if ph == 1:
                idx.append(k if p == order[1] else RING)
            else:
                idx.append(coords[order[1]] if p == order[1] else k)
        return tuple(idx)

    def lead_t(ph, c, k, t):
        if ph == 0:
            return divide(t), divide(t)
        mine = tuple(t if i is RING else i for i in lead(ph, c, k))
        return (t,) * (2 - ph), mine

    def source(ph, s, c, k, half):
        lo, n = rows(s, c, half)
        if ph == 0:
            idx = [RING] * 3
            idx[RS_ORDER[c][0]] = k
            return g_ref.at[tuple(idx) + (pl.ds(table[s, c][0] + lo, n), ALL)]
        return own.at[(s * 3 + c,) + lead(ph, c, k) + (pl.ds(lo, n), ALL)]

    def slot(ref, ph, i, lo, n):
        return ref.at[(i,) + (RING,) * (2 - ph) + (pl.ds(lo, n), ALL)]

    def start(ph, s, c, d, piece, src, dst):
        i = (((ph * SUBS + s) * 3 + c) * 2 + d) * 3 + piece
        target = peer(coords, RS_ORDER[c][ph], DELTAS[d])
        copy = pltpu.make_async_remote_copy(src_ref=src, dst_ref=dst, send_sem=ssem.at[i], recv_sem=rsem.at[i],
                                            device_id={"data": target}, device_id_type=MESH)
        copy.start()
        copies[ph, s, c, d, piece] = copy

    def at(c, ph, delta):
        return wrap(coords[RS_ORDER[c][ph]] + delta)

    def send_a(ph, s, c):
        for d in BOTH:
            n = rows(s, c, d)[1]
            start(ph, s, c, d, 0, source(ph, s, c, at(c, ph, 2), d), slot(ra[ph], ph, s * 6 + c * 2 + d, 0, n))

    def send_b1(ph, s, c):
        for d in BOTH:
            lo, n = rows(s, c, 1 - d)
            start(ph, s, c, d, 1, source(ph, s, c, at(c, ph, DELTAS[d]), 1 - d), slot(rb[ph], ph, s * 6 + c * 2 + d, lo, n))

    def load(s, c):
        for d in BOTH:
            i = s * 9 + c * 3 + d
            n = rows(s, c, d)[1]
            copy = pltpu.make_async_copy(source(0, s, c, at(c, 0, DELTAS[d]), d), slot(lb, 0, s % 2 * 6 + c * 2 + d, 0, n), lsem.at[i])
            copy.start()
            copies["lb", s, c, d] = copy
        n = rows(s, c, 2)[1]
        copy = pltpu.make_async_copy(source(0, s, c, at(c, 0, 0), 2), slot(own, 0, s * 3 + c, 0, n), lsem.at[s * 9 + c * 3 + 2])
        copy.start()
        copies["own", s, c] = copy

    def forward(ph, s, c):
        for d in BOTH:
            i = s * 6 + c * 2 + d
            lo, n = rows(s, c, d)
            if ph == 0:
                copies["lb", s, c, d].wait()
            copies[ph, s, c, d, 0].wait_recv()
            buf = ra[ph]
            k = at(c, ph, DELTAS[d])

            def body(t, carry, d=d, i=i, n=n, lo=lo, buf=buf, k=k):
                where, mine = lead_t(ph, c, k, t)
                term = lb[(s % 2 * 6 + c * 2 + d,) + where + (upto(n), ALL)] if ph == 0 else own[(s * 3 + c,) + mine + (pl.ds(lo, n), ALL)]
                buf[(i,) + where + (upto(n), ALL)] += term
                return carry

            lax.fori_loop(0, LEADS[ph], body, 0)
            start(ph, s, c, d, 2, slot(buf, ph, i, 0, n), slot(rb[ph], ph, i, lo, n))

    def finish(ph, s, c):
        if ph == 0:
            copies["own", s, c].wait()
        for d in BOTH:
            copies[ph, s, c, d, 1].wait_recv()
            copies[ph, s, c, d, 2].wait_recv()
        n = rows(s, c, 2)[1]
        i, j = s * 6 + c * 2, s * 3 + c
        buf = rb[ph]
        k = at(c, ph, 0)
        span = upto(n)

        def body(t, carry):
            where, mine = lead_t(ph, c, k, t)
            mine = (j,) + mine + (span, ALL)
            total = own[mine] + buf[(i,) + where + (span, ALL)] + buf[(i + 1,) + where + (span, ALL)]
            if ph < 2:
                own[mine] = total
            else:
                out_ref[pl.ds(table[s, c][0], n), :] = total
            return carry

        lax.fori_loop(0, LEADS[ph], body, 0)

    def st0(s):
        for c in AXES:
            send_a(0, s, c)
            load(s, c)

    def st0b(s):
        for c in AXES:
            send_b1(0, s, c)

    def mid(ph, s):
        for c in AXES:
            forward(ph, s, c)

    def turn(ph, s):
        for c in AXES:
            finish(ph, s, c)
            if ph < 2:
                send_a(ph + 1, s, c)
                send_b1(ph + 1, s, c)

    def opening(s):
        if s < SUBS:
            grads(s)
            st0(s)

    def second(s):
        if s < SUBS:
            st0b(s)

    steps = []
    for s in range(SUBS):
        done = 3 * s + 4
        steps.append((max(s, 3 * s - 1), 0, mid, 0, s))
        for ph in AXES:
            steps.append((done + 4 * ph, 1, turn, ph, s))
            if ph:
                steps.append((done + 4 * ph - 2, 1, mid, ph, s))
    load_x.start()
    load_du(0).start()
    load_g.start()
    greet(coords, range(1, 4), True)
    opening(0)
    second(0)
    opening(1)
    for _, _, act, ph, s in sorted(steps, key=lambda e: e[:2]):
        act(ph, s)
        if act is mid and ph == 0:
            second(s + 1)
            opening(s + 2)
    for key, copy in copies.items():
        if not isinstance(key[0], str):
            copy.wait_send()
    part = out_ref[...]
    acc[0, 0] = jnp.sum((part * part).reshape(-1, 8, 128), axis=0)
    acc[0, 1] = loss_ref[...]
    sum_everywhere(coords, acc, got, tsem, usem)
    total_ref[...] = acc[4]


def reduce_scatter(x, du, a, g, loss):
    sems = 54 * SUBS
    f32 = jnp.float32
    dma = pltpu.SemaphoreType.DMA
    vmem = pl.BlockSpec(memory_space=pltpu.VMEM)
    anywhere = pl.BlockSpec(memory_space=pl.ANY)

    def slots(n, axes, rows, subs=SUBS):
        return pltpu.VMEM((subs * n,) + (4,) * axes + (rows, LANES), f32)

    part, totals, _ = pl.pallas_call(
        rs_kernel,
        out_shape=(jax.ShapeDtypeStruct((ROWS, LANES), f32), jax.ShapeDtypeStruct((2, 8, LANES), f32),
                   jax.ShapeDtypeStruct((4, 4, 4, ROWS, LANES), f32)),
        in_specs=[anywhere] * 4 + [vmem],
        out_specs=(vmem, vmem, anywhere),
        scratch_shapes=[slots(6, 2, 48), slots(6, 2, 88), slots(6, 2, 48, 2), slots(3, 2, 88), slots(6, 1, 48), slots(6, 1, 88),
                        slots(6, 0, 48), slots(6, 0, 88), dma((sems,)), dma((sems,)), dma((SUBS * 9,)),
                        pltpu.VMEM((5, 2, 8, LANES), f32), pltpu.VMEM((4, 4, 2, 8, LANES), f32), dma((10,)), dma((10,)),
                        pltpu.VMEM((ROWS, ROWS), BF16), pltpu.VMEM((ROWS, ROWS), BF16), pltpu.VMEM((2, ROWS, ROWS), BF16),
                        pltpu.VMEM((2, ROWS, COLS), BF16), pltpu.VMEM((2, 2, 4, SUB_ROWS, LANES), f32),
                        pltpu.VMEM((2, 4, SUB_ROWS, LANES), f32), dma((2,)), dma((2,)), dma((2,)), dma((2,)), dma((2,))],
        compiler_params=pltpu.CompilerParams(collective_id=0, has_side_effects=True, vmem_limit_bytes=63 * MIB),
        name="grad_rs",
    )(x, du, a, g, loss)
    return part, totals


def ag_split():
    table = []
    start = 0
    for c, n in enumerate((22, 21, 21)):
        first = (n + c % 2) // 2
        table.append(tuple(16 * k for k in (start, first, n - first)))
        start += n
    return table


def ag_kernel(w_ref, wide_ref, out_ref, stage, ssem, rsem, lsem):
    coords = coords_of(lax.axis_index("data"))
    table = ag_split()
    copies = {}

    def rows(c, half):
        start, n0, n1 = table[c]
        return (start, n0) if half == 0 else (start + n0, n1)

    def region(c, unit, shift, half):
        first, second, third = AG_ORDER[c]
        idx = [None] * 3
        if unit == 0:
            idx[first], idx[second], idx[third] = wrap(coords[first] + shift), coords[second], coords[third]
        elif unit == 1:
            idx[first], idx[second], idx[third] = RING, wrap(coords[second] + shift), coords[third]
        else:
            q = wrap(coords[second] + UNIT_SHIFT[unit])
            idx[first], idx[second], idx[third] = RING, q, wrap(coords[third] + shift)
        lo, n = rows(c, half)
        return out_ref.at[tuple(idx) + (pl.ds(lo, n), ALL)]

    def start(c, unit, d, piece, src, dst):
        i = ((unit * 3 + c) * 2 + d) * 3 + piece
        target = peer(coords, AG_ORDER[c][min(unit, 2)], DELTAS[d])
        copy = pltpu.make_async_remote_copy(src_ref=src, dst_ref=dst, send_sem=ssem.at[i], recv_sem=rsem.at[i],
                                            device_id={"data": target}, device_id_type=MESH)
        copy.start()
        copies[c, unit, d, piece] = copy

    def begin(unit):
        for c in AXES:
            for d in BOTH:
                for piece, half in ((0, d), (1, 1 - d)):
                    lo, n = rows(c, half)
                    here = region(c, unit, 0, half)
                    src = w_ref.at[pl.ds(lo, n), :] if unit == 0 else here
                    start(c, unit, d, piece, src, here)

    def middle(unit):
        for c in AXES:
            for d in BOTH:
                copies[c, unit, d, 0].wait_recv()
                part = region(c, unit, -DELTAS[d], d)
                start(c, unit, d, 2, part, part)

    def arrive(unit, piece):
        for c in AXES:
            for d in BOTH:
                copies[c, unit, d, piece].wait_recv()

    flights = []

    def widen(unit):
        for c in AXES:
            start, n0, n1 = table[c]
            n = n0 + n1
            second = AG_ORDER[c][1]
            q = wrap(coords[second] + UNIT_SHIFT[unit])
            i = len(flights)
            if i > 1:
                flights[i - 2].wait()

            def body(t, carry):
                u, v = divide(t)
                where = [u, v]
                where.insert(second, q)
                stage[i % 2, u, v, upto(n), :] = out_ref[tuple(where) + (pl.ds(start, n), ALL)].astype(jnp.float32)
                return carry

            lax.fori_loop(0, 16, body, 0)
            where = [RING] * 2
            where.insert(second, q)
            flights.append(pltpu.make_async_copy(stage.at[i % 2, :, :, upto(n), :],
                                                 wide_ref.at[tuple(where) + (pl.ds(start, n), ALL)], lsem.at[i]))
            flights[i].start()

    greet(coords, DELTAS, False)
    begin(0)
    out_ref[tuple(coords)] = w_ref[...]
    middle(0)
    arrive(0, 1)
    arrive(0, 2)
    begin(1)
    begin(2)
    middle(1)
    arrive(1, 1)
    begin(3)
    begin(4)
    middle(2)
    arrive(1, 2)
    begin(5)
    middle(3)
    middle(4)
    middle(5)
    for unit in UNIT_SHIFT:
        arrive(unit, 1)
        arrive(unit, 2)
        widen(unit)
    for flight in flights[-2:]:
        flight.wait()
    for copy in copies.values():
        copy.wait_send()


def all_gather_rows(w):
    dma = pltpu.SemaphoreType.DMA
    sems = 36 * 3
    return pl.pallas_call(
        ag_kernel,
        out_shape=jax.ShapeDtypeStruct((4, 4, 4, 1024, 128), jnp.float32),
        in_specs=[pl.BlockSpec(memory_space=pltpu.VMEM)],
        out_specs=pl.BlockSpec(memory_space=pl.ANY),
        scratch_shapes=[pltpu.VMEM((4, 4, 4, 1024, 128), w.dtype), pltpu.VMEM((2, 4, 4, 352, 128), jnp.float32),
                        dma((sems,)), dma((sems,)), dma((12,))],
        compiler_params=pltpu.CompilerParams(collective_id=1, has_side_effects=True, vmem_limit_bytes=40 * MIB),
        name="weight_ag",
    )(w)


def dot32(a, b, dims=((1,), (0,))):
    return lax.dot_general(a, b, (dims, ((), ())), preferred_element_type=F32)


def dot_t(a, b):
    return dot32(a, b, ((1,), (1,)))


def block_kernel(scale, w_ref, xin_ref, t_ref, x_out, a_out, du_out, g_out, loss_ref,
                 w1, w2, xb, hb, gb, ab, db, tb, raw, wide, wsem, insem, outsem, hs, hr, gs, gr):
    stage = lax.axis_index("stage")
    first = stage == 0
    last = stage == 1
    other = {"stage": 1 - stage}

    def chunk(i):
        return pltpu.make_async_copy(w_ref.at[:, pl.ds(pl.multiple_of(i * CHUNK, CHUNK), CHUNK)], raw.at[lax.rem(i, SLOTS)],
                                     wsem.at[lax.rem(i, SLOTS)])

    load_x = pltpu.make_async_copy(xin_ref, xb, insem.at[0])
    load_t = pltpu.make_async_copy(t_ref, tb, insem.at[1])

    def prefetch(i, carry):
        chunk(i).start()
        return carry

    lax.fori_loop(0, SLOTS, prefetch, 0)

    @pl.when(first)
    def _():
        load_x.start()

    @pl.when(last)
    def _():
        load_t.start()

    barrier = pltpu.get_barrier_semaphore()
    pl.semaphore_signal(barrier, inc=1, device_id=other, device_id_type=MESH)
    pl.semaphore_wait(barrier, 1)

    def convert(i, weight, blocks, pitch):
        rows = PIECE // (blocks * LANES)
        chunk(i).wait()

        def body(q, carry):
            for j in range(PIECE // ROWS):
                line = raw[lax.rem(i, SLOTS), :, pl.ds(pl.multiple_of(q * PIECE + j * ROWS, ROWS), ROWS)]
                at = (j * 8 // blocks) * pitch + j * 8 % blocks
                wide[at:at + 8, :] = line.astype(F32).reshape(8, LANES)
            base = pl.ds(pl.multiple_of((lax.rem(i, CHUNKS // 2) * 4 + q) * rows, rows), rows)
            for cb in range(blocks):
                weight[base, cb * LANES:(cb + 1) * LANES] = wide[pl.ds(cb, rows, stride=pitch), :].astype(BF16)
            return carry

        lax.fori_loop(0, 4, body, 0)

        @pl.when(i < CHUNKS - SLOTS)
        def _():
            chunk(i + SLOTS).start()

    def convert_first(i, carry):
        convert(i, w1, WIDE // LANES, PITCH)
        return carry

    def convert_second(i, carry):
        convert(i, w2, ROWS // LANES, ROWS // LANES)
        return carry

    lax.fori_loop(0, CHUNKS // 2, convert_first, 0)
    lax.fori_loop(CHUNKS // 2, CHUNKS, convert_second, 0)

    @pl.when(first)
    def _():
        load_x.wait()

    @pl.when(last)
    def _():
        load_t.wait()

    def span(i):
        return pl.ds(pl.multiple_of(i * TILE, TILE), TILE)

    def cols(j):
        return pl.ds(pl.multiple_of(j * COLS, COLS), COLS)

    def send_h(i):
        return pltpu.make_async_remote_copy(src_ref=hb.at[span(i)], dst_ref=xb.at[span(i)], send_sem=hs.at[i], recv_sem=hr.at[i],
                                            device_id=other, device_id_type=MESH)

    def send_g(i):
        return pltpu.make_async_remote_copy(src_ref=hb.at[span(i)], dst_ref=gb.at[span(i)], send_sem=gs.at[i], recv_sem=gr.at[i],
                                            device_id=other, device_id_type=MESH)

    def outputs(i):
        pairs = ((xb, x_out), (ab, a_out), (db, du_out), (gb, g_out))
        return [pltpu.make_async_copy(src.at[span(i)], dst.at[span(i)], outsem.at[i * 4 + k]) for k, (src, dst) in enumerate(pairs)]

    def forward(i):
        def up(j, carry):
            u = dot32(xb[span(i), :], w1[:, cols(j)]).astype(BF16)
            db[span(i), cols(j)] = u
            uf = u.astype(F32)
            half = 0.5 * uf
            ab[span(i), cols(j)] = (half + half * jnp.tanh(uf * (GELU_A + GELU_B * (uf * uf)))).astype(BF16)
            return carry

        def down(j, carry):
            hb[span(i), cols(j)] = (xb[span(i), cols(j)].astype(F32) + dot32(ab[span(i), :], w2[:, cols(j)])).astype(BF16)
            return carry

        lax.fori_loop(0, WIDE // COLS, up, 0, unroll=2)
        lax.fori_loop(0, ROWS // COLS, down, 0)

    def top(i):
        res = hb[span(i), :].astype(F32) - tb[span(i), :].astype(F32)
        gb[span(i), :] = (res * scale).astype(BF16)
        sums = jnp.sum((res * res).reshape(-1, 8, ROWS), axis=0)
        loss_ref[...] += sum(sums[:, k * LANES:(k + 1) * LANES] for k in range(ROWS // LANES))

    def backward(i):
        def body(j, carry):
            e = dot_t(gb[span(i), :], w2[cols(j), :])
            u = db[span(i), cols(j)].astype(F32)
            sq = u * u
            gate = 0.5 + 0.5 * jnp.tanh(u * (GELU_A + GELU_B * sq))
            slope = gate + gate * ((1.0 - gate) * (u * (2.0 * GELU_A + (6.0 * GELU_B) * sq)))
            db[span(i), cols(j)] = (e * slope).astype(BF16)
            return carry

        lax.fori_loop(0, WIDE // COLS, body, 0, unroll=2)

    def below(i):
        def body(j, carry):
            hb[span(i), cols(j)] = (gb[span(i), cols(j)].astype(F32) + dot_t(db[span(i), :], w1[cols(j), :])).astype(BF16)
            return carry

        lax.fori_loop(0, ROWS // COLS, body, 0)

    loss_ref[...] = jnp.zeros_like(loss_ref)

    def tick(it, carry):
        i = lax.rem(it, STEPS)

        @pl.when(it < STEPS)
        def _():
            @pl.when(last)
            def _():
                send_h(i).wait_recv()

            forward(i)

            @pl.when(first)
            def _():
                send_h(i).start()

            @pl.when(last)
            def _():
                top(i)

        @pl.when(it // STEPS + stage == 1)
        def _():
            @pl.when(first)
            def _():
                send_g(i).wait_recv()

            backward(i)

            @pl.when(last)
            def _():
                below(i)
                send_g(i).start()

            for copy in outputs(i):
                copy.start()
        return carry

    lax.fori_loop(0, 2 * STEPS, tick, 0)

    def drain(i, carry):
        @pl.when(first)
        def _():
            send_h(i).wait_send()

        @pl.when(last)
        def _():
            send_g(i).wait_send()

        for copy in outputs(i):
            copy.wait()
        return carry

    lax.fori_loop(0, STEPS, drain, 0)


def block_passes(flat, x_in, targets, token_count):
    anywhere = pl.BlockSpec(memory_space=pl.ANY)
    dma = pltpu.SemaphoreType.DMA
    narrow, wide = (ROWS, ROWS), (ROWS, WIDE)

    def shape(dims):
        return jax.ShapeDtypeStruct(dims, BF16)

    def room(dims):
        return pltpu.VMEM(dims, BF16)

    return pl.pallas_call(
        functools.partial(block_kernel, 1.0 / token_count),
        out_shape=(shape(narrow), shape(wide), shape(wide), shape(narrow), jax.ShapeDtypeStruct((8, LANES), F32)),
        in_specs=[anywhere] * 3,
        out_specs=(anywhere,) * 4 + (pl.BlockSpec(memory_space=pltpu.VMEM),),
        scratch_shapes=[room(wide), room((WIDE, ROWS)), room(narrow), room(narrow), room(narrow), room(wide), room(wide), room(narrow),
                        room((SLOTS, 1, CHUNK)), pltpu.VMEM((32 * PITCH, LANES), F32),
                        dma((SLOTS,)), dma((2,)), dma((STEPS * 4,)), dma((STEPS,)), dma((STEPS,)), dma((STEPS,)), dma((STEPS,))],
        compiler_params=pltpu.CompilerParams(collective_id=2, has_side_effects=True, vmem_limit_bytes=60 * MIB),
        name="block",
    )(flat, x_in, targets)


def adam_kernel(rate, token_count, part_ref, total_ref, tau_ref, w_ref, m_ref, v_ref, w_out, m_out, v_out, b_out, loss_out, grad):
    early = lax.axis_index("data") < 32

    def reorder(rows):
        blocks = ROWS // rows
        for r in range(rows):
            grad[r * blocks:(r + 1) * blocks, :] = part_ref[pl.ds(r, blocks, stride=rows), :]

    @pl.when(early)
    def _():
        reorder(32)

    @pl.when(jnp.logical_not(early))
    def _():
        reorder(LANES)

    nu = jnp.sqrt(jnp.sum(total_ref[0], keepdims=True))
    scaled = jnp.minimum(1.0, tau_ref[...] / nu) * grad[...]
    m_new = ADAM_BETA1 * m_ref[...] + (1.0 - ADAM_BETA1) * scaled
    v_new = ADAM_BETA2 * v_ref[...] + (1.0 - ADAM_BETA2) * scaled * scaled
    m_hat = m_new / (1.0 - ADAM_BETA1 ** ADAM_STEP)
    v_hat = v_new / (1.0 - ADAM_BETA2 ** ADAM_STEP)
    w_new = w_ref[...] - rate * (m_hat / (jnp.sqrt(v_hat) + ADAM_EPS) + WEIGHT_DECAY * w_ref[...])
    w_out[...] = w_new
    m_out[...] = m_new
    v_out[...] = v_new
    b_out[...] = w_new.astype(BF16)
    loss_out[...] = (0.5 * jnp.sum(total_ref[1], keepdims=True)) / token_count


def adam(rate, token_count, part, totals, tau, w, m, v):
    state = jax.ShapeDtypeStruct(part.shape, F32)
    vmem = pl.BlockSpec(memory_space=pltpu.VMEM)
    return pl.pallas_call(
        functools.partial(adam_kernel, rate, token_count),
        out_shape=(state, state, state, jax.ShapeDtypeStruct(part.shape, BF16), jax.ShapeDtypeStruct((1, 1), F32)),
        in_specs=[vmem] * 6,
        out_specs=(vmem,) * 5,
        scratch_shapes=[pltpu.VMEM(part.shape, F32)],
        name="adam",
    )(part, totals, tau, w, m, v)


def solution(mesh):
    data_size = mesh.shape['data']

    def device_step(x_in, targets, w_work, w_master, m_prior, v_prior, clip_tau):
        token_count = x_in.shape[0] * x_in.shape[1] * data_size
        x, a, du, g, loss = block_passes(w_work.reshape(1, -1), x_in.reshape(ROWS, ROWS), targets.reshape(ROWS, ROWS), token_count)
        part, totals = reduce_scatter(x, du, a, g, loss)
        rate = LR_BASE / math.sqrt(x_in.shape[-1])
        state = [z.reshape(ROWS, LANES) for z in (w_master, m_prior, v_prior)]
        w_new, m_new, v_new, w_bf, loss_mean = adam(rate, token_count, part, totals, clip_tau.reshape(1, 1), *state)
        w_all = lax.optimization_barrier(all_gather_rows(w_bf).reshape(w_work.shape)).astype(BF16)
        return (loss_mean.reshape(()), w_all) + tuple(z.reshape(w_master.shape) for z in (w_new, m_new, v_new))

    row_spec = P(None, 'data', None)
    shard_spec = P('stage', None, 'data')
    stage_spec = P('stage', None, None)
    return jax.shard_map(device_step, mesh=mesh, in_specs=(row_spec, row_spec, stage_spec, shard_spec, shard_spec, shard_spec, P()), out_specs=(P(), stage_spec, shard_spec, shard_spec, shard_spec), check_vma=False)
```

```python
import functools
import math
import jax
import jax.numpy as jnp
from jax import lax
from jax.experimental import pallas as pl
from jax.experimental.pallas import tpu as pltpu
from jax.sharding import PartitionSpec as P

ADAM_BETA1 = 0.9
ADAM_BETA2 = 0.95
ADAM_EPS = 1e-8
WEIGHT_DECAY = 0.1
ADAM_STEP = 10
LR_BASE = 0.05
MESH = pl.DeviceIdType.MESH
MIB = 1024 * 1024

UNITS = (1, 2, 2, 2, 1)
SUBS = len(UNITS)
ALL = slice(None)
RING = pl.ds(0, 4)
BOTH = range(2)
AXES = range(3)
LEADS = (16, 4, 1)
ROWWISE = ((0,), (0,))
DELTAS = (1, -1)
RS_ORDER = ((2, 1, 0), (1, 0, 2), (0, 2, 1))
UNIT_SHIFT = {2: 0, 3: -1, 4: 1, 5: 2}
AG_ORDER = ((0, 1, 2), (1, 2, 0), (2, 0, 1))


ROWS = 1024
WIDE = 4096
TILE = 256
COLS = 512
LANES = 128
STEPS = ROWS // TILE
PIECE = 131072
CHUNKS = 2 * ROWS * WIDE // PIECE
SLOTS = 16
PITCH = 40
GELU_A = math.sqrt(2.0 / math.pi)
GELU_B = GELU_A * 0.044715
BF16 = jnp.bfloat16
F32 = jnp.float32


def upto(n):
    return pl.ds(0, n)


def divide(t):
    return t // 4, lax.rem(t, 4)


def wrap(k):
    return lax.rem(k + 4, 4)


def rs_split():
    table, half_at, full_at = {}, [0], [0]
    start = 0
    for s, units in enumerate(UNITS):
        most = 0
        for c in AXES:
            n = (16 * units + (c + s) % 3) // 3
            first = (n + (s + c) % 2) // 2
            table[s, c] = tuple(8 * k for k in (start, first, n - first))
            start += n
            most = max(most, n)
        half_at.append(half_at[s] + (most + 1) // 2 * 8)
        full_at.append(full_at[s] + most * 8)
    return table, half_at, full_at


def coords_of(me):
    return [me // 16, lax.rem(me // 4, 4), lax.rem(me, 4)]


def peer(coords, pos, delta):
    moved = list(coords)
    moved[pos] = wrap(coords[pos] + delta)
    z, y, x = moved
    return z * 16 + y * 4 + x


def greet(coords, deltas, partner):
    barrier = pltpu.get_barrier_semaphore()
    ids = [{"data": peer(coords, pos, delta)} for pos in AXES for delta in deltas]
    if partner:
        ids.append({"stage": 1 - lax.axis_index("stage")})
    for other in ids:
        pl.semaphore_signal(barrier, inc=1, device_id=other, device_id_type=MESH)
    pl.semaphore_wait(barrier, len(ids))


def sum_everywhere(coords, acc, got, ssem, rsem):
    copies = []
    for ph in range(4):
        if ph < 3:
            mine = coords[ph]
            targets = [{"data": peer(coords, ph, k)} for k in range(1, 4)]
        else:
            mine = lax.axis_index("stage")
            targets = [{"stage": 1 - mine}]
        batch = []
        for k, target in enumerate(targets):
            i = ph * 3 + k
            batch.append(pltpu.make_async_remote_copy(src_ref=acc.at[ph], dst_ref=got.at[ph, mine], send_sem=ssem.at[i],
                                                      recv_sem=rsem.at[i], device_id=target, device_id_type=MESH))
        for copy in batch:
            copy.start()
        got[ph, mine] = acc[ph]
        for copy in batch:
            copy.wait_recv()
        acc[ph + 1] = sum(got[ph, k] for k in range(len(batch) + 1))
        copies += batch
    for copy in copies:
        copy.wait_send()


def rs_kernel(x_ref, du_ref, a_ref, top_ref, loss_ref, out_ref, total_ref, g_ref, ra1, rb1, lb, own, ra2, rb2, ra3, rb3, ssem, rsem, lsem,
              acc, got, tsem, usem, xb, gb, dub, ab, put1, put2, insem, dusem, asem, psem1, psem2):
    coords = coords_of(lax.axis_index("data"))
    table, half_at, full_at = rs_split()
    ra = (ra1, ra2, ra3)
    rb = (rb1, rb2, rb3)
    copies = {}

    load_x = pltpu.make_async_copy(x_ref, xb, insem.at[0])
    load_g = pltpu.make_async_copy(top_ref, gb, insem.at[1])

    def load_du(s):
        width = UNITS[s] * COLS
        return pltpu.make_async_copy(du_ref.at[:, pl.ds(sum(UNITS[:s]) * COLS, width)], dub.at[s % 2, :, upto(width)], dusem.at[s % 2])

    def load_a(m):
        return pltpu.make_async_copy(a_ref.at[:, pl.ds(pl.multiple_of(m * COLS, COLS), COLS)], ab.at[lax.rem(m, 2)], asem.at[lax.rem(m, 2)])

    def grads(s):
        size = UNITS[s] * LANES
        band = pl.ds(sum(UNITS[:s]) * LANES, size)
        width = UNITS[s] * COLS
        load_a(0).start()
        if s + 1 < SUBS:
            load_du(s + 1).start()
        load_du(s).wait()
        if s == 0:
            load_x.wait()
            load_g.wait()

        def write1(m):
            return pltpu.make_async_copy(put1.at[lax.rem(m, 2), :, :, upto(size)], g_ref.at[m // 2, pl.ds(lax.rem(m, 2) * 2, 2), :, band, :],
                                         psem1.at[lax.rem(m, 2)])

        def write2(m):
            return pltpu.make_async_copy(put2.at[lax.rem(m, 2), :, upto(size)], g_ref.at[m // 4 + 2, lax.rem(m, 4), :, band, :],
                                         psem2.at[lax.rem(m, 2)])

        def first(m, carry):
            val = dot32(xb[:, pl.ds(pl.multiple_of(m * TILE, TILE), TILE)], dub[s % 2, :, upto(width)], ROWWISE)

            @pl.when(m > 1)
            def _():
                write1(m - 2).wait()

            for ct in range(width // LANES):
                put1[lax.rem(m, 2), :, :, ct * 32:(ct + 1) * 32, :] = val[:, ct * LANES:(ct + 1) * LANES].reshape(2, 4, 32, LANES)
            write1(m).start()
            return carry

        def second(m, carry):
            load_a(m).wait()

            @pl.when(m < 7)
            def _():
                load_a(m + 1).start()

            val = dot32(ab[lax.rem(m, 2)], gb[:, band], ROWWISE)

            @pl.when(m > 1)
            def _():
                write2(m - 2).wait()

            for ct in range(UNITS[s]):
                part = slice(ct * LANES, (ct + 1) * LANES)
                put2[lax.rem(m, 2), :, part, :] = val[:, part].reshape(4, LANES, LANES)
            write2(m).start()
            return carry

        lax.fori_loop(0, 4, first, 0)
        lax.fori_loop(0, 8, second, 0)
        for m in BOTH:
            write1(m + 2).wait()
            write2(m + 6).wait()

    def rows(s, c, half):
        start, n0, n1 = table[s, c]
        if half == 0:
            return 0, n0
        if half == 1:
            return n0, n1
        return 0, n0 + n1

    def lead(ph, c, k):
        order = RS_ORDER[c]
        left = [p for p in AXES if p != order[0]]
        idx = []
        for p in left:
            if ph == 1:
                idx.append(k if p == order[1] else RING)
            else:
                idx.append(coords[order[1]] if p == order[1] else k)
        return tuple(idx)

    def lead_t(ph, c, k, t):
        if ph == 0:
            return divide(t), divide(t)
        mine = tuple(t if i is RING else i for i in lead(ph, c, k))
        return (t,) * (2 - ph), mine

    def source(ph, s, c, k, half):
        lo, n = rows(s, c, half)
        if ph == 0:
            idx = [RING] * 3
            idx[RS_ORDER[c][0]] = k
            return g_ref.at[tuple(idx) + (pl.ds(table[s, c][0] + lo, n), ALL)]
        return own.at[(c,) + lead(ph, c, k) + (pl.ds(full_at[s] + lo, n), ALL)]

    def slot(ref, ph, i, lo, n):
        return ref.at[(i,) + (RING,) * (2 - ph) + (pl.ds(lo, n), ALL)]

    def start(ph, s, c, d, piece, src, dst):
        i = (((ph * SUBS + s) * 3 + c) * 2 + d) * 3 + piece
        target = peer(coords, RS_ORDER[c][ph], DELTAS[d])
        copy = pltpu.make_async_remote_copy(src_ref=src, dst_ref=dst, send_sem=ssem.at[i], recv_sem=rsem.at[i],
                                            device_id={"data": target}, device_id_type=MESH)
        copy.start()
        copies[ph, s, c, d, piece] = copy

    def at(c, ph, delta):
        return wrap(coords[RS_ORDER[c][ph]] + delta)

    def send_a(ph, s, c):
        for d in BOTH:
            n = rows(s, c, d)[1]
            start(ph, s, c, d, 0, source(ph, s, c, at(c, ph, 2), d), slot(ra[ph], ph, c * 2 + d, half_at[s], n))

    def send_b1(ph, s, c):
        for d in BOTH:
            lo, n = rows(s, c, 1 - d)
            start(ph, s, c, d, 1, source(ph, s, c, at(c, ph, DELTAS[d]), 1 - d), slot(rb[ph], ph, c * 2 + d, full_at[s] + lo, n))

    def load(s, c):
        for d in BOTH:
            i = s * 9 + c * 3 + d
            n = rows(s, c, d)[1]
            copy = pltpu.make_async_copy(source(0, s, c, at(c, 0, DELTAS[d]), d), slot(lb, 0, s % 2 * 6 + c * 2 + d, 0, n), lsem.at[i])
            copy.start()
            copies["lb", s, c, d] = copy
        n = rows(s, c, 2)[1]
        copy = pltpu.make_async_copy(source(0, s, c, at(c, 0, 0), 2), slot(own, 0, c, full_at[s], n), lsem.at[s * 9 + c * 3 + 2])
        copy.start()
        copies["own", s, c] = copy

    def forward(ph, s, c):
        for d in BOTH:
            i = c * 2 + d
            lo, n = rows(s, c, d)
            if ph == 0:
                copies["lb", s, c, d].wait()
            copies[ph, s, c, d, 0].wait_recv()
            buf = ra[ph]
            k = at(c, ph, DELTAS[d])

            def body(t, carry, d=d, i=i, n=n, lo=lo, buf=buf, k=k):
                where, mine = lead_t(ph, c, k, t)
                term = lb[(s % 2 * 6 + c * 2 + d,) + where + (upto(n), ALL)] if ph == 0 else own[(c,) + mine + (pl.ds(full_at[s] + lo, n), ALL)]
                buf[(i,) + where + (pl.ds(half_at[s], n), ALL)] += term
                return carry

            lax.fori_loop(0, LEADS[ph], body, 0)
            start(ph, s, c, d, 2, slot(buf, ph, i, half_at[s], n), slot(rb[ph], ph, i, full_at[s] + lo, n))

    def finish(ph, s, c):
        if ph == 0:
            copies["own", s, c].wait()
        for d in BOTH:
            copies[ph, s, c, d, 1].wait_recv()
            copies[ph, s, c, d, 2].wait_recv()
        n = rows(s, c, 2)[1]
        i = c * 2
        buf = rb[ph]
        k = at(c, ph, 0)
        span = pl.ds(full_at[s], n)

        def body(t, carry):
            where, mine = lead_t(ph, c, k, t)
            mine = (c,) + mine + (span, ALL)
            total = own[mine] + buf[(i,) + where + (span, ALL)] + buf[(i + 1,) + where + (span, ALL)]
            if ph < 2:
                own[mine] = total
            else:
                out_ref[pl.ds(table[s, c][0], n), :] = total
            return carry

        lax.fori_loop(0, LEADS[ph], body, 0)

    def st0(s):
        for c in AXES:
            send_a(0, s, c)
            load(s, c)

    def st0b(s):
        for c in AXES:
            send_b1(0, s, c)

    def mid(ph, s):
        for c in AXES:
            forward(ph, s, c)

    def turn(ph, s):
        for c in AXES:
            finish(ph, s, c)
            if ph < 2:
                send_a(ph + 1, s, c)
                send_b1(ph + 1, s, c)

    def opening(s):
        if s < SUBS:
            grads(s)
            st0(s)

    def second(s):
        if s < SUBS:
            st0b(s)

    queue = [(mid, 0), (None, 0), (mid, 1)]
    for s in range(SUBS):
        queue += [(turn, s), (None, s + 1), (mid, s + 2)]
    steps, clock = [], 0
    for act, s in queue:
        if s < SUBS:
            clock += UNITS[s]
            steps.append((clock, 0, act, 0, s))
            if act is turn:
                for ph in range(1, 3):
                    steps.append((clock + 3 * ph - 2, 1, mid, ph, s))
                    steps.append((clock + 3 * ph, 1, turn, ph, s))
    steps = [e for e in steps if e[2]]
    load_x.start()
    load_du(0).start()
    load_g.start()
    greet(coords, range(1, 4), True)
    opening(0)
    second(0)
    opening(1)
    for _, _, act, ph, s in sorted(steps, key=lambda e: e[:2]):
        act(ph, s)
        if act is mid and ph == 0:
            second(s + 1)
            opening(s + 2)
    for key, copy in copies.items():
        if not isinstance(key[0], str):
            copy.wait_send()
    part = out_ref[...]
    acc[0, 0] = jnp.sum((part * part).reshape(-1, 8, 128), axis=0)
    acc[0, 1] = loss_ref[...]
    sum_everywhere(coords, acc, got, tsem, usem)
    total_ref[...] = acc[4]


def reduce_scatter(x, du, a, g, loss):
    sems = 54 * SUBS
    f32 = jnp.float32
    dma = pltpu.SemaphoreType.DMA
    vmem = pl.BlockSpec(memory_space=pltpu.VMEM)
    anywhere = pl.BlockSpec(memory_space=pl.ANY)

    _, half_at, full_at = rs_split()

    def slots(n, axes, rows):
        return pltpu.VMEM((n,) + (4,) * axes + (rows, LANES), f32)

    def landing(axes):
        return [slots(6, axes, half_at[-1]), slots(6, axes, full_at[-1])]

    part, totals, _ = pl.pallas_call(
        rs_kernel,
        out_shape=(jax.ShapeDtypeStruct((ROWS, LANES), f32), jax.ShapeDtypeStruct((2, 8, LANES), f32),
                   jax.ShapeDtypeStruct((4, 4, 4, ROWS, LANES), f32)),
        in_specs=[anywhere] * 4 + [vmem],
        out_specs=(vmem, vmem, anywhere),
        scratch_shapes=[*landing(2), slots(12, 2, 48), slots(3, 2, full_at[-1]), *landing(1), *landing(0),
                        dma((sems,)), dma((sems,)), dma((SUBS * 9,)),
                        pltpu.VMEM((5, 2, 8, LANES), f32), pltpu.VMEM((4, 4, 2, 8, LANES), f32), dma((10,)), dma((10,)),
                        pltpu.VMEM((ROWS, ROWS), BF16), pltpu.VMEM((ROWS, ROWS), BF16), pltpu.VMEM((2, ROWS, ROWS), BF16),
                        pltpu.VMEM((2, ROWS, COLS), BF16), pltpu.VMEM((2, 2, 4, TILE, LANES), f32),
                        pltpu.VMEM((2, 4, TILE, LANES), f32), dma((2,)), dma((2,)), dma((2,)), dma((2,)), dma((2,))],
        compiler_params=pltpu.CompilerParams(collective_id=0, has_side_effects=True, vmem_limit_bytes=63 * MIB),
        name="grad_rs",
    )(x, du, a, g, loss)
    return part, totals


def ag_split():
    table = []
    start = 0
    for c, n in enumerate((22, 21, 21)):
        first = (n + c % 2) // 2
        table.append(tuple(16 * k for k in (start, first, n - first)))
        start += n
    return table


def ag_kernel(w_ref, wide_ref, out_ref, ssem, rsem):
    coords = coords_of(lax.axis_index("data"))
    table = ag_split()
    copies = {}

    def rows(c, half):
        start, n0, n1 = table[c]
        return (start, n0) if half == 0 else (start + n0, n1)

    def region(c, unit, shift, half):
        first, second, third = AG_ORDER[c]
        idx = [None] * 3
        if unit == 0:
            idx[first], idx[second], idx[third] = wrap(coords[first] + shift), coords[second], coords[third]
        elif unit == 1:
            idx[first], idx[second], idx[third] = RING, wrap(coords[second] + shift), coords[third]
        else:
            q = wrap(coords[second] + UNIT_SHIFT[unit])
            idx[first], idx[second], idx[third] = RING, q, wrap(coords[third] + shift)
        lo, n = rows(c, half)
        return out_ref.at[tuple(idx) + (pl.ds(lo, n), ALL)]

    def start(c, unit, d, piece, src, dst):
        i = ((unit * 3 + c) * 2 + d) * 3 + piece
        target = peer(coords, AG_ORDER[c][min(unit, 2)], DELTAS[d])
        copy = pltpu.make_async_remote_copy(src_ref=src, dst_ref=dst, send_sem=ssem.at[i], recv_sem=rsem.at[i],
                                            device_id={"data": target}, device_id_type=MESH)
        copy.start()
        copies[c, unit, d, piece] = copy

    def begin(unit):
        for c in AXES:
            for d in BOTH:
                for piece, half in ((0, d), (1, 1 - d)):
                    lo, n = rows(c, half)
                    here = region(c, unit, 0, half)
                    src = w_ref.at[pl.ds(lo, n), :] if unit == 0 else here
                    start(c, unit, d, piece, src, here)

    def middle(unit):
        for c in AXES:
            for d in BOTH:
                copies[c, unit, d, 0].wait_recv()
                part = region(c, unit, -DELTAS[d], d)
                start(c, unit, d, 2, part, part)

    def arrive(unit, piece):
        for c in AXES:
            for d in BOTH:
                copies[c, unit, d, piece].wait_recv()

    def pack(unit, *shifts):
        for shift in shifts:
            for c in AXES:
                start, n0, n1 = table[c]
                _, second, third = AG_ORDER[c]
                at = {second: wrap(coords[second] + UNIT_SHIFT[unit]), third: wrap(coords[third] + shift)}

                def body(t, carry, at=at, start=start, n=n0 + n1):
                    where = tuple(at.get(p, t) for p in AXES)
                    z, y, x = where
                    base = (z * 16 + y * 4 + x) * PIECE + start * LANES
                    for k in range(n // 16):
                        line = out_ref[where + (pl.ds(start + k * 16, 16), ALL)].astype(F32)
                        line = line.reshape(1, 2 * ROWS).astype(BF16)
                        wide_ref[:, pl.ds(pl.multiple_of(base + k * 2 * ROWS, 2 * ROWS), 2 * ROWS)] = line
                    return carry

                lax.fori_loop(0, 4, body, 0)

    greet(coords, DELTAS, False)
    begin(0)
    out_ref[tuple(coords)] = w_ref[...]
    middle(0)
    arrive(0, 1)
    arrive(0, 2)
    begin(1)
    begin(2)
    pack(2, 0)
    middle(1)
    arrive(1, 1)
    begin(3)
    begin(4)
    middle(2)
    pack(3, 0)
    pack(4, 0)
    arrive(1, 2)
    begin(5)
    pack(5, 0)
    for unit in UNIT_SHIFT:
        if unit + 1 in UNIT_SHIFT:
            middle(unit + 1)
        arrive(unit, 1)
        pack(unit, *DELTAS)
        arrive(unit, 2)
        pack(unit, 2)
    for copy in copies.values():
        copy.wait_send()


def all_gather_rows(w):
    dma = pltpu.SemaphoreType.DMA
    sems = 36 * 3
    return pl.pallas_call(
        ag_kernel,
        out_shape=pltpu.VMEM((1, 64 * w.size), BF16),
        in_specs=[pl.BlockSpec(memory_space=pltpu.VMEM)],
        out_specs=pl.BlockSpec(memory_space=pltpu.VMEM),
        scratch_shapes=[pltpu.VMEM((4, 4, 4, ROWS, LANES), w.dtype), dma((sems,)), dma((sems,))],
        compiler_params=pltpu.CompilerParams(collective_id=1, has_side_effects=True, vmem_limit_bytes=24 * MIB),
        name="weight_ag",
    )(w)


def dot32(a, b, dims=((1,), (0,))):
    return lax.dot_general(a, b, (dims, ((), ())), preferred_element_type=F32)


def dot_t(a, b):
    return dot32(a, b, ((1,), (1,)))


def block_kernel(scale, w_ref, xin_ref, t_ref, x_out, a_out, du_out, g_out, loss_ref,
                 w1, w2, xb, hb, gb, ab, db, tb, raw, wide, wsem, insem, outsem, hs, hr, gs, gr):
    stage = lax.axis_index("stage")
    first = stage == 0
    last = stage == 1
    other = {"stage": 1 - stage}

    def chunk(i):
        return pltpu.make_async_copy(w_ref.at[:, pl.ds(pl.multiple_of(i * PIECE, PIECE), PIECE)], raw.at[lax.rem(i, SLOTS)],
                                     wsem.at[lax.rem(i, SLOTS)])

    load_x = pltpu.make_async_copy(xin_ref, xb, insem.at[0])
    load_t = pltpu.make_async_copy(t_ref, tb, insem.at[1])

    def prefetch(i, carry):
        chunk(i).start()
        return carry

    lax.fori_loop(0, SLOTS, prefetch, 0)

    @pl.when(first)
    def _():
        load_x.start()

    @pl.when(last)
    def _():
        load_t.start()

    barrier = pltpu.get_barrier_semaphore()
    pl.semaphore_signal(barrier, inc=1, device_id=other, device_id_type=MESH)
    pl.semaphore_wait(barrier, 1)

    def convert(i, weight, blocks, pitch):
        rows = PIECE // (blocks * LANES)
        chunk(i).wait()

        slot = lax.rem(i, SLOTS)
        for j in range(PIECE // ROWS):
            line = raw[slot, :, j * ROWS:(j + 1) * ROWS]
            at = (j * 8 // blocks) * pitch + j * 8 % blocks
            wide[at:at + 8, :] = line.astype(F32).reshape(8, LANES)
        base = pl.ds(pl.multiple_of(lax.rem(i, CHUNKS // 2) * rows, rows), rows)
        for cb in range(blocks):
            weight[cb, base, :] = wide[pl.ds(cb, rows, stride=pitch), :].astype(BF16)

        @pl.when(i < CHUNKS - SLOTS)
        def _():
            chunk(i + SLOTS).start()

    def convert_first(i, carry):
        convert(i, w1, WIDE // LANES, PITCH)
        return carry

    def convert_second(i, carry):
        convert(i, w2, ROWS // LANES, ROWS // LANES)
        return carry

    lax.fori_loop(0, CHUNKS // 2, convert_first, 0)
    lax.fori_loop(CHUNKS // 2, CHUNKS, convert_second, 0)

    @pl.when(first)
    def _():
        load_x.wait()

    @pl.when(last)
    def _():
        load_t.wait()

    def span(i):
        return pl.ds(pl.multiple_of(i * TILE, TILE), TILE)

    def cols(j):
        return pl.ds(pl.multiple_of(j * COLS, COLS), COLS)

    def blocks(j):
        return [j * (COLS // LANES) + q for q in range(COLS // LANES)]

    def beside(weight, which, part):
        return jnp.concatenate([weight[cb, part, :] for cb in which], axis=1)

    def send_h(i):
        return pltpu.make_async_remote_copy(src_ref=hb.at[span(i)], dst_ref=xb.at[span(i)], send_sem=hs.at[i], recv_sem=hr.at[i],
                                            device_id=other, device_id_type=MESH)

    def send_g(i):
        return pltpu.make_async_remote_copy(src_ref=hb.at[span(i)], dst_ref=gb.at[span(i)], send_sem=gs.at[i], recv_sem=gr.at[i],
                                            device_id=other, device_id_type=MESH)

    def outputs(i):
        pairs = ((xb, x_out), (ab, a_out), (db, du_out), (gb, g_out))
        return [pltpu.make_async_copy(src.at[span(i)], dst.at[span(i)], outsem.at[i * 4 + k]) for k, (src, dst) in enumerate(pairs)]

    def forward(i):
        def up(j, carry):
            u = dot32(xb[span(i), :], beside(w1, blocks(j), ALL)).astype(BF16)
            db[span(i), cols(j)] = u
            uf = u.astype(F32)
            half = 0.5 * uf
            ab[span(i), cols(j)] = (half + half * jnp.tanh(uf * (GELU_A + GELU_B * (uf * uf)))).astype(BF16)
            return carry

        def down(j, carry):
            hb[span(i), cols(j)] = (xb[span(i), cols(j)].astype(F32) + dot32(ab[span(i), :], beside(w2, blocks(j), ALL))).astype(BF16)
            return carry

        lax.fori_loop(0, WIDE // COLS, up, 0, unroll=2)
        lax.fori_loop(0, ROWS // COLS, down, 0)

    def top(i):
        res = hb[span(i), :].astype(F32) - tb[span(i), :].astype(F32)
        gb[span(i), :] = (res * scale).astype(BF16)
        sums = jnp.sum((res * res).reshape(-1, 8, ROWS), axis=0)
        loss_ref[...] += sum(sums[:, k * LANES:(k + 1) * LANES] for k in range(ROWS // LANES))

    def backward(i):
        def body(j, carry):
            e = dot_t(gb[span(i), :], beside(w2, range(ROWS // LANES), cols(j)))
            u = db[span(i), cols(j)].astype(F32)
            sq = u * u
            gate = 0.5 + 0.5 * jnp.tanh(u * (GELU_A + GELU_B * sq))
            slope = gate + gate * ((1.0 - gate) * (u * (2.0 * GELU_A + (6.0 * GELU_B) * sq)))
            db[span(i), cols(j)] = (e * slope).astype(BF16)
            return carry

        lax.fori_loop(0, WIDE // COLS, body, 0, unroll=2)

    def below(i):
        def body(j, carry):
            hb[span(i), cols(j)] = (gb[span(i), cols(j)].astype(F32) + dot_t(db[span(i), :], beside(w1, range(WIDE // LANES), cols(j)))).astype(BF16)
            return carry

        lax.fori_loop(0, ROWS // COLS, body, 0)

    loss_ref[...] = jnp.zeros_like(loss_ref)

    def tick(it, carry):
        i = lax.rem(it, STEPS)

        @pl.when(it < STEPS)
        def _():
            @pl.when(last)
            def _():
                send_h(i).wait_recv()

            forward(i)

            @pl.when(first)
            def _():
                send_h(i).start()

            @pl.when(last)
            def _():
                top(i)

        @pl.when(it // STEPS + stage == 1)
        def _():
            @pl.when(first)
            def _():
                send_g(i).wait_recv()

            backward(i)

            @pl.when(last)
            def _():
                below(i)
                send_g(i).start()

            for copy in outputs(i):
                copy.start()
        return carry

    lax.fori_loop(0, 2 * STEPS, tick, 0)

    def drain(i, carry):
        @pl.when(first)
        def _():
            send_h(i).wait_send()

        @pl.when(last)
        def _():
            send_g(i).wait_send()

        for copy in outputs(i):
            copy.wait()
        return carry

    lax.fori_loop(0, STEPS, drain, 0)


def block_passes(flat, x_in, targets, token_count):
    anywhere = pl.BlockSpec(memory_space=pl.ANY)
    dma = pltpu.SemaphoreType.DMA
    narrow, wide = (ROWS, ROWS), (ROWS, WIDE)

    def shape(dims):
        return jax.ShapeDtypeStruct(dims, BF16)

    def room(dims):
        return pltpu.VMEM(dims, BF16)

    return pl.pallas_call(
        functools.partial(block_kernel, 1.0 / token_count),
        out_shape=(shape(narrow), shape(wide), shape(wide), shape(narrow), jax.ShapeDtypeStruct((8, LANES), F32)),
        in_specs=[anywhere] * 3,
        out_specs=(anywhere,) * 4 + (pl.BlockSpec(memory_space=pltpu.VMEM),),
        scratch_shapes=[room((WIDE // LANES, ROWS, LANES)), room((ROWS // LANES, WIDE, LANES)), room(narrow), room(narrow), room(narrow), room(wide), room(wide), room(narrow),
                        room((SLOTS, 1, PIECE)), pltpu.VMEM((32 * PITCH, LANES), F32),
                        dma((SLOTS,)), dma((2,)), dma((STEPS * 4,)), dma((STEPS,)), dma((STEPS,)), dma((STEPS,)), dma((STEPS,))],
        compiler_params=pltpu.CompilerParams(collective_id=2, has_side_effects=True, vmem_limit_bytes=60 * MIB),
        name="block",
    )(flat, x_in, targets)


def adam_kernel(rate, token_count, part_ref, total_ref, tau_ref, w_ref, m_ref, v_ref, w_out, m_out, v_out, b_out, loss_out, grad):
    early = lax.axis_index("data") < 32

    def reorder(rows):
        blocks = ROWS // rows
        for r in range(rows):
            grad[r * blocks:(r + 1) * blocks, :] = part_ref[pl.ds(r, blocks, stride=rows), :]

    @pl.when(early)
    def _():
        reorder(32)

    @pl.when(jnp.logical_not(early))
    def _():
        reorder(LANES)

    nu = jnp.sqrt(jnp.sum(total_ref[0], keepdims=True))
    scaled = jnp.minimum(1.0, tau_ref[...] / nu) * grad[...]
    m_new = ADAM_BETA1 * m_ref[...] + (1.0 - ADAM_BETA1) * scaled
    v_new = ADAM_BETA2 * v_ref[...] + (1.0 - ADAM_BETA2) * scaled * scaled
    m_hat = m_new / (1.0 - ADAM_BETA1 ** ADAM_STEP)
    v_hat = v_new / (1.0 - ADAM_BETA2 ** ADAM_STEP)
    w_new = w_ref[...] - rate * (m_hat / (jnp.sqrt(v_hat) + ADAM_EPS) + WEIGHT_DECAY * w_ref[...])
    w_out[...] = w_new
    m_out[...] = m_new
    v_out[...] = v_new
    b_out[...] = w_new.astype(BF16)
    loss_out[...] = (0.5 * jnp.sum(total_ref[1], keepdims=True)) / token_count


def adam(rate, token_count, part, totals, tau, w, m, v):
    state = jax.ShapeDtypeStruct(part.shape, F32)
    vmem = pl.BlockSpec(memory_space=pltpu.VMEM)
    return pl.pallas_call(
        functools.partial(adam_kernel, rate, token_count),
        out_shape=(state, state, state, jax.ShapeDtypeStruct(part.shape, BF16), jax.ShapeDtypeStruct((1, 1), F32)),
        in_specs=[vmem] * 6,
        out_specs=(vmem,) * 5,
        scratch_shapes=[pltpu.VMEM(part.shape, F32)],
        name="adam",
    )(part, totals, tau, w, m, v)


def solution(mesh):
    data_size = mesh.shape['data']

    def device_step(x_in, targets, w_work, w_master, m_prior, v_prior, clip_tau):
        token_count = x_in.shape[0] * x_in.shape[1] * data_size
        x, a, du, g, loss = block_passes(w_work.reshape(1, -1), x_in.reshape(ROWS, ROWS), targets.reshape(ROWS, ROWS), token_count)
        part, totals = reduce_scatter(x, du, a, g, loss)
        rate = LR_BASE / math.sqrt(x_in.shape[-1])
        state = [z.reshape(ROWS, LANES) for z in (w_master, m_prior, v_prior)]
        w_new, m_new, v_new, w_bf, loss_mean = adam(rate, token_count, part, totals, clip_tau.reshape(1, 1), *state)
        w_all = all_gather_rows(w_bf).reshape(w_work.shape)
        return (loss_mean.reshape(()), w_all) + tuple(z.reshape(w_master.shape) for z in (w_new, m_new, v_new))

    row_spec = P(None, 'data', None)
    shard_spec = P('stage', None, 'data')
    stage_spec = P('stage', None, None)
    return jax.shard_map(device_step, mesh=mesh, in_specs=(row_spec, row_spec, stage_spec, shard_spec, shard_spec, shard_spec, P()), out_specs=(P(), stage_spec, shard_spec, shard_spec, shard_spec), check_vma=False)
```

```python
import functools
import math
import jax
import jax.numpy as jnp
from jax import lax
from jax.experimental import pallas as pl
from jax.experimental.pallas import tpu as pltpu
from jax.sharding import PartitionSpec as P

ADAM_BETA1 = 0.9
ADAM_BETA2 = 0.95
ADAM_EPS = 1e-8
WEIGHT_DECAY = 0.1
ADAM_STEP = 10
LR_BASE = 0.05
MESH = pl.DeviceIdType.MESH
MIB = 1024 * 1024

UNITS = (1, 2, 2, 2, 1)
DELAY = 30
SUBS = len(UNITS)
ALL = slice(None)
RING = pl.ds(0, 4)
BOTH = range(2)
AXES = range(3)
LEADS = (16, 4, 1)
ROWWISE = ((0,), (0,))
DELTAS = (1, -1)
RS_ORDER = ((2, 1, 0), (1, 0, 2), (0, 2, 1))
UNIT_SHIFT = {2: 0, 3: -1, 4: 1, 5: 2}
AG_ORDER = ((0, 1, 2), (1, 2, 0), (2, 0, 1))


ROWS = 1024
WIDE = 4096
TILE = 256
COLS = 512
LANES = 128
STEPS = ROWS // TILE
PIECE = 131072
CHUNKS = 2 * ROWS * WIDE // PIECE
SLOTS = 16
PITCH = 40
GELU_A = math.sqrt(2.0 / math.pi)
GELU_B = GELU_A * 0.044715
BF16 = jnp.bfloat16
F32 = jnp.float32


def upto(n):
    return pl.ds(0, n)


def divide(t):
    return t // 4, lax.rem(t, 4)


def wrap(k):
    return lax.rem(k + 4, 4)


def rs_split():
    table, half_at, full_at = {}, [0], [0]
    start = 0
    for s, units in enumerate(UNITS):
        most = 0
        for c in AXES:
            n = (16 * units + (c + s) % 3) // 3
            first = (n + (s + c) % 2) // 2
            table[s, c] = tuple(8 * k for k in (start, first, n - first))
            start += n
            most = max(most, n)
        half_at.append(half_at[s] + (most + 1) // 2 * 8)
        full_at.append(full_at[s] + most * 8)
    return table, half_at, full_at


def coords_of(me):
    return [me // 16, lax.rem(me // 4, 4), lax.rem(me, 4)]


def peer(coords, pos, delta):
    moved = list(coords)
    moved[pos] = wrap(coords[pos] + delta)
    z, y, x = moved
    return z * 16 + y * 4 + x


def greet(coords, deltas, partner):
    barrier = pltpu.get_barrier_semaphore()
    ids = [{"data": peer(coords, pos, delta)} for pos in AXES for delta in deltas]
    if partner:
        ids.append({"stage": 1 - lax.axis_index("stage")})
    for other in ids:
        pl.semaphore_signal(barrier, inc=1, device_id=other, device_id_type=MESH)
    pl.semaphore_wait(barrier, len(ids))


def sum_everywhere(coords, acc, got, ssem, rsem):
    copies = []
    for ph in range(4):
        if ph < 3:
            mine = coords[ph]
            targets = [{"data": peer(coords, ph, k)} for k in range(1, 4)]
        else:
            mine = lax.axis_index("stage")
            targets = [{"stage": 1 - mine}]
        batch = []
        for k, target in enumerate(targets):
            i = ph * 3 + k
            batch.append(pltpu.make_async_remote_copy(src_ref=acc.at[ph], dst_ref=got.at[ph, mine], send_sem=ssem.at[i],
                                                      recv_sem=rsem.at[i], device_id=target, device_id_type=MESH))
        for copy in batch:
            copy.start()
        got[ph, mine] = acc[ph]
        for copy in batch:
            copy.wait_recv()
        acc[ph + 1] = sum(got[ph, k] for k in range(len(batch) + 1))
        copies += batch
    for copy in copies:
        copy.wait_send()


def rs_kernel(x_ref, du_ref, a_ref, top_ref, loss_ref, out_ref, total_ref, g_ref, ra1, rb1, lb, own, ra2, rb2, ra3, rb3, ssem, rsem, lsem,
              acc, got, tsem, usem, xb, gb, dub, ab, put1, put2, insem, dusem, asem, psem1, psem2):
    coords = coords_of(lax.axis_index("data"))
    table, half_at, full_at = rs_split()
    ra = (ra1, ra2, ra3)
    rb = (rb1, rb2, rb3)
    copies = {}

    load_x = pltpu.make_async_copy(x_ref, xb, insem.at[0])
    load_g = pltpu.make_async_copy(top_ref, gb, insem.at[1])

    def load_du(s):
        width = UNITS[s] * COLS
        return pltpu.make_async_copy(du_ref.at[:, pl.ds(sum(UNITS[:s]) * COLS, width)], dub.at[s % 2, :, upto(width)], dusem.at[s % 2])

    def load_a(m):
        return pltpu.make_async_copy(a_ref.at[:, pl.ds(pl.multiple_of(m * COLS, COLS), COLS)], ab.at[lax.rem(m, 2)], asem.at[lax.rem(m, 2)])

    def grads(s):
        size = UNITS[s] * LANES
        band = pl.ds(sum(UNITS[:s]) * LANES, size)
        width = UNITS[s] * COLS
        load_a(0).start()
        if s + 1 < SUBS:
            load_du(s + 1).start()
        load_du(s).wait()
        if s == 0:
            load_x.wait()
            load_g.wait()

        def write1(m):
            return pltpu.make_async_copy(put1.at[lax.rem(m, 2), :, :, upto(size)], g_ref.at[m // 2, pl.ds(lax.rem(m, 2) * 2, 2), :, band, :],
                                         psem1.at[lax.rem(m, 2)])

        def write2(m):
            return pltpu.make_async_copy(put2.at[lax.rem(m, 2), :, upto(size)], g_ref.at[m // 4 + 2, lax.rem(m, 4), :, band, :],
                                         psem2.at[lax.rem(m, 2)])

        def first(m, carry):
            val = dot32(xb[:, pl.ds(pl.multiple_of(m * TILE, TILE), TILE)], dub[s % 2, :, upto(width)], ROWWISE)

            @pl.when(m > 1)
            def _():
                write1(m - 2).wait()

            for ct in range(width // LANES):
                put1[lax.rem(m, 2), :, :, ct * 32:(ct + 1) * 32, :] = val[:, ct * LANES:(ct + 1) * LANES].reshape(2, 4, 32, LANES)
            write1(m).start()
            return carry

        def second(m, carry):
            load_a(m).wait()

            @pl.when(m < 7)
            def _():
                load_a(m + 1).start()

            val = dot32(ab[lax.rem(m, 2)], gb[:, band], ROWWISE)

            @pl.when(m > 1)
            def _():
                write2(m - 2).wait()

            for ct in range(UNITS[s]):
                part = slice(ct * LANES, (ct + 1) * LANES)
                put2[lax.rem(m, 2), :, part, :] = val[:, part].reshape(4, LANES, LANES)
            write2(m).start()
            return carry

        lax.fori_loop(0, 4, first, 0)
        lax.fori_loop(0, 8, second, 0)
        for m in BOTH:
            write1(m + 2).wait()
            write2(m + 6).wait()

    def rows(s, c, half):
        start, n0, n1 = table[s, c]
        if half == 0:
            return 0, n0
        if half == 1:
            return n0, n1
        return 0, n0 + n1

    def lead(ph, c, k):
        order = RS_ORDER[c]
        left = [p for p in AXES if p != order[0]]
        idx = []
        for p in left:
            if ph == 1:
                idx.append(k if p == order[1] else RING)
            else:
                idx.append(coords[order[1]] if p == order[1] else k)
        return tuple(idx)

    def lead_t(ph, c, k, t):
        if ph == 0:
            return divide(t), divide(t)
        mine = tuple(t if i is RING else i for i in lead(ph, c, k))
        return (t,) * (2 - ph), mine

    def source(ph, s, c, k, half):
        lo, n = rows(s, c, half)
        if ph == 0:
            idx = [RING] * 3
            idx[RS_ORDER[c][0]] = k
            return g_ref.at[tuple(idx) + (pl.ds(table[s, c][0] + lo, n), ALL)]
        return own.at[(c,) + lead(ph, c, k) + (pl.ds(full_at[s] + lo, n), ALL)]

    def slot(ref, ph, i, lo, n):
        return ref.at[(i,) + (RING,) * (2 - ph) + (pl.ds(lo, n), ALL)]

    def start(ph, s, c, d, piece, src, dst):
        i = (((ph * SUBS + s) * 3 + c) * 2 + d) * 3 + piece
        target = peer(coords, RS_ORDER[c][ph], DELTAS[d])
        copy = pltpu.make_async_remote_copy(src_ref=src, dst_ref=dst, send_sem=ssem.at[i], recv_sem=rsem.at[i],
                                            device_id={"data": target}, device_id_type=MESH)
        copy.start()
        copies[ph, s, c, d, piece] = copy

    def at(c, ph, delta):
        return wrap(coords[RS_ORDER[c][ph]] + delta)

    def send_a(ph, s, c):
        for d in BOTH:
            n = rows(s, c, d)[1]
            start(ph, s, c, d, 0, source(ph, s, c, at(c, ph, 2), d), slot(ra[ph], ph, c * 2 + d, half_at[s], n))

    def send_b1(ph, s, c):
        for d in BOTH:
            lo, n = rows(s, c, 1 - d)
            start(ph, s, c, d, 1, source(ph, s, c, at(c, ph, DELTAS[d]), 1 - d), slot(rb[ph], ph, c * 2 + d, full_at[s] + lo, n))

    def load(s, c):
        for d in BOTH:
            i = s * 9 + c * 3 + d
            n = rows(s, c, d)[1]
            copy = pltpu.make_async_copy(source(0, s, c, at(c, 0, DELTAS[d]), d), slot(lb, 0, s % 2 * 6 + c * 2 + d, 0, n), lsem.at[i])
            copy.start()
            copies["lb", s, c, d] = copy
        n = rows(s, c, 2)[1]
        copy = pltpu.make_async_copy(source(0, s, c, at(c, 0, 0), 2), slot(own, 0, c, full_at[s], n), lsem.at[s * 9 + c * 3 + 2])
        copy.start()
        copies["own", s, c] = copy

    def forward(ph, s, c):
        for d in BOTH:
            i = c * 2 + d
            lo, n = rows(s, c, d)
            if ph == 0:
                copies["lb", s, c, d].wait()
            copies[ph, s, c, d, 0].wait_recv()
            buf = ra[ph]
            k = at(c, ph, DELTAS[d])

            def body(t, carry, d=d, i=i, n=n, lo=lo, buf=buf, k=k):
                where, mine = lead_t(ph, c, k, t)
                term = lb[(s % 2 * 6 + c * 2 + d,) + where + (upto(n), ALL)] if ph == 0 else own[(c,) + mine + (pl.ds(full_at[s] + lo, n), ALL)]
                buf[(i,) + where + (pl.ds(half_at[s], n), ALL)] += term
                return carry

            lax.fori_loop(0, LEADS[ph], body, 0)
            start(ph, s, c, d, 2, slot(buf, ph, i, half_at[s], n), slot(rb[ph], ph, i, full_at[s] + lo, n))

    def finish(ph, s, c):
        if ph == 0:
            copies["own", s, c].wait()
        for d in BOTH:
            copies[ph, s, c, d, 1].wait_recv()
            copies[ph, s, c, d, 2].wait_recv()
        n = rows(s, c, 2)[1]
        i = c * 2
        buf = rb[ph]
        k = at(c, ph, 0)
        span = pl.ds(full_at[s], n)

        def body(t, carry):
            where, mine = lead_t(ph, c, k, t)
            mine = (c,) + mine + (span, ALL)
            total = own[mine] + buf[(i,) + where + (span, ALL)] + buf[(i + 1,) + where + (span, ALL)]
            if ph < 2:
                own[mine] = total
            else:
                out_ref[pl.ds(table[s, c][0], n), :] = total
            return carry

        lax.fori_loop(0, LEADS[ph], body, 0)

    def st0(s):
        for c in AXES:
            send_a(0, s, c)
            load(s, c)

    def st0b(s):
        for c in AXES:
            send_b1(0, s, c)

    def mid(ph, s):
        for c in AXES:
            forward(ph, s, c)

    def turn(ph, s):
        for c in AXES:
            finish(ph, s, c)
            if ph < 2:
                send_a(ph + 1, s, c)
                send_b1(ph + 1, s, c)

    def opening(s):
        if s < SUBS:
            grads(s)
            st0(s)

    def second(s):
        if s < SUBS:
            st0b(s)

    queue = [(mid, 0), (None, 0), (mid, 1)]
    for s in range(SUBS):
        queue += [(turn, s), (None, s + 1), (mid, s + 2)]
    steps, clock = [], 0
    for act, s in queue:
        if s < SUBS:
            clock += UNITS[s]
            steps.append((clock, 0, act, 0, s))
            if act is turn:
                for ph in range(1, 3):
                    steps.append((clock + DELAY * ph - DELAY // 2, 1, mid, ph, s))
                    steps.append((clock + DELAY * ph, 1, turn, ph, s))
    steps = [e for e in steps if e[2]]
    load_x.start()
    load_du(0).start()
    load_g.start()
    greet(coords, range(1, 4), True)
    opening(0)
    second(0)
    opening(1)
    for _, _, act, ph, s in sorted(steps, key=lambda e: e[:2]):
        act(ph, s)
        if act is mid and ph == 0:
            second(s + 1)
            opening(s + 2)
    for key, copy in copies.items():
        if not isinstance(key[0], str):
            copy.wait_send()
    part = out_ref[...]
    acc[0, 0] = jnp.sum((part * part).reshape(-1, 8, 128), axis=0)
    acc[0, 1] = loss_ref[...]
    sum_everywhere(coords, acc, got, tsem, usem)
    total_ref[...] = acc[4]


def reduce_scatter(x, du, a, g, loss):
    sems = 54 * SUBS
    f32 = jnp.float32
    dma = pltpu.SemaphoreType.DMA
    vmem = pl.BlockSpec(memory_space=pltpu.VMEM)
    anywhere = pl.BlockSpec(memory_space=pl.ANY)

    _, half_at, full_at = rs_split()

    def slots(n, axes, rows):
        return pltpu.VMEM((n,) + (4,) * axes + (rows, LANES), f32)

    def landing(axes):
        return [slots(6, axes, half_at[-1]), slots(6, axes, full_at[-1])]

    part, totals, _ = pl.pallas_call(
        rs_kernel,
        out_shape=(jax.ShapeDtypeStruct((ROWS, LANES), f32), jax.ShapeDtypeStruct((2, 8, LANES), f32),
                   jax.ShapeDtypeStruct((4, 4, 4, ROWS, LANES), f32)),
        in_specs=[anywhere] * 4 + [vmem],
        out_specs=(vmem, vmem, anywhere),
        scratch_shapes=[*landing(2), slots(12, 2, 48), slots(3, 2, full_at[-1]), *landing(1), *landing(0),
                        dma((sems,)), dma((sems,)), dma((SUBS * 9,)),
                        pltpu.VMEM((5, 2, 8, LANES), f32), pltpu.VMEM((4, 4, 2, 8, LANES), f32), dma((10,)), dma((10,)),
                        pltpu.VMEM((ROWS, ROWS), BF16), pltpu.VMEM((ROWS, ROWS), BF16), pltpu.VMEM((2, ROWS, ROWS), BF16),
                        pltpu.VMEM((2, ROWS, COLS), BF16), pltpu.VMEM((2, 2, 4, TILE, LANES), f32),
                        pltpu.VMEM((2, 4, TILE, LANES), f32), dma((2,)), dma((2,)), dma((2,)), dma((2,)), dma((2,))],
        compiler_params=pltpu.CompilerParams(collective_id=0, has_side_effects=True, vmem_limit_bytes=63 * MIB),
        name="grad_rs",
    )(x, du, a, g, loss)
    return part, totals


def ag_split():
    table = []
    start = 0
    for c, n in enumerate((22, 21, 21)):
        first = (n + c % 2) // 2
        table.append(tuple(16 * k for k in (start, first, n - first)))
        start += n
    return table


def ag_kernel(w_ref, wide_ref, out_ref, ssem, rsem):
    coords = coords_of(lax.axis_index("data"))
    table = ag_split()
    copies = {}

    def rows(c, half):
        start, n0, n1 = table[c]
        return (start, n0) if half == 0 else (start + n0, n1)

    def region(c, unit, shift, half):
        first, second, third = AG_ORDER[c]
        idx = [None] * 3
        if unit == 0:
            idx[first], idx[second], idx[third] = wrap(coords[first] + shift), coords[second], coords[third]
        elif unit == 1:
            idx[first], idx[second], idx[third] = RING, wrap(coords[second] + shift), coords[third]
        else:
            q = wrap(coords[second] + UNIT_SHIFT[unit])
            idx[first], idx[second], idx[third] = RING, q, wrap(coords[third] + shift)
        lo, n = rows(c, half)
        return out_ref.at[tuple(idx) + (pl.ds(lo, n), ALL)]

    def start(c, unit, d, piece, src, dst):
        i = ((unit * 3 + c) * 2 + d) * 3 + piece
        target = peer(coords, AG_ORDER[c][min(unit, 2)], DELTAS[d])
        copy = pltpu.make_async_remote_copy(src_ref=src, dst_ref=dst, send_sem=ssem.at[i], recv_sem=rsem.at[i],
                                            device_id={"data": target}, device_id_type=MESH)
        copy.start()
        copies[c, unit, d, piece] = copy

    def begin(unit):
        for c in AXES:
            for d in BOTH:
                for piece, half in ((0, d), (1, 1 - d)):
                    lo, n = rows(c, half)
                    here = region(c, unit, 0, half)
                    src = w_ref.at[pl.ds(lo, n), :] if unit == 0 else here
                    start(c, unit, d, piece, src, here)

    def middle(unit):
        for c in AXES:
            for d in BOTH:
                copies[c, unit, d, 0].wait_recv()
                part = region(c, unit, -DELTAS[d], d)
                start(c, unit, d, 2, part, part)

    def arrive(unit, piece):
        for c in AXES:
            for d in BOTH:
                copies[c, unit, d, piece].wait_recv()

    def pack(unit, *shifts):
        for shift in shifts:
            for c in AXES:
                start, n0, n1 = table[c]
                _, second, third = AG_ORDER[c]
                at = {second: wrap(coords[second] + UNIT_SHIFT[unit]), third: wrap(coords[third] + shift)}

                def body(t, carry, at=at, start=start, n=n0 + n1):
                    where = tuple(at.get(p, t) for p in AXES)
                    z, y, x = where
                    base = (z * 16 + y * 4 + x) * PIECE + start * LANES
                    for k in range(n // 16):
                        line = out_ref[where + (pl.ds(start + k * 16, 16), ALL)].astype(F32)
                        line = line.reshape(1, 2 * ROWS).astype(BF16)
                        wide_ref[:, pl.ds(pl.multiple_of(base + k * 2 * ROWS, 2 * ROWS), 2 * ROWS)] = line
                    return carry

                lax.fori_loop(0, 4, body, 0)

    greet(coords, DELTAS, False)
    begin(0)
    out_ref[tuple(coords)] = w_ref[...]
    middle(0)
    arrive(0, 1)
    arrive(0, 2)
    begin(1)
    begin(2)
    pack(2, 0)
    middle(1)
    arrive(1, 1)
    begin(3)
    begin(4)
    middle(2)
    pack(3, 0)
    pack(4, 0)
    arrive(1, 2)
    begin(5)
    pack(5, 0)
    for unit in UNIT_SHIFT:
        if unit + 1 in UNIT_SHIFT:
            middle(unit + 1)
        arrive(unit, 1)
        pack(unit, *DELTAS)
        arrive(unit, 2)
        pack(unit, 2)
    for copy in copies.values():
        copy.wait_send()


def all_gather_rows(w):
    dma = pltpu.SemaphoreType.DMA
    sems = 36 * 3
    return pl.pallas_call(
        ag_kernel,
        out_shape=pltpu.VMEM((1, 64 * w.size), BF16),
        in_specs=[pl.BlockSpec(memory_space=pltpu.VMEM)],
        out_specs=pl.BlockSpec(memory_space=pltpu.VMEM),
        scratch_shapes=[pltpu.VMEM((4, 4, 4, ROWS, LANES), w.dtype), dma((sems,)), dma((sems,))],
        compiler_params=pltpu.CompilerParams(collective_id=1, has_side_effects=True, vmem_limit_bytes=24 * MIB),
        name="weight_ag",
    )(w)


def dot32(a, b, dims=((1,), (0,))):
    return lax.dot_general(a, b, (dims, ((), ())), preferred_element_type=F32)


def dot_t(a, b):
    return dot32(a, b, ((1,), (1,)))


def block_kernel(scale, w_ref, xin_ref, t_ref, x_out, a_out, du_out, g_out, loss_ref,
                 w1, w2, xb, hb, gb, ab, db, tb, raw, wide, wsem, insem, outsem, hs, hr, gs, gr):
    stage = lax.axis_index("stage")
    first = stage == 0
    last = stage == 1
    other = {"stage": 1 - stage}

    def chunk(i):
        return pltpu.make_async_copy(w_ref.at[:, pl.ds(pl.multiple_of(i * PIECE, PIECE), PIECE)], raw.at[lax.rem(i, SLOTS)],
                                     wsem.at[lax.rem(i, SLOTS)])

    load_x = pltpu.make_async_copy(xin_ref, xb, insem.at[0])
    load_t = pltpu.make_async_copy(t_ref, tb, insem.at[1])

    def prefetch(i, carry):
        chunk(i).start()
        return carry

    lax.fori_loop(0, SLOTS, prefetch, 0)

    @pl.when(first)
    def _():
        load_x.start()

    @pl.when(last)
    def _():
        load_t.start()

    barrier = pltpu.get_barrier_semaphore()
    pl.semaphore_signal(barrier, inc=1, device_id=other, device_id_type=MESH)
    pl.semaphore_wait(barrier, 1)

    def convert(i, weight, blocks, pitch):
        rows = PIECE // (blocks * LANES)
        chunk(i).wait()

        slot = lax.rem(i, SLOTS)
        for j in range(PIECE // ROWS):
            line = raw[slot, :, j * ROWS:(j + 1) * ROWS]
            at = (j * 8 // blocks) * pitch + j * 8 % blocks
            wide[at:at + 8, :] = line.astype(F32).reshape(8, LANES)
        base = pl.ds(pl.multiple_of(lax.rem(i, CHUNKS // 2) * rows, rows), rows)
        for cb in range(blocks):
            weight[cb, base, :] = wide[pl.ds(cb, rows, stride=pitch), :].astype(BF16)

        @pl.when(i < CHUNKS - SLOTS)
        def _():
            chunk(i + SLOTS).start()

    def convert_first(i, carry):
        convert(i, w1, WIDE // LANES, PITCH)
        return carry

    def convert_second(i, carry):
        convert(i, w2, ROWS // LANES, ROWS // LANES)
        return carry

    lax.fori_loop(0, CHUNKS // 2, convert_first, 0)
    lax.fori_loop(CHUNKS // 2, CHUNKS, convert_second, 0)

    @pl.when(first)
    def _():
        load_x.wait()

    @pl.when(last)
    def _():
        load_t.wait()

    def span(i):
        return pl.ds(pl.multiple_of(i * TILE, TILE), TILE)

    def cols(j):
        return pl.ds(pl.multiple_of(j * COLS, COLS), COLS)

    def blocks(j):
        return [j * (COLS // LANES) + q for q in range(COLS // LANES)]

    def beside(weight, which, part):
        return jnp.concatenate([weight[cb, part, :] for cb in which], axis=1)

    def send_h(i):
        return pltpu.make_async_remote_copy(src_ref=hb.at[span(i)], dst_ref=xb.at[span(i)], send_sem=hs.at[i], recv_sem=hr.at[i],
                                            device_id=other, device_id_type=MESH)

    def send_g(i):
        return pltpu.make_async_remote_copy(src_ref=hb.at[span(i)], dst_ref=gb.at[span(i)], send_sem=gs.at[i], recv_sem=gr.at[i],
                                            device_id=other, device_id_type=MESH)

    def outputs(i):
        pairs = ((xb, x_out), (ab, a_out), (db, du_out), (gb, g_out))
        return [pltpu.make_async_copy(src.at[span(i)], dst.at[span(i)], outsem.at[i * 4 + k]) for k, (src, dst) in enumerate(pairs)]

    def forward(i):
        def up(j, carry):
            u = dot32(xb[span(i), :], beside(w1, blocks(j), ALL)).astype(BF16)
            db[span(i), cols(j)] = u
            uf = u.astype(F32)
            half = 0.5 * uf
            ab[span(i), cols(j)] = (half + half * jnp.tanh(uf * (GELU_A + GELU_B * (uf * uf)))).astype(BF16)
            return carry

        def down(j, carry):
            hb[span(i), cols(j)] = (xb[span(i), cols(j)].astype(F32) + dot32(ab[span(i), :], beside(w2, blocks(j), ALL))).astype(BF16)
            return carry

        lax.fori_loop(0, WIDE // COLS, up, 0, unroll=2)
        lax.fori_loop(0, ROWS // COLS, down, 0)

    def top(i):
        res = hb[span(i), :].astype(F32) - tb[span(i), :].astype(F32)
        gb[span(i), :] = (res * scale).astype(BF16)
        sums = jnp.sum((res * res).reshape(-1, 8, ROWS), axis=0)
        loss_ref[...] += sum(sums[:, k * LANES:(k + 1) * LANES] for k in range(ROWS // LANES))

    def backward(i):
        def body(j, carry):
            e = dot_t(gb[span(i), :], beside(w2, range(ROWS // LANES), cols(j)))
            u = db[span(i), cols(j)].astype(F32)
            sq = u * u
            gate = 0.5 + 0.5 * jnp.tanh(u * (GELU_A + GELU_B * sq))
            slope = gate + gate * ((1.0 - gate) * (u * (2.0 * GELU_A + (6.0 * GELU_B) * sq)))
            db[span(i), cols(j)] = (e * slope).astype(BF16)
            return carry

        lax.fori_loop(0, WIDE // COLS, body, 0, unroll=2)

    def below(i):
        def body(j, carry):
            hb[span(i), cols(j)] = (gb[span(i), cols(j)].astype(F32) + dot_t(db[span(i), :], beside(w1, range(WIDE // LANES), cols(j)))).astype(BF16)
            return carry

        lax.fori_loop(0, ROWS // COLS, body, 0)

    loss_ref[...] = jnp.zeros_like(loss_ref)

    def tick(it, carry):
        i = lax.rem(it, STEPS)

        @pl.when(it < STEPS)
        def _():
            @pl.when(last)
            def _():
                send_h(i).wait_recv()

            forward(i)

            @pl.when(first)
            def _():
                send_h(i).start()

            @pl.when(last)
            def _():
                top(i)

        @pl.when(it // STEPS + stage == 1)
        def _():
            @pl.when(first)
            def _():
                send_g(i).wait_recv()

            backward(i)

            @pl.when(last)
            def _():
                below(i)
                send_g(i).start()

            for copy in outputs(i):
                copy.start()
        return carry

    lax.fori_loop(0, 2 * STEPS, tick, 0)

    def drain(i, carry):
        @pl.when(first)
        def _():
            send_h(i).wait_send()

        @pl.when(last)
        def _():
            send_g(i).wait_send()

        for copy in outputs(i):
            copy.wait()
        return carry

    lax.fori_loop(0, STEPS, drain, 0)


def block_passes(flat, x_in, targets, token_count):
    anywhere = pl.BlockSpec(memory_space=pl.ANY)
    dma = pltpu.SemaphoreType.DMA
    narrow, wide = (ROWS, ROWS), (ROWS, WIDE)

    def shape(dims):
        return jax.ShapeDtypeStruct(dims, BF16)

    def room(dims):
        return pltpu.VMEM(dims, BF16)

    return pl.pallas_call(
        functools.partial(block_kernel, 1.0 / token_count),
        out_shape=(shape(narrow), shape(wide), shape(wide), shape(narrow), jax.ShapeDtypeStruct((8, LANES), F32)),
        in_specs=[anywhere] * 3,
        out_specs=(anywhere,) * 4 + (pl.BlockSpec(memory_space=pltpu.VMEM),),
        scratch_shapes=[room((WIDE // LANES, ROWS, LANES)), room((ROWS // LANES, WIDE, LANES)), room(narrow), room(narrow), room(narrow), room(wide), room(wide), room(narrow),
                        room((SLOTS, 1, PIECE)), pltpu.VMEM((32 * PITCH, LANES), F32),
                        dma((SLOTS,)), dma((2,)), dma((STEPS * 4,)), dma((STEPS,)), dma((STEPS,)), dma((STEPS,)), dma((STEPS,))],
        compiler_params=pltpu.CompilerParams(collective_id=2, has_side_effects=True, vmem_limit_bytes=60 * MIB),
        name="block",
    )(flat, x_in, targets)


def adam_kernel(rate, token_count, part_ref, total_ref, tau_ref, w_ref, m_ref, v_ref, w_out, m_out, v_out, b_out, loss_out, grad):
    early = lax.axis_index("data") < 32

    def reorder(rows):
        blocks = ROWS // rows
        for r in range(rows):
            grad[r * blocks:(r + 1) * blocks, :] = part_ref[pl.ds(r, blocks, stride=rows), :]

    @pl.when(early)
    def _():
        reorder(32)

    @pl.when(jnp.logical_not(early))
    def _():
        reorder(LANES)

    nu = jnp.sqrt(jnp.sum(total_ref[0], keepdims=True))
    scaled = jnp.minimum(1.0, tau_ref[...] / nu) * grad[...]
    m_new = ADAM_BETA1 * m_ref[...] + (1.0 - ADAM_BETA1) * scaled
    v_new = ADAM_BETA2 * v_ref[...] + (1.0 - ADAM_BETA2) * scaled * scaled
    m_hat = m_new / (1.0 - ADAM_BETA1 ** ADAM_STEP)
    v_hat = v_new / (1.0 - ADAM_BETA2 ** ADAM_STEP)
    w_new = w_ref[...] - rate * (m_hat / (jnp.sqrt(v_hat) + ADAM_EPS) + WEIGHT_DECAY * w_ref[...])
    w_out[...] = w_new
    m_out[...] = m_new
    v_out[...] = v_new
    b_out[...] = w_new.astype(BF16)
    loss_out[...] = (0.5 * jnp.sum(total_ref[1], keepdims=True)) / token_count


def adam(rate, token_count, part, totals, tau, w, m, v):
    state = jax.ShapeDtypeStruct(part.shape, F32)
    vmem = pl.BlockSpec(memory_space=pltpu.VMEM)
    return pl.pallas_call(
        functools.partial(adam_kernel, rate, token_count),
        out_shape=(state, state, state, jax.ShapeDtypeStruct(part.shape, BF16), jax.ShapeDtypeStruct((1, 1), F32)),
        in_specs=[vmem] * 6,
        out_specs=(vmem,) * 5,
        scratch_shapes=[pltpu.VMEM(part.shape, F32)],
        name="adam",
    )(part, totals, tau, w, m, v)


def solution(mesh):
    data_size = mesh.shape['data']

    def device_step(x_in, targets, w_work, w_master, m_prior, v_prior, clip_tau):
        token_count = x_in.shape[0] * x_in.shape[1] * data_size
        x, a, du, g, loss = block_passes(w_work.reshape(1, -1), x_in.reshape(ROWS, ROWS), targets.reshape(ROWS, ROWS), token_count)
        part, totals = reduce_scatter(x, du, a, g, loss)
        rate = LR_BASE / math.sqrt(x_in.shape[-1])
        state = [z.reshape(ROWS, LANES) for z in (w_master, m_prior, v_prior)]
        w_new, m_new, v_new, w_bf, loss_mean = adam(rate, token_count, part, totals, clip_tau.reshape(1, 1), *state)
        w_all = all_gather_rows(w_bf).reshape(w_work.shape)
        return (loss_mean.reshape(()), w_all) + tuple(z.reshape(w_master.shape) for z in (w_new, m_new, v_new))

    row_spec = P(None, 'data', None)
    shard_spec = P('stage', None, 'data')
    stage_spec = P('stage', None, None)
    return jax.shard_map(device_step, mesh=mesh, in_specs=(row_spec, row_spec, stage_spec, shard_spec, shard_spec, shard_spec, P()), out_specs=(P(), stage_spec, shard_spec, shard_spec, shard_spec), check_vma=False)
```

```python
import functools
import math
import jax
import jax.numpy as jnp
from jax import lax
from jax.experimental import pallas as pl
from jax.experimental.pallas import tpu as pltpu
from jax.sharding import PartitionSpec as P

ADAM_BETA1 = 0.9
ADAM_BETA2 = 0.95
ADAM_EPS = 1e-8
WEIGHT_DECAY = 0.1
ADAM_STEP = 10
LR_BASE = 0.05
MESH = pl.DeviceIdType.MESH
MIB = 1024 * 1024

UNITS = (1, 2, 2, 2, 1)
DELAY = 30
DEPTH = 4
SUBS = len(UNITS)
ALL = slice(None)
RING = pl.ds(0, 4)
BOTH = range(2)
AXES = range(3)
LEADS = (16, 4, 1)
ROWWISE = ((0,), (0,))
DELTAS = (1, -1)
RS_ORDER = ((2, 1, 0), (1, 0, 2), (0, 2, 1))
UNIT_SHIFT = {2: 0, 3: -1, 4: 1, 5: 2}
AG_ORDER = ((0, 1, 2), (1, 2, 0), (2, 0, 1))


ROWS = 1024
WIDE = 4096
TILE = 256
COLS = 512
LANES = 128
STEPS = ROWS // TILE
PIECE = 131072
CHUNKS = 2 * ROWS * WIDE // PIECE
SLOTS = 16
PITCH = 40
GELU_A = math.sqrt(2.0 / math.pi)
GELU_B = GELU_A * 0.044715
BF16 = jnp.bfloat16
F32 = jnp.float32


def upto(n):
    return pl.ds(0, n)


def divide(t):
    return t // 4, lax.rem(t, 4)


def wrap(k):
    return lax.rem(k + 4, 4)


def rs_split():
    table, half_at, full_at = {}, [0], [0]
    start = 0
    for s, units in enumerate(UNITS):
        most = 0
        for c in AXES:
            n = (16 * units + (c + s) % 3) // 3
            first = (n + (s + c) % 2) // 2
            table[s, c] = tuple(8 * k for k in (start, first, n - first))
            start += n
            most = max(most, n)
        half_at.append(half_at[s] + (most + 1) // 2 * 8)
        full_at.append(full_at[s] + most * 8)
    return table, half_at, full_at


def coords_of(me):
    return [me // 16, lax.rem(me // 4, 4), lax.rem(me, 4)]


def peer(coords, pos, delta):
    moved = list(coords)
    moved[pos] = wrap(coords[pos] + delta)
    z, y, x = moved
    return z * 16 + y * 4 + x


def greet(coords, deltas, partner):
    barrier = pltpu.get_barrier_semaphore()
    ids = [{"data": peer(coords, pos, delta)} for pos in AXES for delta in deltas]
    if partner:
        ids.append({"stage": 1 - lax.axis_index("stage")})
    for other in ids:
        pl.semaphore_signal(barrier, inc=1, device_id=other, device_id_type=MESH)
    pl.semaphore_wait(barrier, len(ids))


def sum_everywhere(coords, acc, got, ssem, rsem):
    copies = []
    for ph in range(4):
        if ph < 3:
            mine = coords[ph]
            targets = [{"data": peer(coords, ph, k)} for k in range(1, 4)]
        else:
            mine = lax.axis_index("stage")
            targets = [{"stage": 1 - mine}]
        batch = []
        for k, target in enumerate(targets):
            i = ph * 3 + k
            batch.append(pltpu.make_async_remote_copy(src_ref=acc.at[ph], dst_ref=got.at[ph, mine], send_sem=ssem.at[i],
                                                      recv_sem=rsem.at[i], device_id=target, device_id_type=MESH))
        for copy in batch:
            copy.start()
        got[ph, mine] = acc[ph]
        for copy in batch:
            copy.wait_recv()
        acc[ph + 1] = sum(got[ph, k] for k in range(len(batch) + 1))
        copies += batch
    for copy in copies:
        copy.wait_send()


def rs_kernel(x_ref, du_ref, a_ref, top_ref, loss_ref, out_ref, total_ref, g_ref, ra1, rb1, lb, own, ra2, rb2, ra3, rb3, ssem, rsem, lsem,
              acc, got, tsem, usem, xb, gb, dub, ab, put1, put2, insem, dusem, asem, psem1, psem2):
    coords = coords_of(lax.axis_index("data"))
    table, half_at, full_at = rs_split()
    ra = (ra1, ra2, ra3)
    rb = (rb1, rb2, rb3)
    copies = {}

    load_x = pltpu.make_async_copy(x_ref, xb, insem.at[0])
    load_g = pltpu.make_async_copy(top_ref, gb, insem.at[1])

    def load_du(s):
        width = UNITS[s] * COLS
        return pltpu.make_async_copy(du_ref.at[:, pl.ds(sum(UNITS[:s]) * COLS, width)], dub.at[:, upto(width)], dusem)

    def load_a(m):
        return pltpu.make_async_copy(a_ref.at[:, pl.ds(pl.multiple_of(m * COLS, COLS), COLS)], ab.at[lax.rem(m, DEPTH)],
                                     asem.at[lax.rem(m, DEPTH)])

    def first_blocks():
        for m in range(DEPTH - 1):
            load_a(m).start()

    def grads(s):
        size = UNITS[s] * LANES
        band = pl.ds(sum(UNITS[:s]) * LANES, size)
        width = UNITS[s] * COLS
        if s:
            first_blocks()
        load_du(s).wait()
        if s == 0:
            load_x.wait()
            load_g.wait()

        def write1(m):
            return pltpu.make_async_copy(put1.at[lax.rem(m, 2), :, :, upto(size)], g_ref.at[m // 2, pl.ds(lax.rem(m, 2) * 2, 2), :, band, :],
                                         psem1.at[lax.rem(m, 2)])

        def write2(m):
            return pltpu.make_async_copy(put2.at[lax.rem(m, DEPTH), :, upto(size)], g_ref.at[m // 4 + 2, lax.rem(m, 4), :, band, :],
                                         psem2.at[lax.rem(m, DEPTH)])

        def first(m, carry):
            val = dot32(xb[:, pl.ds(pl.multiple_of(m * TILE, TILE), TILE)], dub[:, upto(width)], ROWWISE)

            @pl.when(m > 1)
            def _():
                write1(m - 2).wait()

            for ct in range(width // LANES):
                put1[lax.rem(m, 2), :, :, ct * 32:(ct + 1) * 32, :] = val[:, ct * LANES:(ct + 1) * LANES].reshape(2, 4, 32, LANES)
            write1(m).start()
            return carry

        def second(m, carry):
            load_a(m).wait()

            @pl.when(m < WIDE // COLS - DEPTH + 1)
            def _():
                load_a(m + DEPTH - 1).start()

            val = dot32(ab[lax.rem(m, DEPTH)], gb[:, band], ROWWISE)

            @pl.when(m >= DEPTH)
            def _():
                write2(m - DEPTH).wait()

            for ct in range(UNITS[s]):
                part = slice(ct * LANES, (ct + 1) * LANES)
                put2[lax.rem(m, DEPTH), :, part, :] = val[:, part].reshape(4, LANES, LANES)
            write2(m).start()
            return carry

        lax.fori_loop(0, 4, first, 0)
        if s + 1 < SUBS:
            load_du(s + 1).start()
        lax.fori_loop(0, WIDE // COLS, second, 0)
        for m in BOTH:
            write1(m + 2).wait()
        for m in range(DEPTH):
            write2(m + WIDE // COLS - DEPTH).wait()

    def rows(s, c, half):
        start, n0, n1 = table[s, c]
        if half == 0:
            return 0, n0
        if half == 1:
            return n0, n1
        return 0, n0 + n1

    def lead(ph, c, k):
        order = RS_ORDER[c]
        left = [p for p in AXES if p != order[0]]
        idx = []
        for p in left:
            if ph == 1:
                idx.append(k if p == order[1] else RING)
            else:
                idx.append(coords[order[1]] if p == order[1] else k)
        return tuple(idx)

    def lead_t(ph, c, k, t):
        if ph == 0:
            return divide(t), divide(t)
        mine = tuple(t if i is RING else i for i in lead(ph, c, k))
        return (t,) * (2 - ph), mine

    def source(ph, s, c, k, half):
        lo, n = rows(s, c, half)
        if ph == 0:
            idx = [RING] * 3
            idx[RS_ORDER[c][0]] = k
            return g_ref.at[tuple(idx) + (pl.ds(table[s, c][0] + lo, n), ALL)]
        return own.at[(c,) + lead(ph, c, k) + (pl.ds(full_at[s] + lo, n), ALL)]

    def slot(ref, ph, i, lo, n):
        return ref.at[(i,) + (RING,) * (2 - ph) + (pl.ds(lo, n), ALL)]

    def start(ph, s, c, d, piece, src, dst):
        i = (((ph * SUBS + s) * 3 + c) * 2 + d) * 3 + piece
        target = peer(coords, RS_ORDER[c][ph], DELTAS[d])
        copy = pltpu.make_async_remote_copy(src_ref=src, dst_ref=dst, send_sem=ssem.at[i], recv_sem=rsem.at[i],
                                            device_id={"data": target}, device_id_type=MESH)
        copy.start()
        copies[ph, s, c, d, piece] = copy

    def at(c, ph, delta):
        return wrap(coords[RS_ORDER[c][ph]] + delta)

    def send_a(ph, s, c):
        for d in BOTH:
            n = rows(s, c, d)[1]
            start(ph, s, c, d, 0, source(ph, s, c, at(c, ph, 2), d), slot(ra[ph], ph, c * 2 + d, half_at[s], n))

    def send_b1(ph, s, c):
        for d in BOTH:
            lo, n = rows(s, c, 1 - d)
            start(ph, s, c, d, 1, source(ph, s, c, at(c, ph, DELTAS[d]), 1 - d), slot(rb[ph], ph, c * 2 + d, full_at[s] + lo, n))

    def load(s, c):
        for d in BOTH:
            i = s * 9 + c * 3 + d
            n = rows(s, c, d)[1]
            copy = pltpu.make_async_copy(source(0, s, c, at(c, 0, DELTAS[d]), d), slot(lb, 0, s % 2 * 6 + c * 2 + d, 0, n), lsem.at[i])
            copy.start()
            copies["lb", s, c, d] = copy
        n = rows(s, c, 2)[1]
        copy = pltpu.make_async_copy(source(0, s, c, at(c, 0, 0), 2), slot(own, 0, c, full_at[s], n), lsem.at[s * 9 + c * 3 + 2])
        copy.start()
        copies["own", s, c] = copy

    def forward(ph, s, c):
        for d in BOTH:
            i = c * 2 + d
            lo, n = rows(s, c, d)
            if ph == 0:
                copies["lb", s, c, d].wait()
            copies[ph, s, c, d, 0].wait_recv()
            buf = ra[ph]
            k = at(c, ph, DELTAS[d])

            def body(t, carry, d=d, i=i, n=n, lo=lo, buf=buf, k=k):
                where, mine = lead_t(ph, c, k, t)
                term = lb[(s % 2 * 6 + c * 2 + d,) + where + (upto(n), ALL)] if ph == 0 else own[(c,) + mine + (pl.ds(full_at[s] + lo, n), ALL)]
                buf[(i,) + where + (pl.ds(half_at[s], n), ALL)] += term
                return carry

            lax.fori_loop(0, LEADS[ph], body, 0)
            start(ph, s, c, d, 2, slot(buf, ph, i, half_at[s], n), slot(rb[ph], ph, i, full_at[s] + lo, n))

    def finish(ph, s, c):
        if ph == 0:
            copies["own", s, c].wait()
        for d in BOTH:
            copies[ph, s, c, d, 1].wait_recv()
            copies[ph, s, c, d, 2].wait_recv()
        n = rows(s, c, 2)[1]
        i = c * 2
        buf = rb[ph]
        k = at(c, ph, 0)
        span = pl.ds(full_at[s], n)

        def body(t, carry):
            where, mine = lead_t(ph, c, k, t)
            mine = (c,) + mine + (span, ALL)
            total = own[mine] + buf[(i,) + where + (span, ALL)] + buf[(i + 1,) + where + (span, ALL)]
            if ph < 2:
                own[mine] = total
            else:
                out_ref[pl.ds(table[s, c][0], n), :] = total
            return carry

        lax.fori_loop(0, LEADS[ph], body, 0)

    def st0(s):
        for c in AXES:
            send_a(0, s, c)
            load(s, c)

    def st0b(s):
        for c in AXES:
            send_b1(0, s, c)

    def mid(ph, s):
        for c in AXES:
            forward(ph, s, c)

    def turn(ph, s):
        for c in AXES:
            finish(ph, s, c)
            if ph < 2:
                send_a(ph + 1, s, c)
                send_b1(ph + 1, s, c)

    def opening(s):
        if s < SUBS:
            grads(s)
            st0(s)

    def second(s):
        if s < SUBS:
            st0b(s)

    queue = [(mid, 0), (None, 0), (mid, 1)]
    for s in range(SUBS):
        queue += [(turn, s), (None, s + 1), (mid, s + 2)]
    steps, clock = [], 0
    for act, s in queue:
        if s < SUBS:
            clock += UNITS[s]
            steps.append((clock, 0, act, 0, s))
            if act is turn:
                for ph in range(1, 3):
                    steps.append((clock + DELAY * ph - DELAY // 2, 1, mid, ph, s))
                    steps.append((clock + DELAY * ph, 1, turn, ph, s))
    steps = [e for e in steps if e[2]]
    load_x.start()
    load_du(0).start()
    load_g.start()
    first_blocks()
    greet(coords, range(1, 4), True)
    opening(0)
    second(0)
    opening(1)
    for _, _, act, ph, s in sorted(steps, key=lambda e: e[:2]):
        act(ph, s)
        if act is mid and ph == 0:
            second(s + 1)
            opening(s + 2)
    for key, copy in copies.items():
        if not isinstance(key[0], str):
            copy.wait_send()
    part = out_ref[...]
    acc[0, 0] = jnp.sum((part * part).reshape(-1, 8, 128), axis=0)
    acc[0, 1] = loss_ref[...]
    sum_everywhere(coords, acc, got, tsem, usem)
    total_ref[...] = acc[4]


def reduce_scatter(x, du, a, g, loss):
    sems = 54 * SUBS
    f32 = jnp.float32
    dma = pltpu.SemaphoreType.DMA
    vmem = pl.BlockSpec(memory_space=pltpu.VMEM)
    anywhere = pl.BlockSpec(memory_space=pl.ANY)

    _, half_at, full_at = rs_split()

    def slots(n, axes, rows):
        return pltpu.VMEM((n,) + (4,) * axes + (rows, LANES), f32)

    def landing(axes):
        return [slots(6, axes, half_at[-1]), slots(6, axes, full_at[-1])]

    part, totals, _ = pl.pallas_call(
        rs_kernel,
        out_shape=(jax.ShapeDtypeStruct((ROWS, LANES), f32), jax.ShapeDtypeStruct((2, 8, LANES), f32),
                   jax.ShapeDtypeStruct((4, 4, 4, ROWS, LANES), f32)),
        in_specs=[anywhere] * 4 + [vmem],
        out_specs=(vmem, vmem, anywhere),
        scratch_shapes=[*landing(2), slots(12, 2, 48), slots(3, 2, full_at[-1]), *landing(1), *landing(0),
                        dma((sems,)), dma((sems,)), dma((SUBS * 9,)),
                        pltpu.VMEM((5, 2, 8, LANES), f32), pltpu.VMEM((4, 4, 2, 8, LANES), f32), dma((10,)), dma((10,)),
                        pltpu.VMEM((ROWS, ROWS), BF16), pltpu.VMEM((ROWS, ROWS), BF16), pltpu.VMEM((ROWS, ROWS), BF16),
                        pltpu.VMEM((DEPTH, ROWS, COLS), BF16), pltpu.VMEM((2, 2, 4, TILE, LANES), f32),
                        pltpu.VMEM((DEPTH, 4, TILE, LANES), f32), dma((2,)), dma, dma((DEPTH,)), dma((2,)), dma((DEPTH,))],
        compiler_params=pltpu.CompilerParams(collective_id=0, has_side_effects=True, vmem_limit_bytes=63 * MIB),
        name="grad_rs",
    )(x, du, a, g, loss)
    return part, totals


def ag_split():
    table = []
    start = 0
    for c, n in enumerate((22, 21, 21)):
        first = (n + c % 2) // 2
        table.append(tuple(16 * k for k in (start, first, n - first)))
        start += n
    return table


def ag_kernel(w_ref, wide_ref, out_ref, ssem, rsem):
    coords = coords_of(lax.axis_index("data"))
    table = ag_split()
    copies = {}

    def rows(c, half):
        start, n0, n1 = table[c]
        return (start, n0) if half == 0 else (start + n0, n1)

    def region(c, unit, shift, half):
        first, second, third = AG_ORDER[c]
        idx = [None] * 3
        if unit == 0:
            idx[first], idx[second], idx[third] = wrap(coords[first] + shift), coords[second], coords[third]
        elif unit == 1:
            idx[first], idx[second], idx[third] = RING, wrap(coords[second] + shift), coords[third]
        else:
            q = wrap(coords[second] + UNIT_SHIFT[unit])
            idx[first], idx[second], idx[third] = RING, q, wrap(coords[third] + shift)
        lo, n = rows(c, half)
        return out_ref.at[tuple(idx) + (pl.ds(lo, n), ALL)]

    def start(c, unit, d, piece, src, dst):
        i = ((unit * 3 + c) * 2 + d) * 3 + piece
        target = peer(coords, AG_ORDER[c][min(unit, 2)], DELTAS[d])
        copy = pltpu.make_async_remote_copy(src_ref=src, dst_ref=dst, send_sem=ssem.at[i], recv_sem=rsem.at[i],
                                            device_id={"data": target}, device_id_type=MESH)
        copy.start()
        copies[c, unit, d, piece] = copy

    def begin(unit):
        for c in AXES:
            for d in BOTH:
                for piece, half in ((0, d), (1, 1 - d)):
                    lo, n = rows(c, half)
                    here = region(c, unit, 0, half)
                    src = w_ref.at[pl.ds(lo, n), :] if unit == 0 else here
                    start(c, unit, d, piece, src, here)

    def middle(unit):
        for c in AXES:
            for d in BOTH:
                copies[c, unit, d, 0].wait_recv()
                part = region(c, unit, -DELTAS[d], d)
                start(c, unit, d, 2, part, part)

    def arrive(unit, piece):
        for c in AXES:
            for d in BOTH:
                copies[c, unit, d, piece].wait_recv()

    def pack(unit, *shifts):
        for shift in shifts:
            for c in AXES:
                start, n0, n1 = table[c]
                _, second, third = AG_ORDER[c]
                at = {second: wrap(coords[second] + UNIT_SHIFT[unit]), third: wrap(coords[third] + shift)}

                def body(t, carry, at=at, start=start, n=n0 + n1):
                    where = tuple(at.get(p, t) for p in AXES)
                    z, y, x = where
                    base = (z * 16 + y * 4 + x) * PIECE + start * LANES
                    for k in range(n // 16):
                        line = out_ref[where + (pl.ds(start + k * 16, 16), ALL)].astype(F32)
                        line = line.reshape(1, 2 * ROWS).astype(BF16)
                        wide_ref[:, pl.ds(pl.multiple_of(base + k * 2 * ROWS, 2 * ROWS), 2 * ROWS)] = line
                    return carry

                lax.fori_loop(0, 4, body, 0)

    greet(coords, DELTAS, False)
    begin(0)
    out_ref[tuple(coords)] = w_ref[...]
    middle(0)
    arrive(0, 1)
    arrive(0, 2)
    begin(1)
    begin(2)
    pack(2, 0)
    middle(1)
    arrive(1, 1)
    begin(3)
    begin(4)
    middle(2)
    pack(3, 0)
    pack(4, 0)
    arrive(1, 2)
    begin(5)
    pack(5, 0)
    for unit in UNIT_SHIFT:
        if unit + 1 in UNIT_SHIFT:
            middle(unit + 1)
        arrive(unit, 1)
        pack(unit, *DELTAS)
        arrive(unit, 2)
        pack(unit, 2)
    for copy in copies.values():
        copy.wait_send()


def all_gather_rows(w):
    dma = pltpu.SemaphoreType.DMA
    sems = 36 * 3
    return pl.pallas_call(
        ag_kernel,
        out_shape=pltpu.VMEM((1, 64 * w.size), BF16),
        in_specs=[pl.BlockSpec(memory_space=pltpu.VMEM)],
        out_specs=pl.BlockSpec(memory_space=pltpu.VMEM),
        scratch_shapes=[pltpu.VMEM((4, 4, 4, ROWS, LANES), w.dtype), dma((sems,)), dma((sems,))],
        compiler_params=pltpu.CompilerParams(collective_id=1, has_side_effects=True, vmem_limit_bytes=24 * MIB),
        name="weight_ag",
    )(w)


def dot32(a, b, dims=((1,), (0,))):
    return lax.dot_general(a, b, (dims, ((), ())), preferred_element_type=F32)


def dot_t(a, b):
    return dot32(a, b, ((1,), (1,)))


def block_kernel(scale, w_ref, xin_ref, t_ref, x_out, a_out, du_out, g_out, loss_ref,
                 w1, w2, xb, hb, gb, ab, db, tb, raw, wide, wsem, insem, outsem, hs, hr, gs, gr):
    stage = lax.axis_index("stage")
    first = stage == 0
    last = stage == 1
    other = {"stage": 1 - stage}

    def chunk(i):
        return pltpu.make_async_copy(w_ref.at[:, pl.ds(pl.multiple_of(i * PIECE, PIECE), PIECE)], raw.at[lax.rem(i, SLOTS)],
                                     wsem.at[lax.rem(i, SLOTS)])

    load_x = pltpu.make_async_copy(xin_ref, xb, insem.at[0])
    load_t = pltpu.make_async_copy(t_ref, tb, insem.at[1])

    def prefetch(i, carry):
        chunk(i).start()
        return carry

    lax.fori_loop(0, SLOTS, prefetch, 0)

    @pl.when(first)
    def _():
        load_x.start()

    @pl.when(last)
    def _():
        load_t.start()

    barrier = pltpu.get_barrier_semaphore()
    pl.semaphore_signal(barrier, inc=1, device_id=other, device_id_type=MESH)
    pl.semaphore_wait(barrier, 1)

    def convert(i, weight, blocks, pitch):
        rows = PIECE // (blocks * LANES)
        chunk(i).wait()

        slot = lax.rem(i, SLOTS)
        for j in range(PIECE // ROWS):
            line = raw[slot, :, j * ROWS:(j + 1) * ROWS]
            at = (j * 8 // blocks) * pitch + j * 8 % blocks
            wide[at:at + 8, :] = line.astype(F32).reshape(8, LANES)
        base = pl.ds(pl.multiple_of(lax.rem(i, CHUNKS // 2) * rows, rows), rows)
        for cb in range(blocks):
            weight[cb, base, :] = wide[pl.ds(cb, rows, stride=pitch), :].astype(BF16)

        @pl.when(i < CHUNKS - SLOTS)
        def _():
            chunk(i + SLOTS).start()

    def convert_first(i, carry):
        convert(i, w1, WIDE // LANES, PITCH)
        return carry

    def convert_second(i, carry):
        convert(i, w2, ROWS // LANES, ROWS // LANES)
        return carry

    lax.fori_loop(0, CHUNKS // 2, convert_first, 0)
    lax.fori_loop(CHUNKS // 2, CHUNKS, convert_second, 0)

    @pl.when(first)
    def _():
        load_x.wait()

    @pl.when(last)
    def _():
        load_t.wait()

    def span(i):
        return pl.ds(pl.multiple_of(i * TILE, TILE), TILE)

    def cols(j):
        return pl.ds(pl.multiple_of(j * COLS, COLS), COLS)

    def blocks(j):
        return [j * (COLS // LANES) + q for q in range(COLS // LANES)]

    def beside(weight, which, part):
        return jnp.concatenate([weight[cb, part, :] for cb in which], axis=1)

    def send_h(i):
        return pltpu.make_async_remote_copy(src_ref=hb.at[span(i)], dst_ref=xb.at[span(i)], send_sem=hs.at[i], recv_sem=hr.at[i],
                                            device_id=other, device_id_type=MESH)

    def send_g(i):
        return pltpu.make_async_remote_copy(src_ref=hb.at[span(i)], dst_ref=gb.at[span(i)], send_sem=gs.at[i], recv_sem=gr.at[i],
                                            device_id=other, device_id_type=MESH)

    def outputs(i):
        pairs = ((xb, x_out), (ab, a_out), (db, du_out), (gb, g_out))
        return [pltpu.make_async_copy(src.at[span(i)], dst.at[span(i)], outsem.at[i * 4 + k]) for k, (src, dst) in enumerate(pairs)]

    def forward(i):
        def up(j, carry):
            u = dot32(xb[span(i), :], beside(w1, blocks(j), ALL)).astype(BF16)
            db[span(i), cols(j)] = u
            uf = u.astype(F32)
            half = 0.5 * uf
            ab[span(i), cols(j)] = (half + half * jnp.tanh(uf * (GELU_A + GELU_B * (uf * uf)))).astype(BF16)
            return carry

        def down(j, carry):
            hb[span(i), cols(j)] = (xb[span(i), cols(j)].astype(F32) + dot32(ab[span(i), :], beside(w2, blocks(j), ALL))).astype(BF16)
            return carry

        lax.fori_loop(0, WIDE // COLS, up, 0, unroll=2)
        lax.fori_loop(0, ROWS // COLS, down, 0)

    def top(i):
        res = hb[span(i), :].astype(F32) - tb[span(i), :].astype(F32)
        gb[span(i), :] = (res * scale).astype(BF16)
        sums = jnp.sum((res * res).reshape(-1, 8, ROWS), axis=0)
        loss_ref[...] += sum(sums[:, k * LANES:(k + 1) * LANES] for k in range(ROWS // LANES))

    def backward(i):
        def body(j, carry):
            e = dot_t(gb[span(i), :], beside(w2, range(ROWS // LANES), cols(j)))
            u = db[span(i), cols(j)].astype(F32)
            sq = u * u
            gate = 0.5 + 0.5 * jnp.tanh(u * (GELU_A + GELU_B * sq))
            slope = gate + gate * ((1.0 - gate) * (u * (2.0 * GELU_A + (6.0 * GELU_B) * sq)))
            db[span(i), cols(j)] = (e * slope).astype(BF16)
            return carry

        lax.fori_loop(0, WIDE // COLS, body, 0, unroll=2)

    def below(i):
        def body(j, carry):
            hb[span(i), cols(j)] = (gb[span(i), cols(j)].astype(F32) + dot_t(db[span(i), :], beside(w1, range(WIDE // LANES), cols(j)))).astype(BF16)
            return carry

        lax.fori_loop(0, ROWS // COLS, body, 0)

    loss_ref[...] = jnp.zeros_like(loss_ref)

    def tick(it, carry):
        i = lax.rem(it, STEPS)

        @pl.when(it < STEPS)
        def _():
            @pl.when(last)
            def _():
                send_h(i).wait_recv()

            forward(i)

            @pl.when(first)
            def _():
                send_h(i).start()

            @pl.when(last)
            def _():
                top(i)

        @pl.when(it // STEPS + stage == 1)
        def _():
            @pl.when(first)
            def _():
                send_g(i).wait_recv()

            backward(i)

            @pl.when(last)
            def _():
                below(i)
                send_g(i).start()

            for copy in outputs(i):
                copy.start()
        return carry

    lax.fori_loop(0, 2 * STEPS, tick, 0)

    def drain(i, carry):
        @pl.when(first)
        def _():
            send_h(i).wait_send()

        @pl.when(last)
        def _():
            send_g(i).wait_send()

        for copy in outputs(i):
            copy.wait()
        return carry

    lax.fori_loop(0, STEPS, drain, 0)


def block_passes(flat, x_in, targets, token_count):
    anywhere = pl.BlockSpec(memory_space=pl.ANY)
    dma = pltpu.SemaphoreType.DMA
    narrow, wide = (ROWS, ROWS), (ROWS, WIDE)

    def shape(dims):
        return jax.ShapeDtypeStruct(dims, BF16)

    def room(dims):
        return pltpu.VMEM(dims, BF16)

    return pl.pallas_call(
        functools.partial(block_kernel, 1.0 / token_count),
        out_shape=(shape(narrow), shape(wide), shape(wide), shape(narrow), jax.ShapeDtypeStruct((8, LANES), F32)),
        in_specs=[anywhere] * 3,
        out_specs=(anywhere,) * 4 + (pl.BlockSpec(memory_space=pltpu.VMEM),),
        scratch_shapes=[room((WIDE // LANES, ROWS, LANES)), room((ROWS // LANES, WIDE, LANES)), room(narrow), room(narrow), room(narrow), room(wide), room(wide), room(narrow),
                        room((SLOTS, 1, PIECE)), pltpu.VMEM((32 * PITCH, LANES), F32),
                        dma((SLOTS,)), dma((2,)), dma((STEPS * 4,)), dma((STEPS,)), dma((STEPS,)), dma((STEPS,)), dma((STEPS,))],
        compiler_params=pltpu.CompilerParams(collective_id=2, has_side_effects=True, vmem_limit_bytes=60 * MIB),
        name="block",
    )(flat, x_in, targets)


def adam_kernel(rate, token_count, part_ref, total_ref, tau_ref, w_ref, m_ref, v_ref, w_out, m_out, v_out, b_out, loss_out, grad):
    early = lax.axis_index("data") < 32

    def reorder(rows):
        blocks = ROWS // rows
        for r in range(rows):
            grad[r * blocks:(r + 1) * blocks, :] = part_ref[pl.ds(r, blocks, stride=rows), :]

    @pl.when(early)
    def _():
        reorder(32)

    @pl.when(jnp.logical_not(early))
    def _():
        reorder(LANES)

    nu = jnp.sqrt(jnp.sum(total_ref[0], keepdims=True))
    scaled = jnp.minimum(1.0, tau_ref[...] / nu) * grad[...]
    m_new = ADAM_BETA1 * m_ref[...] + (1.0 - ADAM_BETA1) * scaled
    v_new = ADAM_BETA2 * v_ref[...] + (1.0 - ADAM_BETA2) * scaled * scaled
    m_hat = m_new / (1.0 - ADAM_BETA1 ** ADAM_STEP)
    v_hat = v_new / (1.0 - ADAM_BETA2 ** ADAM_STEP)
    w_new = w_ref[...] - rate * (m_hat / (jnp.sqrt(v_hat) + ADAM_EPS) + WEIGHT_DECAY * w_ref[...])
    w_out[...] = w_new
    m_out[...] = m_new
    v_out[...] = v_new
    b_out[...] = w_new.astype(BF16)
    loss_out[...] = (0.5 * jnp.sum(total_ref[1], keepdims=True)) / token_count


def adam(rate, token_count, part, totals, tau, w, m, v):
    state = jax.ShapeDtypeStruct(part.shape, F32)
    vmem = pl.BlockSpec(memory_space=pltpu.VMEM)
    return pl.pallas_call(
        functools.partial(adam_kernel, rate, token_count),
        out_shape=(state, state, state, jax.ShapeDtypeStruct(part.shape, BF16), jax.ShapeDtypeStruct((1, 1), F32)),
        in_specs=[vmem] * 6,
        out_specs=(vmem,) * 5,
        scratch_shapes=[pltpu.VMEM(part.shape, F32)],
        name="adam",
    )(part, totals, tau, w, m, v)


def solution(mesh):
    data_size = mesh.shape['data']

    def device_step(x_in, targets, w_work, w_master, m_prior, v_prior, clip_tau):
        token_count = x_in.shape[0] * x_in.shape[1] * data_size
        x, a, du, g, loss = block_passes(w_work.reshape(1, -1), x_in.reshape(ROWS, ROWS), targets.reshape(ROWS, ROWS), token_count)
        part, totals = reduce_scatter(x, du, a, g, loss)
        rate = LR_BASE / math.sqrt(x_in.shape[-1])
        state = [z.reshape(ROWS, LANES) for z in (w_master, m_prior, v_prior)]
        w_new, m_new, v_new, w_bf, loss_mean = adam(rate, token_count, part, totals, clip_tau.reshape(1, 1), *state)
        w_all = all_gather_rows(w_bf).reshape(w_work.shape)
        return (loss_mean.reshape(()), w_all) + tuple(z.reshape(w_master.shape) for z in (w_new, m_new, v_new))

    row_spec = P(None, 'data', None)
    shard_spec = P('stage', None, 'data')
    stage_spec = P('stage', None, None)
    return jax.shard_map(device_step, mesh=mesh, in_specs=(row_spec, row_spec, stage_spec, shard_spec, shard_spec, shard_spec, P()), out_specs=(P(), stage_spec, shard_spec, shard_spec, shard_spec), check_vma=False)
```

```python
import functools
import math
import jax
import jax.numpy as jnp
from jax import lax
from jax.experimental import pallas as pl
from jax.experimental.pallas import tpu as pltpu
from jax.sharding import PartitionSpec as P

ADAM_BETA1 = 0.9
ADAM_BETA2 = 0.95
ADAM_EPS = 1e-8
WEIGHT_DECAY = 0.1
ADAM_STEP = 10
LR_BASE = 0.05
MESH = pl.DeviceIdType.MESH
MIB = 1024 * 1024

UNITS = (1, 2, 2, 2, 1)
DELAY = 30
DEPTH = 4
SUBS = len(UNITS)
ALL = slice(None)
RING = pl.ds(0, 4)
BOTH = range(2)
AXES = range(3)
LEADS = (16, 4, 1)
ROWWISE = ((0,), (0,))
DELTAS = (1, -1)
RS_ORDER = ((2, 1, 0), (1, 0, 2), (0, 2, 1))
UNIT_SHIFT = {2: 0, 3: -1, 4: 1, 5: 2}
AG_ORDER = ((0, 1, 2), (1, 2, 0), (2, 0, 1))


ROWS = 1024
WIDE = 4096
TILE = 256
COLS = 512
LANES = 128
STEPS = ROWS // TILE
PIECE = 131072
CHUNKS = 2 * ROWS * WIDE // PIECE
SLOTS = 16
PITCH = 40
GELU_A = math.sqrt(2.0 / math.pi)
GELU_B = GELU_A * 0.044715
BF16 = jnp.bfloat16
F32 = jnp.float32


def upto(n):
    return pl.ds(0, n)


def divide(t):
    return t // 4, lax.rem(t, 4)


def wrap(k):
    return lax.rem(k + 4, 4)


def rs_split():
    table, half_at, full_at = {}, [0], [0]
    start = 0
    for s, units in enumerate(UNITS):
        most = 0
        for c in AXES:
            n = (16 * units + (c + s) % 3) // 3
            first = (n + (s + c) % 2) // 2
            table[s, c] = tuple(8 * k for k in (start, first, n - first))
            start += n
            most = max(most, n)
        half_at.append(half_at[s] + (most + 1) // 2 * 8)
        full_at.append(full_at[s] + most * 8)
    return table, half_at, full_at


def coords_of(me):
    return [me // 16, lax.rem(me // 4, 4), lax.rem(me, 4)]


def peer(coords, pos, delta):
    moved = list(coords)
    moved[pos] = wrap(coords[pos] + delta)
    z, y, x = moved
    return z * 16 + y * 4 + x


def greet(coords, deltas, partner):
    barrier = pltpu.get_barrier_semaphore()
    ids = [{"data": peer(coords, pos, delta)} for pos in AXES for delta in deltas]
    if partner:
        ids.append({"stage": 1 - lax.axis_index("stage")})
    for other in ids:
        pl.semaphore_signal(barrier, inc=1, device_id=other, device_id_type=MESH)
    pl.semaphore_wait(barrier, len(ids))


def sum_everywhere(coords, acc, got, ssem, rsem):
    copies = []
    for ph in range(4):
        if ph < 3:
            mine = coords[ph]
            targets = [{"data": peer(coords, ph, k)} for k in range(1, 4)]
        else:
            mine = lax.axis_index("stage")
            targets = [{"stage": 1 - mine}]
        batch = []
        for k, target in enumerate(targets):
            i = ph * 3 + k
            batch.append(pltpu.make_async_remote_copy(src_ref=acc.at[ph], dst_ref=got.at[ph, mine], send_sem=ssem.at[i],
                                                      recv_sem=rsem.at[i], device_id=target, device_id_type=MESH))
        for copy in batch:
            copy.start()
        got[ph, mine] = acc[ph]
        for copy in batch:
            copy.wait_recv()
        acc[ph + 1] = sum(got[ph, k] for k in range(len(batch) + 1))
        copies += batch
    for copy in copies:
        copy.wait_send()


def rs_kernel(x_ref, du_ref, a_ref, top_ref, loss_ref, out_ref, total_ref, g_ref, ra1, rb1, lb, own, ra2, rb2, ra3, rb3, ssem, rsem, lsem,
              acc, got, tsem, usem, xb, gb, dub, ab, put1, put2, insem, dusem, asem, psem1, psem2):
    coords = coords_of(lax.axis_index("data"))
    table, half_at, full_at = rs_split()
    ra = (ra1, ra2, ra3)
    rb = (rb1, rb2, rb3)
    copies = {}

    load_x = pltpu.make_async_copy(x_ref, xb, insem.at[0])
    load_g = pltpu.make_async_copy(top_ref, gb, insem.at[1])

    def load_du(s):
        width = UNITS[s] * COLS
        return pltpu.make_async_copy(du_ref.at[:, pl.ds(sum(UNITS[:s]) * COLS, width)], dub.at[:, upto(width)], dusem)

    def load_a(m):
        return pltpu.make_async_copy(a_ref.at[:, pl.ds(pl.multiple_of(m * COLS, COLS), COLS)], ab.at[lax.rem(m, DEPTH)],
                                     asem.at[lax.rem(m, DEPTH)])

    def first_blocks():
        for m in range(DEPTH - 1):
            load_a(m).start()

    def grads(s):
        size = UNITS[s] * LANES
        band = pl.ds(sum(UNITS[:s]) * LANES, size)
        width = UNITS[s] * COLS
        if s:
            first_blocks()
        load_du(s).wait()
        if s == 0:
            load_x.wait()
            load_g.wait()

        def write1(m):
            return pltpu.make_async_copy(put1.at[lax.rem(m, 2), :, :, upto(size)], g_ref.at[m // 2, pl.ds(lax.rem(m, 2) * 2, 2), :, band, :],
                                         psem1.at[lax.rem(m, 2)])

        def write2(m):
            return pltpu.make_async_copy(put2.at[lax.rem(m, DEPTH), :, upto(size)], g_ref.at[m // 4 + 2, lax.rem(m, 4), :, band, :],
                                         psem2.at[lax.rem(m, DEPTH)])

        def first(m, carry):
            val = dot32(xb[:, pl.ds(pl.multiple_of(m * TILE, TILE), TILE)], dub[:, upto(width)], ROWWISE)

            @pl.when(m > 1)
            def _():
                write1(m - 2).wait()

            for ct in range(width // LANES):
                put1[lax.rem(m, 2), :, :, ct * 32:(ct + 1) * 32, :] = val[:, ct * LANES:(ct + 1) * LANES].reshape(2, 4, 32, LANES)
            write1(m).start()
            return carry

        def second(m, carry):
            load_a(m).wait()

            @pl.when(m < WIDE // COLS - DEPTH + 1)
            def _():
                load_a(m + DEPTH - 1).start()

            val = dot32(ab[lax.rem(m, DEPTH)], gb[:, band], ROWWISE)

            @pl.when(m >= DEPTH)
            def _():
                write2(m - DEPTH).wait()

            for ct in range(UNITS[s]):
                part = slice(ct * LANES, (ct + 1) * LANES)
                put2[lax.rem(m, DEPTH), :, part, :] = val[:, part].reshape(4, LANES, LANES)
            write2(m).start()
            return carry

        lax.fori_loop(0, 4, first, 0)
        if s + 1 < SUBS:
            load_du(s + 1).start()
        lax.fori_loop(0, WIDE // COLS, second, 0)
        for m in BOTH:
            write1(m + 2).wait()
        for m in range(DEPTH):
            write2(m + WIDE // COLS - DEPTH).wait()

    def rows(s, c, half):
        start, n0, n1 = table[s, c]
        if half == 0:
            return 0, n0
        if half == 1:
            return n0, n1
        return 0, n0 + n1

    def lead(ph, c, k):
        order = RS_ORDER[c]
        left = [p for p in AXES if p != order[0]]
        idx = []
        for p in left:
            if ph == 1:
                idx.append(k if p == order[1] else RING)
            else:
                idx.append(coords[order[1]] if p == order[1] else k)
        return tuple(idx)

    def lead_t(ph, c, k, t):
        if ph == 0:
            return divide(t), divide(t)
        mine = tuple(t if i is RING else i for i in lead(ph, c, k))
        return (t,) * (2 - ph), mine

    def source(ph, s, c, k, half):
        lo, n = rows(s, c, half)
        if ph == 0:
            idx = [RING] * 3
            idx[RS_ORDER[c][0]] = k
            return g_ref.at[tuple(idx) + (pl.ds(table[s, c][0] + lo, n), ALL)]
        return own.at[(c,) + lead(ph, c, k) + (pl.ds(full_at[s] + lo, n), ALL)]

    def slot(ref, ph, i, lo, n):
        return ref.at[(i,) + (RING,) * (2 - ph) + (pl.ds(lo, n), ALL)]

    def start(ph, s, c, d, piece, src, dst):
        i = (((ph * SUBS + s) * 3 + c) * 2 + d) * 3 + piece
        target = peer(coords, RS_ORDER[c][ph], DELTAS[d])
        copy = pltpu.make_async_remote_copy(src_ref=src, dst_ref=dst, send_sem=ssem.at[i], recv_sem=rsem.at[i],
                                            device_id={"data": target}, device_id_type=MESH)
        copy.start()
        copies[ph, s, c, d, piece] = copy

    def at(c, ph, delta):
        return wrap(coords[RS_ORDER[c][ph]] + delta)

    def send_a(ph, s, c):
        for d in BOTH:
            n = rows(s, c, d)[1]
            start(ph, s, c, d, 0, source(ph, s, c, at(c, ph, 2), d), slot(ra[ph], ph, c * 2 + d, half_at[s], n))

    def send_b1(ph, s, c):
        for d in BOTH:
            lo, n = rows(s, c, 1 - d)
            start(ph, s, c, d, 1, source(ph, s, c, at(c, ph, DELTAS[d]), 1 - d), slot(rb[ph], ph, c * 2 + d, full_at[s] + lo, n))

    def load(s, c):
        for d in BOTH:
            i = s * 9 + c * 3 + d
            n = rows(s, c, d)[1]
            copy = pltpu.make_async_copy(source(0, s, c, at(c, 0, DELTAS[d]), d), slot(lb, 0, s % 2 * 6 + c * 2 + d, 0, n), lsem.at[i])
            copy.start()
            copies["lb", s, c, d] = copy
        n = rows(s, c, 2)[1]
        copy = pltpu.make_async_copy(source(0, s, c, at(c, 0, 0), 2), slot(own, 0, c, full_at[s], n), lsem.at[s * 9 + c * 3 + 2])
        copy.start()
        copies["own", s, c] = copy

    def forward(ph, s, c):
        for d in BOTH:
            i = c * 2 + d
            lo, n = rows(s, c, d)
            if ph == 0:
                copies["lb", s, c, d].wait()
            copies[ph, s, c, d, 0].wait_recv()
            buf = ra[ph]
            k = at(c, ph, DELTAS[d])

            def body(t, carry, d=d, i=i, n=n, lo=lo, buf=buf, k=k):
                where, mine = lead_t(ph, c, k, t)
                term = lb[(s % 2 * 6 + c * 2 + d,) + where + (upto(n), ALL)] if ph == 0 else own[(c,) + mine + (pl.ds(full_at[s] + lo, n), ALL)]
                buf[(i,) + where + (pl.ds(half_at[s], n), ALL)] += term
                return carry

            lax.fori_loop(0, LEADS[ph], body, 0)
            start(ph, s, c, d, 2, slot(buf, ph, i, half_at[s], n), slot(rb[ph], ph, i, full_at[s] + lo, n))

    def finish(ph, s, c):
        if ph == 0:
            copies["own", s, c].wait()
        for d in BOTH:
            copies[ph, s, c, d, 1].wait_recv()
            copies[ph, s, c, d, 2].wait_recv()
        n = rows(s, c, 2)[1]
        i = c * 2
        buf = rb[ph]
        k = at(c, ph, 0)
        span = pl.ds(full_at[s], n)

        def body(t, carry):
            where, mine = lead_t(ph, c, k, t)
            mine = (c,) + mine + (span, ALL)
            total = own[mine] + buf[(i,) + where + (span, ALL)] + buf[(i + 1,) + where + (span, ALL)]
            if ph < 2:
                own[mine] = total
            else:
                out_ref[pl.ds(table[s, c][0], n), :] = total
            return carry

        lax.fori_loop(0, LEADS[ph], body, 0)

    def st0(s):
        for c in AXES:
            send_a(0, s, c)
            load(s, c)

    def st0b(s):
        for c in AXES:
            send_b1(0, s, c)

    def mid(ph, s):
        for c in AXES:
            forward(ph, s, c)

    def turn(ph, s):
        for c in AXES:
            finish(ph, s, c)
            if ph < 2:
                send_a(ph + 1, s, c)
                send_b1(ph + 1, s, c)

    def opening(s):
        if s < SUBS:
            grads(s)
            st0(s)

    def second(s):
        if s < SUBS:
            st0b(s)

    queue = [(mid, 0), (None, 0), (mid, 1)]
    for s in range(SUBS):
        queue += [(turn, s), (None, s + 1), (mid, s + 2)]
    steps, clock = [], 0
    for act, s in queue:
        if s < SUBS:
            clock += UNITS[s]
            steps.append((clock, 0, act, 0, s))
            if act is turn:
                for ph in range(1, 3):
                    steps.append((clock + DELAY * ph - DELAY // 2, 1, mid, ph, s))
                    steps.append((clock + DELAY * ph, 1, turn, ph, s))
    steps = [e for e in steps if e[2]]
    load_x.start()
    load_du(0).start()
    load_g.start()
    first_blocks()
    greet(coords, range(1, 4), True)
    opening(0)
    second(0)
    opening(1)
    for _, _, act, ph, s in sorted(steps, key=lambda e: e[:2]):
        act(ph, s)
        if act is mid and ph == 0:
            second(s + 1)
            opening(s + 2)
    for key, copy in copies.items():
        if not isinstance(key[0], str):
            copy.wait_send()
    part = out_ref[...]
    acc[0, 0] = jnp.sum((part * part).reshape(-1, 8, 128), axis=0)
    acc[0, 1] = loss_ref[...]
    sum_everywhere(coords, acc, got, tsem, usem)
    total_ref[...] = acc[4]


def reduce_scatter(x, du, a, g, loss):
    sems = 54 * SUBS
    f32 = jnp.float32
    dma = pltpu.SemaphoreType.DMA
    vmem = pl.BlockSpec(memory_space=pltpu.VMEM)
    anywhere = pl.BlockSpec(memory_space=pl.ANY)

    _, half_at, full_at = rs_split()

    def slots(n, axes, rows):
        return pltpu.VMEM((n,) + (4,) * axes + (rows, LANES), f32)

    def landing(axes):
        return [slots(6, axes, half_at[-1]), slots(6, axes, full_at[-1])]

    part, totals, _ = pl.pallas_call(
        rs_kernel,
        out_shape=(jax.ShapeDtypeStruct((ROWS, LANES), f32), jax.ShapeDtypeStruct((2, 8, LANES), f32),
                   jax.ShapeDtypeStruct((4, 4, 4, ROWS, LANES), f32)),
        in_specs=[anywhere] * 4 + [vmem],
        out_specs=(vmem, vmem, anywhere),
        scratch_shapes=[*landing(2), slots(12, 2, 48), slots(3, 2, full_at[-1]), *landing(1), *landing(0),
                        dma((sems,)), dma((sems,)), dma((SUBS * 9,)),
                        pltpu.VMEM((5, 2, 8, LANES), f32), pltpu.VMEM((4, 4, 2, 8, LANES), f32), dma((10,)), dma((10,)),
                        pltpu.VMEM((ROWS, ROWS), BF16), pltpu.VMEM((ROWS, ROWS), BF16), pltpu.VMEM((ROWS, ROWS), BF16),
                        pltpu.VMEM((DEPTH, ROWS, COLS), BF16), pltpu.VMEM((2, 2, 4, TILE, LANES), f32),
                        pltpu.VMEM((DEPTH, 4, TILE, LANES), f32), dma((2,)), dma, dma((DEPTH,)), dma((2,)), dma((DEPTH,))],
        compiler_params=pltpu.CompilerParams(collective_id=0, has_side_effects=True, vmem_limit_bytes=63 * MIB),
        name="grad_rs",
    )(x, du, a, g, loss)
    return part, totals


def ag_split():
    table = []
    start = 0
    for c, n in enumerate((22, 21, 21)):
        first = (n + c % 2) // 2
        table.append(tuple(16 * k for k in (start, first, n - first)))
        start += n
    return table


def ag_kernel(w_ref, wide_ref, out_ref, ssem, rsem):
    coords = coords_of(lax.axis_index("data"))
    table = ag_split()
    copies = {}

    def rows(c, half):
        start, n0, n1 = table[c]
        return (start, n0) if half == 0 else (start + n0, n1)

    def region(c, unit, shift, half):
        first, second, third = AG_ORDER[c]
        idx = [None] * 3
        if unit == 0:
            idx[first], idx[second], idx[third] = wrap(coords[first] + shift), coords[second], coords[third]
        elif unit == 1:
            idx[first], idx[second], idx[third] = RING, wrap(coords[second] + shift), coords[third]
        else:
            q = wrap(coords[second] + UNIT_SHIFT[unit])
            idx[first], idx[second], idx[third] = RING, q, wrap(coords[third] + shift)
        lo, n = rows(c, half)
        return out_ref.at[tuple(idx) + (pl.ds(lo, n), ALL)]

    def start(c, unit, d, piece, src, dst):
        i = ((unit * 3 + c) * 2 + d) * 3 + piece
        target = peer(coords, AG_ORDER[c][min(unit, 2)], DELTAS[d])
        copy = pltpu.make_async_remote_copy(src_ref=src, dst_ref=dst, send_sem=ssem.at[i], recv_sem=rsem.at[i],
                                            device_id={"data": target}, device_id_type=MESH)
        copy.start()
        copies[c, unit, d, piece] = copy

    def begin(unit):
        for c in AXES:
            for d in BOTH:
                for piece, half in ((0, d), (1, 1 - d)):
                    lo, n = rows(c, half)
                    here = region(c, unit, 0, half)
                    src = w_ref.at[pl.ds(lo, n), :] if unit == 0 else here
                    start(c, unit, d, piece, src, here)

    def middle(unit):
        for c in AXES:
            for d in BOTH:
                copies[c, unit, d, 0].wait_recv()
                part = region(c, unit, -DELTAS[d], d)
                start(c, unit, d, 2, part, part)

    def arrive(unit, piece):
        for c in AXES:
            for d in BOTH:
                copies[c, unit, d, piece].wait_recv()

    def pack(unit, *shifts):
        for shift in shifts:
            for c in AXES:
                start, n0, n1 = table[c]
                _, second, third = AG_ORDER[c]
                at = {second: wrap(coords[second] + UNIT_SHIFT[unit]), third: wrap(coords[third] + shift)}

                def body(t, carry, at=at, start=start, n=n0 + n1):
                    where = tuple(at.get(p, t) for p in AXES)
                    z, y, x = where
                    base = (z * 16 + y * 4 + x) * PIECE + start * LANES
                    for k in range(n // 16):
                        line = out_ref[where + (pl.ds(start + k * 16, 16), ALL)].astype(F32)
                        line = line.reshape(1, 2 * ROWS).astype(BF16)
                        wide_ref[:, pl.ds(pl.multiple_of(base + k * 2 * ROWS, 2 * ROWS), 2 * ROWS)] = line
                    return carry

                lax.fori_loop(0, 4, body, 0)

    greet(coords, DELTAS, False)
    begin(0)
    out_ref[tuple(coords)] = w_ref[...]
    middle(0)
    arrive(0, 1)
    arrive(0, 2)
    begin(1)
    begin(2)
    pack(2, 0)
    middle(1)
    arrive(1, 1)
    begin(3)
    begin(4)
    middle(2)
    pack(3, 0)
    pack(4, 0)
    arrive(1, 2)
    begin(5)
    pack(5, 0)
    for unit in UNIT_SHIFT:
        if unit > 2:
            middle(unit)
        arrive(unit, 1)
        pack(unit, *DELTAS)
    for unit in UNIT_SHIFT:
        arrive(unit, 2)
        pack(unit, 2)
    for copy in copies.values():
        copy.wait_send()


def all_gather_rows(w):
    dma = pltpu.SemaphoreType.DMA
    sems = 36 * 3
    return pl.pallas_call(
        ag_kernel,
        out_shape=pltpu.VMEM((1, 64 * w.size), BF16),
        in_specs=[pl.BlockSpec(memory_space=pltpu.VMEM)],
        out_specs=pl.BlockSpec(memory_space=pltpu.VMEM),
        scratch_shapes=[pltpu.VMEM((4, 4, 4, ROWS, LANES), w.dtype), dma((sems,)), dma((sems,))],
        compiler_params=pltpu.CompilerParams(collective_id=1, has_side_effects=True, vmem_limit_bytes=24 * MIB),
        name="weight_ag",
    )(w)


def dot32(a, b, dims=((1,), (0,))):
    return lax.dot_general(a, b, (dims, ((), ())), preferred_element_type=F32)


def dot_t(a, b):
    return dot32(a, b, ((1,), (1,)))


def block_kernel(scale, w_ref, xin_ref, t_ref, x_out, a_out, du_out, g_out, loss_ref,
                 w1, w2, xb, hb, gb, ab, db, tb, raw, wide, wsem, insem, outsem, hs, hr, gs, gr):
    stage = lax.axis_index("stage")
    first = stage == 0
    last = stage == 1
    other = {"stage": 1 - stage}

    def chunk(i):
        return pltpu.make_async_copy(w_ref.at[:, pl.ds(pl.multiple_of(i * PIECE, PIECE), PIECE)], raw.at[lax.rem(i, SLOTS)],
                                     wsem.at[lax.rem(i, SLOTS)])

    load_x = pltpu.make_async_copy(xin_ref, xb, insem.at[0])
    load_t = pltpu.make_async_copy(t_ref, tb, insem.at[1])

    def prefetch(i, carry):
        chunk(i).start()
        return carry

    lax.fori_loop(0, SLOTS, prefetch, 0)

    @pl.when(first)
    def _():
        load_x.start()

    @pl.when(last)
    def _():
        load_t.start()

    barrier = pltpu.get_barrier_semaphore()
    pl.semaphore_signal(barrier, inc=1, device_id=other, device_id_type=MESH)
    pl.semaphore_wait(barrier, 1)

    def convert(i, weight, blocks, pitch):
        rows = PIECE // (blocks * LANES)
        chunk(i).wait()

        slot = lax.rem(i, SLOTS)
        for j in range(PIECE // ROWS):
            line = raw[slot, :, j * ROWS:(j + 1) * ROWS]
            at = (j * 8 // blocks) * pitch + j * 8 % blocks
            wide[at:at + 8, :] = line.astype(F32).reshape(8, LANES)
        base = pl.ds(pl.multiple_of(lax.rem(i, CHUNKS // 2) * rows, rows), rows)
        for cb in range(blocks):
            weight[cb, base, :] = wide[pl.ds(cb, rows, stride=pitch), :].astype(BF16)

        @pl.when(i < CHUNKS - SLOTS)
        def _():
            chunk(i + SLOTS).start()

    def convert_first(i, carry):
        convert(i, w1, WIDE // LANES, PITCH)
        return carry

    def convert_second(i, carry):
        convert(i, w2, ROWS // LANES, ROWS // LANES)
        return carry

    lax.fori_loop(0, CHUNKS // 2, convert_first, 0)
    lax.fori_loop(CHUNKS // 2, CHUNKS, convert_second, 0)

    @pl.when(first)
    def _():
        load_x.wait()

    @pl.when(last)
    def _():
        load_t.wait()

    def span(i):
        return pl.ds(pl.multiple_of(i * TILE, TILE), TILE)

    def cols(j):
        return pl.ds(pl.multiple_of(j * COLS, COLS), COLS)

    def blocks(j):
        return [j * (COLS // LANES) + q for q in range(COLS // LANES)]

    def beside(weight, which, part):
        return jnp.concatenate([weight[cb, part, :] for cb in which], axis=1)

    def send_h(i):
        return pltpu.make_async_remote_copy(src_ref=hb.at[span(i)], dst_ref=xb.at[span(i)], send_sem=hs.at[i], recv_sem=hr.at[i],
                                            device_id=other, device_id_type=MESH)

    def send_g(i):
        return pltpu.make_async_remote_copy(src_ref=hb.at[span(i)], dst_ref=gb.at[span(i)], send_sem=gs.at[i], recv_sem=gr.at[i],
                                            device_id=other, device_id_type=MESH)

    def outputs(i):
        pairs = ((xb, x_out), (ab, a_out), (db, du_out), (gb, g_out))
        return [pltpu.make_async_copy(src.at[span(i)], dst.at[span(i)], outsem.at[i * 4 + k]) for k, (src, dst) in enumerate(pairs)]

    def forward(i):
        def up(j, carry):
            u = dot32(xb[span(i), :], beside(w1, blocks(j), ALL)).astype(BF16)
            db[span(i), cols(j)] = u
            uf = u.astype(F32)
            half = 0.5 * uf
            ab[span(i), cols(j)] = (half + half * jnp.tanh(uf * (GELU_A + GELU_B * (uf * uf)))).astype(BF16)
            return carry

        def down(j, carry):
            hb[span(i), cols(j)] = (xb[span(i), cols(j)].astype(F32) + dot32(ab[span(i), :], beside(w2, blocks(j), ALL))).astype(BF16)
            return carry

        lax.fori_loop(0, WIDE // COLS, up, 0, unroll=2)
        lax.fori_loop(0, ROWS // COLS, down, 0)

    def top(i):
        res = hb[span(i), :].astype(F32) - tb[span(i), :].astype(F32)
        gb[span(i), :] = (res * scale).astype(BF16)
        sums = jnp.sum((res * res).reshape(-1, 8, ROWS), axis=0)
        loss_ref[...] += sum(sums[:, k * LANES:(k + 1) * LANES] for k in range(ROWS // LANES))

    def backward(i):
        def body(j, carry):
            e = dot_t(gb[span(i), :], beside(w2, range(ROWS // LANES), cols(j)))
            u = db[span(i), cols(j)].astype(F32)
            sq = u * u
            gate = 0.5 + 0.5 * jnp.tanh(u * (GELU_A + GELU_B * sq))
            slope = gate + gate * ((1.0 - gate) * (u * (2.0 * GELU_A + (6.0 * GELU_B) * sq)))
            db[span(i), cols(j)] = (e * slope).astype(BF16)
            return carry

        lax.fori_loop(0, WIDE // COLS, body, 0, unroll=2)

    def below(i):
        def body(j, carry):
            hb[span(i), cols(j)] = (gb[span(i), cols(j)].astype(F32) + dot_t(db[span(i), :], beside(w1, range(WIDE // LANES), cols(j)))).astype(BF16)
            return carry

        lax.fori_loop(0, ROWS // COLS, body, 0)

    loss_ref[...] = jnp.zeros_like(loss_ref)

    def tick(it, carry):
        i = lax.rem(it, STEPS)

        @pl.when(it < STEPS)
        def _():
            @pl.when(last)
            def _():
                send_h(i).wait_recv()

            forward(i)

            @pl.when(first)
            def _():
                send_h(i).start()

            for copy in outputs(i)[:2]:
                copy.start()

            @pl.when(last)
            def _():
                top(i)

        @pl.when(it // STEPS + stage == 1)
        def _():
            @pl.when(first)
            def _():
                send_g(i).wait_recv()

            backward(i)

            @pl.when(last)
            def _():
                below(i)
                send_g(i).start()

            for copy in outputs(i)[2:]:
                copy.start()
        return carry

    lax.fori_loop(0, 2 * STEPS, tick, 0)

    def drain(i, carry):
        @pl.when(first)
        def _():
            send_h(i).wait_send()

        @pl.when(last)
        def _():
            send_g(i).wait_send()

        for copy in outputs(i):
            copy.wait()
        return carry

    lax.fori_loop(0, STEPS, drain, 0)


def block_passes(flat, x_in, targets, token_count):
    anywhere = pl.BlockSpec(memory_space=pl.ANY)
    dma = pltpu.SemaphoreType.DMA
    narrow, wide = (ROWS, ROWS), (ROWS, WIDE)

    def shape(dims):
        return jax.ShapeDtypeStruct(dims, BF16)

    def room(dims):
        return pltpu.VMEM(dims, BF16)

    return pl.pallas_call(
        functools.partial(block_kernel, 1.0 / token_count),
        out_shape=(shape(narrow), shape(wide), shape(wide), shape(narrow), jax.ShapeDtypeStruct((8, LANES), F32)),
        in_specs=[anywhere] * 3,
        out_specs=(anywhere,) * 4 + (pl.BlockSpec(memory_space=pltpu.VMEM),),
        scratch_shapes=[room((WIDE // LANES, ROWS, LANES)), room((ROWS // LANES, WIDE, LANES)), room(narrow), room(narrow), room(narrow), room(wide), room(wide), room(narrow),
                        room((SLOTS, 1, PIECE)), pltpu.VMEM((32 * PITCH, LANES), F32),
                        dma((SLOTS,)), dma((2,)), dma((STEPS * 4,)), dma((STEPS,)), dma((STEPS,)), dma((STEPS,)), dma((STEPS,))],
        compiler_params=pltpu.CompilerParams(collective_id=2, has_side_effects=True, vmem_limit_bytes=60 * MIB),
        name="block",
    )(flat, x_in, targets)


def adam_kernel(rate, token_count, part_ref, total_ref, tau_ref, w_ref, m_ref, v_ref, w_out, m_out, v_out, b_out, loss_out, grad):
    early = lax.axis_index("data") < 32

    def reorder(rows):
        blocks = ROWS // rows
        for r in range(rows):
            grad[r * blocks:(r + 1) * blocks, :] = part_ref[pl.ds(r, blocks, stride=rows), :]

    @pl.when(early)
    def _():
        reorder(32)

    @pl.when(jnp.logical_not(early))
    def _():
        reorder(LANES)

    nu = jnp.sqrt(jnp.sum(total_ref[0], keepdims=True))
    scaled = jnp.minimum(1.0, tau_ref[...] / nu) * grad[...]
    m_new = ADAM_BETA1 * m_ref[...] + (1.0 - ADAM_BETA1) * scaled
    v_new = ADAM_BETA2 * v_ref[...] + (1.0 - ADAM_BETA2) * scaled * scaled
    m_hat = m_new / (1.0 - ADAM_BETA1 ** ADAM_STEP)
    v_hat = v_new / (1.0 - ADAM_BETA2 ** ADAM_STEP)
    w_new = w_ref[...] - rate * (m_hat / (jnp.sqrt(v_hat) + ADAM_EPS) + WEIGHT_DECAY * w_ref[...])
    w_out[...] = w_new
    m_out[...] = m_new
    v_out[...] = v_new
    b_out[...] = w_new.astype(BF16)
    loss_out[...] = (0.5 * jnp.sum(total_ref[1], keepdims=True)) / token_count


def adam(rate, token_count, part, totals, tau, w, m, v):
    state = jax.ShapeDtypeStruct(part.shape, F32)
    vmem = pl.BlockSpec(memory_space=pltpu.VMEM)
    return pl.pallas_call(
        functools.partial(adam_kernel, rate, token_count),
        out_shape=(state, state, state, jax.ShapeDtypeStruct(part.shape, BF16), jax.ShapeDtypeStruct((1, 1), F32)),
        in_specs=[vmem] * 6,
        out_specs=(vmem,) * 5,
        scratch_shapes=[pltpu.VMEM(part.shape, F32)],
        name="adam",
    )(part, totals, tau, w, m, v)


def solution(mesh):
    data_size = mesh.shape['data']

    def device_step(x_in, targets, w_work, w_master, m_prior, v_prior, clip_tau):
        token_count = x_in.shape[0] * x_in.shape[1] * data_size
        x, a, du, g, loss = block_passes(w_work.reshape(1, -1), x_in.reshape(ROWS, ROWS), targets.reshape(ROWS, ROWS), token_count)
        part, totals = reduce_scatter(x, du, a, g, loss)
        rate = LR_BASE / math.sqrt(x_in.shape[-1])
        state = [z.reshape(ROWS, LANES) for z in (w_master, m_prior, v_prior)]
        w_new, m_new, v_new, w_bf, loss_mean = adam(rate, token_count, part, totals, clip_tau.reshape(1, 1), *state)
        w_all = all_gather_rows(w_bf).reshape(w_work.shape)
        return (loss_mean.reshape(()), w_all) + tuple(z.reshape(w_master.shape) for z in (w_new, m_new, v_new))

    row_spec = P(None, 'data', None)
    shard_spec = P('stage', None, 'data')
    stage_spec = P('stage', None, None)
    return jax.shard_map(device_step, mesh=mesh, in_specs=(row_spec, row_spec, stage_spec, shard_spec, shard_spec, shard_spec, P()), out_specs=(P(), stage_spec, shard_spec, shard_spec, shard_spec), check_vma=False)
```
